32 devices in a mesh: groups: 2 (over x), expert: 16 (over z, y, core).
Axes of the slice: x: 2, y: 2, z: 4, core: 2. Of those that a mesh axis runs over, the one named last changes fastest.
Arguments:
- hidden_in: bfloat16 [256, 4096], P(('groups', 'expert')), parts along dimension 0, may hold values from -6 to 6
- queries: bfloat16 [256, 4096], P(('groups', 'expert')), parts along dimension 0, may hold values from -8 to 8
- decode_key_value: bfloat16 [256, 2, 256], P(('groups', 'expert')), parts along dimension 0, may hold values from -6 to 6
- local_kv: bfloat16 [1024, 2, 16, 256], P(('groups', 'expert')), parts along dimension 0, may hold values from -8 to 8
- page_table: int32 [256, 16], P(('groups', 'expert')), parts along dimension 0, may hold values from 0 to 31
- seq_blocks: int32 [256], P(('groups', 'expert')), parts along dimension 0, may hold values from 1 to 16
- prompt_kv: bfloat16 [32, 16, 2, 16, 256], P(('groups', 'expert')), parts along dimension 0, may hold values from -8 to 8
- prompt_owner: int32 [32], P('groups'), parts along dimension 0, may hold values from 0 to 15, as said below
- prompt_pages: int32 [32], P('groups'), parts along dimension 0, may hold values from 1 to 16
- norm_gain: float32 [4096], replicated, may hold values from 0.5 to 1.5
- router: bfloat16 [4096, 8], replicated, may hold values from -0.09375 to 0.09375
- w_gate: bfloat16 [16, 4096, 384], P('expert'), may hold values from -0.09375 to 0.09375
- w_up: bfloat16 [16, 4096, 384], P('expert'), may hold values from -0.09375 to 0.09375
- w_down: bfloat16 [16, 384, 4096], P('expert'), may hold values from -0.21875 to 0.21875
- route_ids: int32 [256, 8], P(('groups', 'expert')), parts along dimension 0, may hold values from 0 to 7, as said below
Outputs:
- layer_out: bfloat16 [256, 4096], P(('groups', 'expert')), parts along dimension 0
The draws below stay inside these ranges and needn't reach their ends.
There are 2 independent parts, one for each index of `groups`. The reference program is written for one: setup_inputs(seed, part) draws one part's arguments, and reference() takes and returns one part's arrays. A program takes and returns all parts, laid end to end along the dimension named above; an argument that names none is the same for every part. Nothing has to cross between parts.
Inputs may be any that keep to these rules, and one draw needn't show every extreme that they name: `prompt_owner`: each device is named by at most 2 prompts, and by exactly 2 for some of the devices. `route_ids`: each row names 8 different experts; among the rows of one device no expert is named more than 8 times, a bound that some block reaches. `page_table`: indices among the pages of the sequence's own device.
All inputs are finite; a program needn't handle non-finite values.
Results may differ from the reference program's by a relative error of at most 0.0056.
Values may be sent and summed in bfloat16 or wider, within the bound.
A program may use at most 128 MiB of HBM per device.

```python
import math
import jax
import jax.numpy as jnp
from jax import lax

D = 4096
QUERY_HEADS = 32
KEY_VALUE_HEADS = 2
HEAD_SIZE = 128
PAGE_TOKENS = 16
FW = 768
TOPK = 8
SEQ_DEV = 8
LOCAL_PAGES = 32
MAXB = 16
MAXP = 2
EXPERTS = 8
DECODE_SEQUENCES = 128
PROMPTS = 16
PROMPT_PAGES = 16
CAP = 8
N_EXPERT = 16


def draw_prompt_owner(key, part):
    owner_key, shuffle_key = jax.random.split(jax.random.fold_in(key, 11))
    owners = jax.random.permutation(owner_key, N_EXPERT)
    quarter = N_EXPERT // 4
    listed = jnp.concatenate([owners[:quarter], owners[:quarter], owners[quarter:3 * quarter]])
    shuffle = jax.random.permutation(shuffle_key, N_EXPERT)
    return listed[shuffle].astype(jnp.int32)


def draw_route_ids(key, part):
    device_keys = jax.random.split(jax.random.fold_in(key, 13), N_EXPERT)
    orders = jax.vmap(lambda single: jax.random.permutation(single, EXPERTS))(device_keys)
    window = max(TOPK, (SEQ_DEV * TOPK + CAP - 1) // CAP)
    columns = jnp.arange(SEQ_DEV * TOPK, dtype=jnp.int32) % window
    picked = jnp.take(orders, columns, axis=1)
    return picked.reshape(N_EXPERT * SEQ_DEV, TOPK).astype(jnp.int32)


def common_direction(key):
    random_signs = jax.random.randint(jax.random.fold_in(key, 101), (KEY_VALUE_HEADS * HEAD_SIZE,), 0, 2)
    return (2 * random_signs - 1).astype(jnp.float32)


def starting_noise(key, shape):
    return jnp.clip(jax.random.normal(key, shape, jnp.float32), -6.0, 6.0)


def cache_block(key, salt, leading_share):
    noise_random_key, flag_random_key, strength_random_key, value_random_key = jax.random.split(jax.random.fold_in(key, salt), 4)
    random_noise = starting_noise(noise_random_key, leading_share + (PAGE_TOKENS, KEY_VALUE_HEADS, HEAD_SIZE))
    sign_flags = jax.random.randint(flag_random_key, leading_share + (PAGE_TOKENS, KEY_VALUE_HEADS, 1), 0, 8) == 0
    blend_strength = jax.random.uniform(strength_random_key, leading_share + (PAGE_TOKENS, KEY_VALUE_HEADS, 1), jnp.float32, 5.0, 7.5)
    unit_direction = common_direction(key).reshape(KEY_VALUE_HEADS, HEAD_SIZE)
    cached_keys = jnp.where(sign_flags, 0.3 * random_noise + blend_strength * unit_direction, random_noise)
    cached_keys = jnp.clip(cached_keys, -8.0, 8.0).reshape(leading_share + (PAGE_TOKENS, KEY_VALUE_HEADS * HEAD_SIZE))
    cached_values = starting_noise(value_random_key, leading_share + (PAGE_TOKENS, KEY_VALUE_HEADS * HEAD_SIZE))
    return jnp.stack([cached_keys, cached_values], len(leading_share))


def draw_queries(key, part):
    noise_random_key, flag_random_key, strength_random_key = jax.random.split(jax.random.fold_in(key, 5), 3)
    random_noise = starting_noise(noise_random_key, (DECODE_SEQUENCES, KEY_VALUE_HEADS, QUERY_HEADS // KEY_VALUE_HEADS, HEAD_SIZE))
    sign_flags = jax.random.randint(flag_random_key, (DECODE_SEQUENCES, 1, 1, 1), 0, 4) == 0
    blend_strength = jax.random.uniform(strength_random_key, (DECODE_SEQUENCES, 1, 1, 1), jnp.float32, 2.0, 7.5)
    unit_direction = common_direction(key).reshape(1, KEY_VALUE_HEADS, 1, HEAD_SIZE)
    rows = jnp.where(sign_flags, 0.3 * random_noise + blend_strength * unit_direction, random_noise)
    return jnp.clip(rows, -8.0, 8.0).reshape(DECODE_SEQUENCES, QUERY_HEADS * HEAD_SIZE).astype(jnp.bfloat16)


def draw_local_kv(key, part):
    return cache_block(key, 7, (N_EXPERT * LOCAL_PAGES,)).astype(jnp.bfloat16)


def draw_prompt_kv(key, part):
    return cache_block(key, 8, (PROMPT_PAGES, PROMPTS)).astype(jnp.bfloat16)


def with_ends(drawn, key, smallest, high):
    place = [jax.random.randint(jax.random.fold_in(key, axis), (), 0, length) for axis, length in enumerate(drawn.shape)]
    widest = drawn.shape.index(max(drawn.shape))
    neighbour = place[:widest] + [(place[widest] + 1) % drawn.shape[widest]] + place[widest + 1:]
    return drawn.at[tuple(place)].set(smallest).at[tuple(neighbour)].set(high)


def shard_levels(rng, shape, cuts, least, high):
    gain, own = 1.0, jax.random.fold_in(rng, 6)
    for axis_at, parts in cuts:
        draws = jnp.exp(jax.random.uniform(jax.random.fold_in(own, axis_at), (parts,), jnp.float32, least / len(cuts), high / len(cuts)))
        gain = gain * jnp.repeat(draws, shape[axis_at] // parts).reshape([-1 if axis == axis_at else 1 for axis in range(len(shape))])
    return gain


def bell_draw(stream_key, extent, width, most, cuts=(), kind=jnp.bfloat16):
    values = jax.random.normal(stream_key, extent, jnp.float32) * width
    if len(cuts) > 0:
        values = shard_levels(stream_key, extent, cuts, -0.22, 0.18) * values
    return jnp.clip(values, min=-most, max=most).astype(kind)


def setup_inputs(seed: int = 0, part: int = 0) -> dict:
    splits = jax.random.split(jax.random.key(seed), 16)
    own_keys = jax.random.split(jax.random.fold_in(splits[15], part), 16)
    return {
        "hidden_in": bell_draw(own_keys[0], (DECODE_SEQUENCES, D), 1.0, 6.0, ((0, 16),)),
        "queries": draw_queries(jax.random.fold_in(jax.random.fold_in(splits[15], part), 71), part),
        "decode_key_value": bell_draw(own_keys[2], (DECODE_SEQUENCES, 2, KEY_VALUE_HEADS * HEAD_SIZE), 1.0, 6.0, ((0, 16),)),
        "local_kv": draw_local_kv(jax.random.fold_in(jax.random.fold_in(splits[15], part), 71), part),
        "page_table": with_ends(jax.random.randint(own_keys[4], (DECODE_SEQUENCES, MAXB), 0, LOCAL_PAGES), jax.random.fold_in(own_keys[4], 1), 0, LOCAL_PAGES - 1).astype(jnp.int32),
        "seq_blocks": with_ends(jax.random.randint(own_keys[5], (DECODE_SEQUENCES,), 1, MAXB + 1), jax.random.fold_in(own_keys[5], 1), 1, MAXB).astype(jnp.int32),
        "prompt_kv": draw_prompt_kv(jax.random.fold_in(jax.random.fold_in(splits[15], part), 71), part),
        "prompt_owner": draw_prompt_owner(jax.random.fold_in(jax.random.fold_in(splits[15], part), 71), part),
        "prompt_pages": with_ends(jax.random.randint(own_keys[8], (PROMPTS,), 1, PROMPT_PAGES + 1), jax.random.fold_in(own_keys[8], 1), 1, PROMPT_PAGES).astype(jnp.int32),
        "norm_gain": jnp.clip(1.0 + 0.1 * jax.random.normal(splits[9], (D,), jnp.float32), 0.5, 1.5),
        "router": bell_draw(splits[10], (D, EXPERTS), D ** -0.5, 0.09375),
        "w_gate": bell_draw(splits[11], (2 * EXPERTS, D, FW // 2), D ** -0.5, 0.09375, ((0, 16),)),
        "w_up": bell_draw(splits[12], (2 * EXPERTS, D, FW // 2), D ** -0.5, 0.09375, ((0, 16),)),
        "w_down": bell_draw(splits[13], (2 * EXPERTS, FW // 2, D), FW ** -0.5, 0.21875, ((0, 16),)),
        "route_ids": draw_route_ids(jax.random.fold_in(jax.random.fold_in(splits[15], part), 71), part),
    }


norm_eps = 1e-06
masked_score = -1e+30

def attend(rows_of_queries, rows_of_keys, rows_of_values, allowed, token_own_key, token_own_value):
    decode_tokens = rows_of_queries.shape[0]
    heads_of_queries = rows_of_queries.astype(jnp.float32).reshape(decode_tokens, KEY_VALUE_HEADS, QUERY_HEADS // KEY_VALUE_HEADS, HEAD_SIZE)
    heads_of_keys = rows_of_keys.astype(jnp.float32).reshape(decode_tokens, -1, KEY_VALUE_HEADS, HEAD_SIZE)
    heads_of_values = rows_of_values.astype(jnp.float32).reshape(decode_tokens, -1, KEY_VALUE_HEADS, HEAD_SIZE)
    scale_for_scores = 1.0 / math.sqrt(HEAD_SIZE)
    allowed_mask = allowed[:, None, None, :]
    scores = jnp.einsum('tkgd,tlkd->tkgl', heads_of_queries, heads_of_keys) * scale_for_scores
    scores = jnp.where(allowed_mask, scores, masked_score)
    token_own_score = jnp.einsum('xejp,xep->xej', heads_of_queries, token_own_key.astype(jnp.float32).reshape(decode_tokens, KEY_VALUE_HEADS, HEAD_SIZE)) * scale_for_scores
    peak = jnp.maximum(lax.optimization_barrier(jnp.max(scores, -1)), token_own_score)
    weights = jnp.where(allowed_mask, jnp.exp(scores - peak[..., None]), 0.0)
    own_weight = jnp.exp(token_own_score - peak)
    denominator = lax.optimization_barrier(jnp.sum(weights, -1)) + own_weight
    probs = lax.optimization_barrier((weights / denominator[..., None]).astype(jnp.bfloat16)).astype(jnp.float32)
    token_own_probability = lax.optimization_barrier((own_weight / denominator).astype(jnp.bfloat16)).astype(jnp.float32)
    blended_noise = jnp.einsum('tkgl,tlkd->tkgd', probs, heads_of_values)
    blended_noise = blended_noise + token_own_probability[..., None] * token_own_value.astype(jnp.float32).reshape(decode_tokens, KEY_VALUE_HEADS, 1, HEAD_SIZE)
    return blended_noise.reshape(decode_tokens, QUERY_HEADS * HEAD_SIZE).astype(jnp.bfloat16)

def reference(hidden_in, queries, decode_key_value, local_kv, page_table, seq_blocks, prompt_kv, prompt_owner, prompt_pages, norm_gain, router, w_gate, w_up, w_down, route_ids):
    devices = N_EXPERT
    experts = devices // 2
    key_value_width = KEY_VALUE_HEADS * HEAD_SIZE
    prompt_count = prompt_owner.shape[0]
    prompt_range = jnp.arange(prompt_count, dtype=jnp.int32)
    same_owner = prompt_owner[:, None] == prompt_owner[None, :]
    earlier = prompt_range[None, :] < prompt_range[:, None]
    arrival = lax.optimization_barrier(jnp.sum((same_owner & earlier).astype(jnp.int32), 1))
    matching = (prompt_owner[None, None, :] == jnp.arange(devices, dtype=jnp.int32)[:, None, None]) & (arrival[None, None, :] == jnp.arange(MAXP, dtype=jnp.int32)[None, :, None])
    chosen_prompt = lax.optimization_barrier(jnp.sum(jnp.where(matching, prompt_range[None, None, :], 0), -1)).astype(jnp.int32)
    occupied = jnp.any(matching, -1)

    def owner_attention(inputs):
        owner_index, rows_of_queries, own_kv, pool, table, blocks = inputs
        fetched = pool[table]
        old_keys = fetched[:, :, 0].reshape(SEQ_DEV, MAXB * PAGE_TOKENS, key_value_width)
        old_values = fetched[:, :, 1].reshape(SEQ_DEV, MAXB * PAGE_TOKENS, key_value_width)
        old_allowed = (jnp.arange(MAXB * PAGE_TOKENS, dtype=jnp.int32) // PAGE_TOKENS)[None, :] < blocks[:, None]
        old_out = attend(rows_of_queries, old_keys, old_values, old_allowed, own_kv[:, 0], own_kv[:, 1])
        picks = chosen_prompt[owner_index]
        fresh_pages = jnp.take(prompt_kv, picks, axis=1)
        new_keys = jnp.moveaxis(fresh_pages[:, :, 0], 1, 0).reshape(MAXP, PROMPT_PAGES * PAGE_TOKENS, key_value_width)
        new_values = jnp.moveaxis(fresh_pages[:, :, 1], 1, 0).reshape(MAXP, PROMPT_PAGES * PAGE_TOKENS, key_value_width)
        lengths = prompt_pages[picks]
        new_allowed = (jnp.arange(PROMPT_PAGES * PAGE_TOKENS, dtype=jnp.int32) // PAGE_TOKENS)[None, :] < lengths[:, None]
        new_out = attend(rows_of_queries[:MAXP], new_keys, new_values, new_allowed, own_kv[:MAXP, 0], own_kv[:MAXP, 1])
        new_count = jnp.sum(occupied[owner_index].astype(jnp.int32))
        is_new = jnp.arange(MAXP, dtype=jnp.int32) < new_count
        head_rows = jnp.where(is_new[:, None], new_out, old_out[:MAXP])
        return jnp.concatenate([head_rows, old_out[MAXP:]], 0)
    attention = lax.map(owner_attention, (jnp.arange(devices, dtype=jnp.int32), queries.reshape(devices, SEQ_DEV, QUERY_HEADS * HEAD_SIZE), decode_key_value.reshape(devices, SEQ_DEV, 2, key_value_width), local_kv.reshape(devices, LOCAL_PAGES, 2, PAGE_TOKENS, key_value_width), page_table.reshape(devices, SEQ_DEV, MAXB), seq_blocks.reshape(devices, SEQ_DEV))).reshape(DECODE_SEQUENCES, QUERY_HEADS * HEAD_SIZE)
    residual = (hidden_in.astype(jnp.float32) + attention.astype(jnp.float32)).astype(jnp.bfloat16)
    resid_wide = residual.astype(jnp.float32)
    normed = (resid_wide * lax.rsqrt(lax.optimization_barrier(jnp.mean(resid_wide * resid_wide, -1, keepdims=True)) + norm_eps) * norm_gain).astype(jnp.bfloat16)
    logits = jnp.dot(normed, router, preferred_element_type=jnp.float32)
    selected = jnp.take_along_axis(logits, route_ids, axis=1)
    gate_weights = jax.nn.softmax(selected, -1)
    assigned = SEQ_DEV * TOPK
    expert_ids = route_ids.reshape(devices, assigned)
    chosen = (expert_ids[:, :, None] == jnp.arange(experts, dtype=jnp.int32)[None, None, :]).astype(jnp.int32)
    before = jnp.cumsum(chosen, 1) - chosen
    slot_rank = lax.optimization_barrier(jnp.sum(before * chosen, 2))
    token_index = jnp.arange(devices, dtype=jnp.int32)[:, None] * SEQ_DEV + jnp.arange(assigned, dtype=jnp.int32)[None, :] // TOPK
    gate_flat = gate_weights.reshape(devices, assigned)

    def expert_step(accumulated, expert_index):
        hits = (expert_ids == expert_index)[:, None, :] & (slot_rank[:, None, :] == jnp.arange(CAP, dtype=jnp.int32)[None, :, None])
        present = jnp.any(hits, -1)
        row_token = lax.optimization_barrier(jnp.sum(jnp.where(hits, token_index[:, None, :], 0), -1)).astype(jnp.int32).reshape(-1)
        row_gate = lax.optimization_barrier(jnp.sum(jnp.where(hits, gate_flat[:, None, :], 0.0), -1)).reshape(-1)
        gathered_rows = jnp.where(present.reshape(-1)[:, None], normed[row_token], 0).astype(normed.dtype)
        expert_total = jnp.zeros((devices * CAP, D), jnp.float32)
        for half_index in range(2):
            weight_index = 2 * expert_index + half_index
            gate_proj = jnp.dot(gathered_rows, w_gate[weight_index], preferred_element_type=jnp.float32)
            up_proj = jnp.dot(gathered_rows, w_up[weight_index], preferred_element_type=jnp.float32)
            activated = (jax.nn.silu(gate_proj) * up_proj).astype(jnp.bfloat16)
            expert_total = expert_total + jnp.dot(activated, w_down[weight_index], preferred_element_type=jnp.float32)
        expert_out = lax.optimization_barrier(expert_total.astype(jnp.bfloat16)).astype(jnp.float32)
        accumulated = accumulated.at[row_token].add(expert_out * row_gate[:, None])
        return (accumulated, None)
    accumulated, _ = lax.scan(expert_step, jnp.zeros((DECODE_SEQUENCES, D), jnp.float32), jnp.arange(experts, dtype=jnp.int32))
    return (resid_wide + accumulated).astype(jnp.bfloat16)
```

```python
import functools
import math

import jax
import jax.numpy as jnp
from jax import lax
from jax.experimental import pallas as pl
from jax.experimental.pallas import tpu as pltpu
from jax.sharding import PartitionSpec as P

D = 4096
QUERY_HEADS = 32
KEY_VALUE_HEADS = 2
HEAD_SIZE = 128
PAGE_TOKENS = 16
TOPK = 8
MAXB = 16
MAXP = 2


norm_eps = 1e-06
masked_score = -1e30


def partner(x, axis, apart):
    return lax.ppermute(x, axis, [(i, i ^ 1 << apart) for i in range(lax.axis_size(axis))])


def attend(rows_of_queries, rows_of_keys, rows_of_values, allowed, token_own_key, token_own_value):
    decode_tokens = rows_of_queries.shape[0]
    heads_of_queries = rows_of_queries.reshape(
        decode_tokens, KEY_VALUE_HEADS, QUERY_HEADS // KEY_VALUE_HEADS, HEAD_SIZE
    )
    heads_of_keys = rows_of_keys.reshape(decode_tokens, -1, KEY_VALUE_HEADS, HEAD_SIZE)
    heads_of_values = rows_of_values.reshape(decode_tokens, -1, KEY_VALUE_HEADS, HEAD_SIZE)
    scale_for_scores = 1.0 / math.sqrt(HEAD_SIZE)
    allowed_mask = allowed[:, None, None, :]
    scores = (
        jnp.einsum(
            "tkgd,tlkd->tkgl", heads_of_queries, heads_of_keys, preferred_element_type=jnp.float32
        )
        * scale_for_scores
    )
    scores = jnp.where(allowed_mask, scores, masked_score)
    token_own_score = (
        jnp.einsum(
            "xejp,xep->xej",
            heads_of_queries,
            token_own_key.reshape(decode_tokens, KEY_VALUE_HEADS, HEAD_SIZE),
            preferred_element_type=jnp.float32,
        )
        * scale_for_scores
    )
    peak = jnp.maximum(jnp.max(scores, -1), token_own_score)
    weights = jnp.where(allowed_mask, jnp.exp(scores - peak[..., None]), 0.0)
    own_weight = jnp.exp(token_own_score - peak)
    denominator = jnp.sum(weights, -1) + own_weight
    probs = (weights / denominator[..., None]).astype(jnp.bfloat16)
    token_own_probability = (own_weight / denominator).astype(jnp.bfloat16)
    blended_noise = jnp.einsum(
        "tkgl,tlkd->tkgd", probs, heads_of_values, preferred_element_type=jnp.float32
    )
    blended_noise = blended_noise + token_own_probability.astype(jnp.float32)[
        ..., None
    ] * token_own_value.reshape(decode_tokens, KEY_VALUE_HEADS, 1, HEAD_SIZE).astype(jnp.float32)
    return blended_noise.reshape(decode_tokens, QUERY_HEADS * HEAD_SIZE).astype(jnp.bfloat16)


def routed(
    hidden_in,
    queries,
    decode_key_value,
    local_kv,
    page_table,
    seq_blocks,
    prompt_kv,
    prompt_owner,
    prompt_pages,
    norm_gain,
    router,
    w_gate,
    w_up,
    w_down,
    route_ids,
):
    devices = lax.axis_size("expert")
    position = lax.axis_index("expert")
    experts = devices // 2
    seq_dev = hidden_in.shape[0]
    key_value_width = KEY_VALUE_HEADS * HEAD_SIZE
    capacity = min(seq_dev, max(2, 2 * ((3 * seq_dev * TOPK + 2 * devices - 1) // (2 * devices))))
    half_cap = capacity // 2
    even_core = position % 2 == 0
    prompt_count = prompt_owner.shape[0]
    prompt_range = jnp.arange(prompt_count, dtype=jnp.int32)
    same_owner = prompt_owner[:, None] == prompt_owner[None, :]
    earlier = prompt_range[None, :] < prompt_range[:, None]
    arrival = jnp.sum((same_owner & earlier).astype(jnp.int32), 1)
    matching = (
        prompt_owner[None, None, :] == jnp.arange(devices, dtype=jnp.int32)[:, None, None]
    ) & (arrival[None, None, :] == jnp.arange(MAXP, dtype=jnp.int32)[None, :, None])
    chosen_prompt = jnp.sum(jnp.where(matching, prompt_range[None, None, :], 0), -1)
    occupied = jnp.any(matching, -1)
    own_picks = lax.dynamic_index_in_dim(chosen_prompt, position, 0, keepdims=False)
    own_occupied = lax.dynamic_index_in_dim(occupied, position, 0, keepdims=False)
    page_rows = prompt_kv[0]
    outgoing = jnp.take(page_rows, chosen_prompt.T.reshape(-1), axis=0).reshape(
        MAXP, devices, 2, PAGE_TOKENS, key_value_width
    )
    outgoing = jnp.where(occupied.T[:, :, None, None, None], outgoing, 0)
    arrived = lax.all_to_all(outgoing, "expert", split_axis=1, concat_axis=1, tiled=True)
    lengths = jnp.take(prompt_pages, own_picks)
    new_keys = arrived[:, :, 0].reshape(MAXP, devices * PAGE_TOKENS, key_value_width)
    new_values = arrived[:, :, 1].reshape(MAXP, devices * PAGE_TOKENS, key_value_width)
    new_allowed = (jnp.arange(devices * PAGE_TOKENS, dtype=jnp.int32) // PAGE_TOKENS)[
        None, :
    ] < lengths[:, None]
    fresh_rows = attend(
        queries[:MAXP],
        new_keys,
        new_values,
        new_allowed,
        decode_key_value[:MAXP, 0],
        decode_key_value[:MAXP, 1],
    )
    fetched = local_kv[page_table]
    old_keys = fetched[:, :, 0].reshape(seq_dev, MAXB * PAGE_TOKENS, key_value_width)
    old_values = fetched[:, :, 1].reshape(seq_dev, MAXB * PAGE_TOKENS, key_value_width)
    old_allowed = (jnp.arange(MAXB * PAGE_TOKENS, dtype=jnp.int32) // PAGE_TOKENS)[
        None, :
    ] < seq_blocks[:, None]
    old_out = attend(
        queries, old_keys, old_values, old_allowed, decode_key_value[:, 0], decode_key_value[:, 1]
    )
    new_count = jnp.sum(own_occupied.astype(jnp.int32))
    is_new = jnp.arange(MAXP, dtype=jnp.int32) < new_count
    attention = jnp.concatenate(
        [jnp.where(is_new[:, None], fresh_rows, old_out[:MAXP]), old_out[MAXP:]], 0
    )
    residual = (hidden_in.astype(jnp.float32) + attention.astype(jnp.float32)).astype(jnp.bfloat16)
    resid_wide = residual.astype(jnp.float32)
    normed = (
        resid_wide
        * lax.rsqrt(jnp.mean(resid_wide * resid_wide, -1, keepdims=True) + norm_eps)
        * norm_gain
    ).astype(jnp.bfloat16)
    logits = jnp.dot(normed, router, preferred_element_type=jnp.float32)
    expert_onehot = route_ids[:, :, None] == jnp.arange(experts, dtype=jnp.int32)[None, None, :]
    selected = jnp.sum(jnp.where(expert_onehot, logits[:, None, :], 0.0), -1)
    gate_weights = jax.nn.softmax(selected, -1)
    assigned = seq_dev * TOPK
    expert_ids = route_ids.reshape(assigned)
    chosen = (expert_ids[:, None] == jnp.arange(experts, dtype=jnp.int32)[None, :]).astype(
        jnp.int32
    )
    before = jnp.cumsum(chosen, 0) - chosen
    slot_rank = jnp.sum(before * chosen, 1)
    slot_index = expert_ids * capacity + slot_rank
    placing = slot_index[None, :] == jnp.arange(experts * capacity, dtype=jnp.int32)[:, None]
    selector = jnp.any(placing.reshape(experts * capacity, seq_dev, TOPK), -1).astype(jnp.bfloat16)
    gathered_rows = jnp.dot(selector, normed, preferred_element_type=jnp.float32).astype(
        jnp.bfloat16
    )
    outgoing_half = gathered_rows.reshape(devices, half_cap, D)
    own_half = lax.all_to_all(outgoing_half, "expert", split_axis=0, concat_axis=0, tiled=True)
    partner_half = partner(own_half, "expert", 0)
    received = jnp.where(
        even_core,
        jnp.concatenate([own_half, partner_half], 1),
        jnp.concatenate([partner_half, own_half], 1),
    )
    flattened = received.reshape(devices * capacity, D)
    gate_proj = jnp.dot(flattened, w_gate[0], preferred_element_type=jnp.float32)
    up_proj = jnp.dot(flattened, w_up[0], preferred_element_type=jnp.float32)
    activated = (jax.nn.silu(gate_proj) * up_proj).astype(jnp.bfloat16)
    partial_value = jnp.dot(activated, w_down[0], preferred_element_type=jnp.float32).reshape(
        devices, capacity, D
    )
    kept = jnp.where(even_core, partial_value[:, :half_cap], partial_value[:, half_cap:])
    handed = jnp.where(even_core, partial_value[:, half_cap:], partial_value[:, :half_cap])
    partner_part = partner(handed, "expert", 0)
    finished = (kept + partner_part).astype(jnp.bfloat16)
    returned = lax.all_to_all(finished, "expert", split_axis=0, concat_axis=0, tiled=True)
    expert_sum = returned.reshape(experts * capacity, D)
    picked = jnp.take(expert_sum, slot_index, axis=0).astype(jnp.float32).reshape(seq_dev, TOPK, D)
    expert_mix = jnp.sum(picked * gate_weights[:, :, None], 1)
    return (resid_wide + expert_mix).astype(jnp.bfloat16)


def layer_kernel(
    devices,
    owners,
    prompt_lengths,
    blocks,
    pages_hbm,
    q_hbm,
    dkv_hbm,
    table_hbm,
    kv_hbm,
    hidden_hbm,
    gain_hbm,
    router_hbm,
    ids_hbm,
    gate_hbm,
    up_hbm,
    down_hbm,
    out_hbm,
    pages_ref,
    q_ref,
    dkv_ref,
    table_ref,
    kv_ref,
    hidden_ref,
    gain_ref,
    router_ref,
    ids_ref,
    w_in,
    w_down,
    other_pages,
    q_send,
    q_recv,
    o_send,
    o_recv,
    lse_send,
    lse_recv,
    attn,
    x_a,
    gates_a,
    x_b,
    gates_b,
    part_a,
    core_a,
    y_send,
    y_recv,
    z_send,
    z_recv,
    kept,
    part_b,
    core_b,
    sum_b,
    recv_b,
    out_ref,
    in_sem,
    w_sem,
    page_sem,
    q_sem,
    o_sem,
    lse_sem,
    xa_ssem,
    xa_rsem,
    xb_sem,
    xf_sem,
    c_sem,
    y_sem,
    zs_sem,
    zr_sem,
    cb_sem,
    rb_sem,
    out_sem,
):
    f32, bf16 = jnp.float32, jnp.bfloat16
    me = lax.axis_index("expert")
    lines = devices // 4
    chips = devices // 2
    core, row, line = lax.rem(me, 2), lax.rem(me // 2, 2), me // 4
    unit = row * lines + line
    seqs = hidden_ref.shape[0]
    group = QUERY_HEADS // KEY_VALUE_HEADS
    scale = 1.0 / math.sqrt(HEAD_SIZE)
    old_rows = pl.ds(MAXP, seqs - MAXP)
    new_rows = pl.ds(0, MAXP)

    def device(at_line, at_row, at_core):
        return (at_line * 2 + at_row) * 2 + at_core

    def device_of(at_unit, at_core):
        return device(lax.rem(at_unit, lines), at_unit // lines, at_core)

    def place(at_line, at_row, at_core):
        return (at_core * 2 + at_row) * lines + at_line

    def remote(src, dst, ssem, rsem, to):
        return pltpu.make_async_remote_copy(
            src_ref=src,
            dst_ref=dst,
            send_sem=ssem,
            recv_sem=rsem,
            device_id={"expert": to},
            device_id_type=pl.DeviceIdType.MESH,
        )

    other_row = device(line, 1 - row, core)
    other_core = device(line, row, 1 - core)
    mine = place(line, row, core)

    loads = [
        pltpu.make_async_copy(a, b, in_sem.at[i])
        for i, (a, b) in enumerate(
            (
                (q_hbm, q_ref),
                (pages_hbm, pages_ref),
                (dkv_hbm, dkv_ref),
                (table_hbm, table_ref),
                (kv_hbm, kv_ref),
                (hidden_hbm, hidden_ref),
                (gain_hbm, gain_ref),
                (router_hbm, router_ref),
                (ids_hbm, ids_ref),
            )
        )
    ]
    hidden = w_down.shape[0]
    weights = [
        pltpu.make_async_copy(gate_hbm.at[0], w_in.at[:, pl.ds(0, hidden)], w_sem.at[0]),
        pltpu.make_async_copy(up_hbm.at[0], w_in.at[:, pl.ds(hidden, hidden)], w_sem.at[1]),
        pltpu.make_async_copy(down_hbm.at[0], w_down, w_sem.at[2]),
    ]
    barrier = pltpu.get_barrier_semaphore()

    def greet(k, carry):
        pl.semaphore_signal(
            barrier,
            inc=1,
            device_id={"expert": lax.rem(me + k, devices)},
            device_id_type=pl.DeviceIdType.MESH,
        )
        return carry

    lax.fori_loop(1, devices, greet, 0)
    for copy in loads + weights:
        copy.start()

    fold = seqs // MAXP
    lane_heads = QUERY_HEADS // fold
    packed = lane_heads * HEAD_SIZE
    per_kv = lane_heads // KEY_VALUE_HEADS
    sub = lax.broadcasted_iota(jnp.int32, (seqs, packed), 0) // MAXP

    def head_cols(h):
        return slice(h * HEAD_SIZE, (h + 1) * HEAD_SIZE)

    def turn(x, by):
        by = by % seqs
        return x if by == 0 else pltpu.roll(x, by, 0)

    def pack(rows):
        out = None
        for f in range(fold):
            wide = turn(
                jnp.concatenate([rows[:, head_cols(fold * hh + f)] for hh in range(lane_heads)], 1),
                MAXP * f,
            )
            out = wide if f == 0 else jnp.where(sub == f, wide, out)
        return out

    def spread_rows(rows):
        out = rows
        at = lax.broadcasted_iota(jnp.int32, rows.shape, 0) // MAXP
        for f in range(1, fold):
            out = jnp.where(at == f, turn(rows, MAXP * f), out)
        return out

    def dot_t(a, b):
        return lax.dot_general(a, b, (((1,), (1,)), ((), ())), preferred_element_type=f32)

    loads[0].wait()
    q_packed = pack(q_ref[...].astype(f32))
    q_send[...] = q_packed.astype(bf16)
    pl.semaphore_wait(barrier, devices - 1)

    def q_copy(k):
        to = device_of(lax.rem(unit + k, chips), core)
        return remote(q_send, q_recv.at[unit], q_sem.at[0, k], q_sem.at[1, k], to)

    def q_go(k, carry):
        q_copy(k).start()
        return carry

    lax.fori_loop(1, chips, q_go, 0)
    q_recv[unit] = q_packed.astype(bf16)
    loads[1].wait()
    page_copy = remote(pages_ref, other_pages, page_sem.at[0], page_sem.at[1], other_core)
    page_copy.start()

    for copy in loads[2:]:
        copy.wait()

    def per_seq(values, shape):
        at = lax.broadcasted_iota(jnp.int32, shape, 0)
        return sum(jnp.where(at == s, v, 0) for s, v in enumerate(values))

    tokens = kv_ref.shape[0] * PAGE_TOKENS
    limit = per_seq([blocks[s] for s in range(seqs)], (seqs, tokens))
    page_of = lax.broadcasted_iota(jnp.int32, (seqs, tokens), 1) // PAGE_TOKENS
    held = jnp.zeros((seqs, tokens), f32)
    for b in range(table_ref.shape[1]):
        hit = (page_of == table_ref[:, b : b + 1]) & (limit > b)
        held = held + jnp.where(hit, 1.0, 0.0)
    held = jnp.concatenate([held] * group, 0)

    def heads(h):
        rows = q_ref[...].astype(f32)
        return jnp.concatenate([rows[:, head_cols(h * group + g)] for g in range(group)], 0)

    def own(h, at):
        both = dkv_ref[...].astype(f32)
        return jnp.concatenate([both[:, at, head_cols(h)]] * group, 0)

    def weigh(scores, times, own_score):
        scores = jnp.where(times > 0, scores, masked_score)
        peak = jnp.maximum(jnp.max(scores, -1, keepdims=True), own_score)
        weight = times * jnp.exp(scores - peak)
        own_weight = jnp.exp(own_score - peak)
        total = jnp.sum(weight, -1, keepdims=True) + own_weight
        return (weight / total).astype(bf16), (own_weight / total).astype(bf16).astype(f32)

    for h in range(KEY_VALUE_HEADS):
        at = head_cols(h)
        queries = heads(h)
        own_score = jnp.sum(queries * own(h, 0), -1, keepdims=True) * scale
        keys = kv_ref[:, 0, :, at].reshape(tokens, HEAD_SIZE)
        values = kv_ref[:, 1, :, at].reshape(tokens, HEAD_SIZE)
        probs, own_prob = weigh(dot_t(queries.astype(bf16), keys) * scale, held, own_score)
        mixed = jnp.dot(probs, values, preferred_element_type=f32) + own_prob * own(h, 1)
        for g in range(group):
            attn[:, head_cols(h * group + g)] = mixed[g * seqs : (g + 1) * seqs]

    def residual_of(attention):
        rounded = attention.astype(bf16).astype(f32)
        return (hidden_ref[...].astype(f32) + rounded).astype(bf16).astype(f32)

    def norm_of(wide):
        mean = jnp.mean(wide * wide, -1, keepdims=True)
        return (wide * lax.rsqrt(mean + norm_eps) * gain_ref[...]).astype(bf16)

    def gate_of(normed):
        logits = dot_t(normed, router_ref[...])
        experts = logits.shape[1]
        expert_of = lax.broadcasted_iota(jnp.int32, (seqs, experts), 1)
        times = jnp.zeros((seqs, experts), f32)
        for k in range(ids_ref.shape[1]):
            times = times + jnp.where(ids_ref[:, k : k + 1] == expert_of, 1.0, 0.0)
        picked = jnp.where(times > 0, logits, masked_score)
        gate = times * jnp.exp(picked - jnp.max(picked, -1, keepdims=True))
        gate = gate / jnp.sum(gate, -1, keepdims=True)
        return jnp.concatenate([gate] * (128 // experts), 1)

    normed = norm_of(residual_of(attn[...]))
    x_a[mine] = normed

    def pass_on(pool, spot, at, to):
        buffer, rows, n = pool
        ref = buffer.at[spot, rows]
        return remote(ref, ref, xa_ssem.at[n, at], xa_rsem.at[n, spot], to)

    def first_hops(pool):
        copies = []
        for k in range(1, lines):
            copies.append(pass_on(pool, mine, k, device(lax.rem(line + k, lines), row, core)))
        copies.append(pass_on(pool, mine, 0, other_row))
        copies.append(pass_on(pool, mine, lines, other_core))
        for copy in copies:
            copy.start()
        return copies

    def arrived(pool, spot):
        pass_on(pool, spot, 0, other_core).wait_recv()

    pools = [(x_a, old_rows, 0), (gates_a, pl.ds(0, seqs), 1)]
    sent = first_hops(pools[0])
    gates_a[mine] = gate_of(normed)
    sent += first_hops(pools[1])

    prompts = owners.shape[0]
    shape = (1, prompts * PAGE_TOKENS)
    prompt_of = lax.broadcasted_iota(jnp.int32, shape, 1) // PAGE_TOKENS
    owner_of, length_of = jnp.zeros(shape, jnp.int32), jnp.zeros(shape, jnp.int32)
    for p in range(prompts):
        owner_of = jnp.where(prompt_of == p, owners[p], owner_of)
        length_of = jnp.where(prompt_of == p, prompt_lengths[p], length_of)
    rank_of = jnp.zeros(shape, jnp.int32)
    for p in range(prompts):
        rank_of = rank_of + jnp.where((owner_of == owners[p]) & (prompt_of > p), 1, 0)
    slots = chips * seqs
    at_row = lax.broadcasted_iota(jnp.int32, (slots, 1), 0)
    row_unit = at_row // seqs
    row_owner = device_of(row_unit, core)
    match = (owner_of == row_owner) & (rank_of == lax.rem(at_row, MAXP))

    def allowed_at(position):
        ok = match & (length_of > position)
        return jnp.concatenate([jnp.where(ok, 1.0, 0.0)] * per_kv, 0)

    allowed = (allowed_at(me), allowed_at(other_core))
    page_copy.wait_recv()

    def q_end(k, carry):
        q_copy(k).wait_recv()
        return carry

    lax.fori_loop(1, chips, q_end, 0)
    lane_of = lax.broadcasted_iota(jnp.int32, (slots, 128), 1)
    lse_all = jnp.zeros((slots, 128), f32)
    for h in range(KEY_VALUE_HEADS):
        at = head_cols(h)
        lanes = [h * per_kv + j for j in range(per_kv)]
        queries = jnp.concatenate(
            [q_recv[:, :, head_cols(hh)].reshape(slots, HEAD_SIZE) for hh in lanes], 0
        )
        scores = []
        for ref, ok in zip((pages_ref, other_pages), allowed):
            keys = ref[:, 0, :, at].reshape(prompts * PAGE_TOKENS, HEAD_SIZE)
            scores.append(jnp.where(ok > 0, dot_t(queries, keys) * scale, masked_score))
        peak = jnp.maximum(
            jnp.max(scores[0], -1, keepdims=True), jnp.max(scores[1], -1, keepdims=True)
        )
        total = jnp.zeros((slots * per_kv, 1), f32)
        mixed = jnp.zeros((slots * per_kv, HEAD_SIZE), f32)
        for ref, ok, score in zip((pages_ref, other_pages), allowed, scores):
            weight = ok * jnp.exp(score - peak)
            total = total + jnp.sum(weight, -1, keepdims=True)
            values = ref[:, 1, :, at].reshape(prompts * PAGE_TOKENS, HEAD_SIZE)
            mixed = mixed + jnp.dot(weight.astype(bf16), values, preferred_element_type=f32)
        some = total > 0
        safe = jnp.where(some, total, 1.0)
        mixed = mixed / safe
        lse = jnp.where(some, peak + jnp.log(safe), masked_score)
        for j, hh in enumerate(lanes):
            rows = slice(j * slots, (j + 1) * slots)
            o_send[:, :, head_cols(hh)] = mixed[rows].astype(bf16).reshape(chips, seqs, HEAD_SIZE)
            lse_all = jnp.where(lane_of == hh, lse[rows], lse_all)
    lse_send[...] = lse_all.reshape(chips, seqs, 128)

    def o_copy(k):
        to = lax.rem(unit + k, chips)
        at = device_of(to, core)
        return (
            remote(o_send.at[to], o_recv.at[unit], o_sem.at[0, k], o_sem.at[1, k], at),
            remote(lse_send.at[to], lse_recv.at[unit], lse_sem.at[0, k], lse_sem.at[1, k], at),
        )

    def o_go(k, carry):
        for copy in o_copy(k):
            copy.start()
        return carry

    lax.fori_loop(1, chips, o_go, 0)
    o_recv[unit] = o_send[unit]
    lse_recv[unit] = lse_send[unit]

    def over_core(k):
        spot = place(lax.rem(line + k, lines), 1 - row, core)
        for pool in pools:
            arrived(pool, spot)
            copy = pass_on(pool, spot, 3 * lines - 1 + k, other_core)
            copy.start()
            sent.append(copy)

    over_core(0)
    for k in range(1, lines):
        spot = place(lax.rem(line + k, lines), row, core)
        for pool in pools:
            arrived(pool, spot)
            for step, to in ((0, other_row), (1, other_core)):
                copy = pass_on(pool, spot, lines + 2 * k - 1 + step, to)
                copy.start()
                sent.append(copy)

    own_both = dkv_ref[...].astype(f32)
    own_key = spread_rows(own_both[:, 0])
    own_value = spread_rows(own_both[:, 1])
    lane = lax.broadcasted_iota(jnp.int32, (seqs, 128), 1)
    own_score = jnp.zeros((seqs, 128), f32)
    for hh in range(lane_heads):
        score = jnp.sum(
            q_packed[:, head_cols(hh)] * own_key[:, head_cols(hh // per_kv)], -1, keepdims=True
        )
        own_score = jnp.where(lane == hh, score * scale, own_score)
    new_count = jnp.int32(0)
    for p in range(prompts):
        new_count = new_count + (owners[p] == me).astype(jnp.int32)
    is_new = lax.broadcasted_iota(jnp.int32, (seqs, HEAD_SIZE), 0) < new_count

    def o_end(k, carry):
        for copy in o_copy(k):
            copy.wait_recv()
        return carry

    lax.fori_loop(1, chips, o_end, 0)
    peak = own_score
    for u in range(chips):
        peak = jnp.maximum(peak, lse_recv[u])
    shares = [jnp.exp(lse_recv[u] - peak) for u in range(chips)]
    own_share = jnp.exp(own_score - peak)
    total = own_share
    for share in shares:
        total = total + share
    inverse = 1.0 / total
    shares = [share * inverse for share in shares]
    own_share = own_share * inverse
    for hh in range(lane_heads):
        at = head_cols(hh)
        mixed = own_share[:, hh : hh + 1] * own_value[:, head_cols(hh // per_kv)]
        for u in range(chips):
            mixed = mixed + shares[u][:, hh : hh + 1] * o_recv[u, :, at].astype(f32)
        for f in range(fold):
            cols = head_cols(fold * hh + f)
            attn[:, cols] = jnp.where(is_new, turn(mixed, -MAXP * f), attn[:, cols])
    wide = residual_of(attn[...])
    attn[...] = wide
    normed = norm_of(wide)
    x_b[mine] = normed

    b_pools = [(x_b, new_rows, 0), (gates_b, pl.ds(0, seqs), 1)]

    def b_copy(pool, k):
        buffer, rows, n = pool
        ref = buffer.at[mine, rows]
        to = device_of(lax.rem(unit + k, chips), core)
        return remote(ref, ref, xb_sem.at[0, n, k], xb_sem.at[1, n, k], to)

    def b_forward(pool, k):
        buffer, rows, n = pool
        ref = buffer.at[core * chips + lax.rem(unit + chips - k, chips), rows]
        return remote(ref, ref, xf_sem.at[0, n, k], xf_sem.at[1, n, k], other_core)

    def b_first(pool):
        def go(k, carry):
            b_copy(pool, k).start()
            return carry

        lax.fori_loop(1, chips, go, 0)
        b_forward(pool, 0).start()

    b_first(b_pools[0])
    gates_b[mine] = gate_of(normed)
    b_first(b_pools[1])

    for k in range(1, lines):
        over_core(k)
    for at_row in range(2):
        for k in range(lines):
            for pool in pools:
                arrived(pool, place(k, at_row, 1 - core))
    for copy in weights:
        copy.wait()
    total = devices * seqs
    lanes_of = lax.broadcasted_iota(jnp.int32, (total, 128), 1)

    def activate(x_ref, gates_ref):
        both = jnp.dot(x_ref[...].reshape(total, D), w_in[...], preferred_element_type=f32)
        gate_proj, up_proj = both[:, :hidden], both[:, hidden:]
        scaled = jnp.sum(
            jnp.where(lanes_of == me // 2, gates_ref[...].reshape(total, 128), 0.0),
            -1,
            keepdims=True,
        )
        return (gate_proj / (1.0 + jnp.exp(-gate_proj)) * up_proj * scaled).astype(bf16)

    chunks = c_sem.shape[1]
    width = D // chunks

    def cut(i):
        return slice(i * width, (i + 1) * width)

    def core_copy(i):
        return remote(
            part_a.at[1 - core, :, :, old_rows, cut(i)],
            core_a.at[:, :, old_rows, cut(i)],
            c_sem.at[0, i],
            c_sem.at[1, i],
            other_core,
        )

    def row_copy(i):
        return remote(
            y_send.at[:, old_rows, cut(i)],
            y_recv.at[:, old_rows, cut(i)],
            y_sem.at[0, i],
            y_sem.at[1, i],
            other_row,
        )

    def line_copy(i, k):
        to = lax.rem(line + k, lines)
        return remote(
            z_send.at[k, old_rows, cut(i)],
            z_recv.at[k, old_rows, cut(i)],
            zs_sem.at[k, i],
            zr_sem.at[k, i],
            device(to, row, core),
        )

    activated = activate(x_a, gates_a)
    for i in range(chunks):
        rows = jnp.dot(activated, w_down[:, cut(i)], preferred_element_type=f32)
        part_a[:, :, :, :, cut(i)] = rows.astype(bf16).reshape(2, 2, lines, seqs, width)
        core_copy(i).start()

    def b_pass(k, carry):
        for pool in b_pools:
            b_copy(pool, k).wait_recv()
            b_forward(pool, k).start()
        return carry

    for i in range(chunks):
        core_copy(i).wait()
        y_send[:, :, cut(i)] = (
            part_a[core, 1 - row, :, :, cut(i)].astype(f32)
            + core_a[1 - row, :, :, cut(i)].astype(f32)
        ).astype(bf16)
        row_copy(i).start()

    lax.fori_loop(1, chips, b_pass, 0)

    for i in range(chunks):
        row_copy(i).wait()

        def summed(at_line):
            return (
                part_a[core, row, at_line, :, cut(i)].astype(f32)
                + core_a[row, at_line, :, cut(i)].astype(f32)
                + y_recv[at_line, :, cut(i)].astype(f32)
            )

        for k in range(1, lines):
            z_send[k, :, cut(i)] = summed(lax.rem(line + k, lines)).astype(bf16)
            line_copy(i, k).start()
        kept[:, cut(i)] = attn[:, cut(i)] + summed(line)

    def b_arrive(k, carry):
        for pool in b_pools:
            b_forward(pool, k).wait()
        return carry

    lax.fori_loop(0, chips, b_arrive, 0)
    activated = activate(x_b, gates_b)
    b_chunks = cb_sem.shape[1]
    b_width = D // b_chunks

    def b_core(i):
        at = slice(i * b_width, (i + 1) * b_width)
        return remote(
            part_b.at[1 - core, :, new_rows, at],
            core_b.at[:, new_rows, at],
            cb_sem.at[0, i],
            cb_sem.at[1, i],
            other_core,
        )

    for i in range(b_chunks):
        at = slice(i * b_width, (i + 1) * b_width)
        rows = jnp.dot(activated, w_down[:, at], preferred_element_type=f32)
        part_b[:, :, :, at] = rows.astype(bf16).reshape(2, chips, seqs, b_width)
        b_core(i).start()

    def b_return(k):
        to = lax.rem(unit + k, chips)
        return remote(
            sum_b.at[to, new_rows],
            recv_b.at[unit, new_rows],
            rb_sem.at[0, k],
            rb_sem.at[1, k],
            device_of(to, core),
        )

    for i in range(b_chunks):
        b_core(i).wait()

    def b_sum(k, carry):
        to = lax.rem(unit + k, chips)
        sum_b[to] = (part_b[core, to].astype(f32) + core_b[to].astype(f32)).astype(bf16)
        b_return(k).start()
        return carry

    lax.fori_loop(1, chips, b_sum, 0)
    last = attn[...] + part_b[core, unit].astype(f32) + core_b[unit].astype(f32)

    answer = kept[...]
    for k in range(1, lines):
        for i in range(chunks):
            line_copy(i, k).wait()
        answer = answer + z_recv[k].astype(f32)

    def b_last(k, total):
        b_return(k).wait()
        return total + recv_b[lax.rem(unit + chips - k, chips)].astype(f32)

    for k in range(1, chips):
        last = b_last(k, last)
    is_b = lax.broadcasted_iota(jnp.int32, (seqs, D), 0) < MAXP
    out_ref[...] = jnp.where(is_b, last, answer).astype(bf16)
    out_copy = pltpu.make_async_copy(out_ref, out_hbm, out_sem)
    out_copy.start()

    page_copy.wait_send()
    for copy in sent:
        copy.wait_send()

    def drain(k, carry):
        q_copy(k).wait_send()
        for copy in o_copy(k):
            copy.wait_send()
        for pool in b_pools:
            b_copy(pool, k).wait_send()
        return carry

    lax.fori_loop(1, chips, drain, 0)
    out_copy.wait()


def dense(
    hidden_in,
    queries,
    decode_key_value,
    local_kv,
    page_table,
    seq_blocks,
    prompt_kv,
    prompt_owner,
    prompt_pages,
    norm_gain,
    router,
    w_gate,
    w_up,
    w_down,
    route_ids,
):
    devices = lax.axis_size("expert")
    seqs = hidden_in.shape[0]
    hidden = w_gate.shape[2]
    lines = devices // 4
    chips = devices // 2
    bf16, f32 = jnp.bfloat16, jnp.float32
    chunks = 4
    b_chunks = 2
    packed = D * MAXP // seqs
    loaded = (
        prompt_kv[0],
        queries,
        decode_key_value,
        page_table,
        local_kv,
        hidden_in,
        norm_gain[None, :],
        router.T,
        route_ids,
    )
    smem = pl.BlockSpec(memory_space=pltpu.SMEM)
    hbm = pl.BlockSpec(memory_space=pltpu.HBM)
    dma = pltpu.SemaphoreType.DMA
    return pl.pallas_call(
        functools.partial(layer_kernel, devices),
        out_shape=jax.ShapeDtypeStruct((seqs, D), bf16),
        in_specs=[smem] * 3 + [hbm] * (len(loaded) + 3),
        out_specs=hbm,
        scratch_shapes=[pltpu.VMEM(a.shape, a.dtype) for a in loaded]
        + [
            pltpu.VMEM((D, 2 * hidden), bf16),
            pltpu.VMEM((hidden, D), bf16),
            pltpu.VMEM(loaded[0].shape, bf16),
            pltpu.VMEM((seqs, packed), bf16),
            pltpu.VMEM((chips, seqs, packed), bf16),
            pltpu.VMEM((chips, seqs, packed), bf16),
            pltpu.VMEM((chips, seqs, packed), bf16),
            pltpu.VMEM((chips, seqs, 128), f32),
            pltpu.VMEM((chips, seqs, 128), f32),
            pltpu.VMEM((seqs, D), f32),
            pltpu.VMEM((devices, seqs, D), bf16),
            pltpu.VMEM((devices, seqs, 128), f32),
            pltpu.VMEM((devices, seqs, D), bf16),
            pltpu.VMEM((devices, seqs, 128), f32),
            pltpu.VMEM((2, 2, lines, seqs, D), bf16),
            pltpu.VMEM((2, lines, seqs, D), bf16),
            pltpu.VMEM((lines, seqs, D), bf16),
            pltpu.VMEM((lines, seqs, D), bf16),
            pltpu.VMEM((lines, seqs, D), bf16),
            pltpu.VMEM((lines, seqs, D), bf16),
            pltpu.VMEM((seqs, D), f32),
            pltpu.VMEM((2, chips, seqs, D), bf16),
            pltpu.VMEM((chips, seqs, D), bf16),
            pltpu.VMEM((chips, seqs, D), bf16),
            pltpu.VMEM((chips, seqs, D), bf16),
            pltpu.VMEM((seqs, D), bf16),
            dma((len(loaded),)),
            dma((3,)),
            dma((2,)),
            dma((2, chips)),
            dma((2, chips)),
            dma((2, chips)),
            dma((2, 4 * lines)),
            dma((2, devices)),
            dma((2, 2, chips)),
            dma((2, 2, chips)),
            dma((2, chunks)),
            dma((2, chunks)),
            dma((lines, chunks)),
            dma((lines, chunks)),
            dma((2, b_chunks)),
            dma((2, chips)),
            dma(()),
        ],
        compiler_params=pltpu.CompilerParams(
            collective_id=0, has_side_effects=True, vmem_limit_bytes=67043328
        ),
    )(prompt_owner, prompt_pages, seq_blocks, *loaded, w_gate, w_up, w_down)


def local(*arrays):
    devices = lax.axis_size("expert")
    experts = arrays[10].shape[1]
    if experts == TOPK and devices == 2 * experts and devices % 4 == 0:
        return dense(*arrays)
    return routed(*arrays)


def solution(mesh):
    return jax.shard_map(
        local,
        mesh=mesh,
        in_specs=(
            P(("groups", "expert"), None),
            P(("groups", "expert"), None),
            P(("groups", "expert"), None, None),
            P(("groups", "expert"), None, None, None),
            P(("groups", "expert"), None),
            P(("groups", "expert")),
            P(("groups", "expert"), None, None, None, None),
            P("groups"),
            P("groups"),
            P(),
            P(),
            P("expert", None, None),
            P("expert", None, None),
            P("expert", None, None),
            P(("groups", "expert"), None),
        ),
        out_specs=P(("groups", "expert"), None),
        check_vma=False,
    )
```

```python
import functools
import math

import jax
import jax.numpy as jnp
from jax import lax
from jax.experimental import pallas as pl
from jax.experimental.pallas import tpu as pltpu
from jax.sharding import PartitionSpec as P

D = 4096
QUERY_HEADS = 32
KEY_VALUE_HEADS = 2
HEAD_SIZE = 128
PAGE_TOKENS = 16
TOPK = 8
MAXB = 16
MAXP = 2


norm_eps = 1e-06
masked_score = -1e30


def partner(x, axis, apart):
    return lax.ppermute(x, axis, [(i, i ^ 1 << apart) for i in range(lax.axis_size(axis))])


def attend(rows_of_queries, rows_of_keys, rows_of_values, allowed, token_own_key, token_own_value):
    decode_tokens = rows_of_queries.shape[0]
    heads_of_queries = rows_of_queries.reshape(
        decode_tokens, KEY_VALUE_HEADS, QUERY_HEADS // KEY_VALUE_HEADS, HEAD_SIZE
    )
    heads_of_keys = rows_of_keys.reshape(decode_tokens, -1, KEY_VALUE_HEADS, HEAD_SIZE)
    heads_of_values = rows_of_values.reshape(decode_tokens, -1, KEY_VALUE_HEADS, HEAD_SIZE)
    scale_for_scores = 1.0 / math.sqrt(HEAD_SIZE)
    allowed_mask = allowed[:, None, None, :]
    scores = (
        jnp.einsum(
            "tkgd,tlkd->tkgl", heads_of_queries, heads_of_keys, preferred_element_type=jnp.float32
        )
        * scale_for_scores
    )
    scores = jnp.where(allowed_mask, scores, masked_score)
    token_own_score = (
        jnp.einsum(
            "xejp,xep->xej",
            heads_of_queries,
            token_own_key.reshape(decode_tokens, KEY_VALUE_HEADS, HEAD_SIZE),
            preferred_element_type=jnp.float32,
        )
        * scale_for_scores
    )
    peak = jnp.maximum(jnp.max(scores, -1), token_own_score)
    weights = jnp.where(allowed_mask, jnp.exp(scores - peak[..., None]), 0.0)
    own_weight = jnp.exp(token_own_score - peak)
    denominator = jnp.sum(weights, -1) + own_weight
    probs = (weights / denominator[..., None]).astype(jnp.bfloat16)
    token_own_probability = (own_weight / denominator).astype(jnp.bfloat16)
    blended_noise = jnp.einsum(
        "tkgl,tlkd->tkgd", probs, heads_of_values, preferred_element_type=jnp.float32
    )
    blended_noise = blended_noise + token_own_probability.astype(jnp.float32)[
        ..., None
    ] * token_own_value.reshape(decode_tokens, KEY_VALUE_HEADS, 1, HEAD_SIZE).astype(jnp.float32)
    return blended_noise.reshape(decode_tokens, QUERY_HEADS * HEAD_SIZE).astype(jnp.bfloat16)


def routed(
    hidden_in,
    queries,
    decode_key_value,
    local_kv,
    page_table,
    seq_blocks,
    prompt_kv,
    prompt_owner,
    prompt_pages,
    norm_gain,
    router,
    w_gate,
    w_up,
    w_down,
    route_ids,
):
    devices = lax.axis_size("expert")
    position = lax.axis_index("expert")
    experts = devices // 2
    seq_dev = hidden_in.shape[0]
    key_value_width = KEY_VALUE_HEADS * HEAD_SIZE
    capacity = min(seq_dev, max(2, 2 * ((3 * seq_dev * TOPK + 2 * devices - 1) // (2 * devices))))
    half_cap = capacity // 2
    even_core = position % 2 == 0
    prompt_count = prompt_owner.shape[0]
    prompt_range = jnp.arange(prompt_count, dtype=jnp.int32)
    same_owner = prompt_owner[:, None] == prompt_owner[None, :]
    earlier = prompt_range[None, :] < prompt_range[:, None]
    arrival = jnp.sum((same_owner & earlier).astype(jnp.int32), 1)
    matching = (
        prompt_owner[None, None, :] == jnp.arange(devices, dtype=jnp.int32)[:, None, None]
    ) & (arrival[None, None, :] == jnp.arange(MAXP, dtype=jnp.int32)[None, :, None])
    chosen_prompt = jnp.sum(jnp.where(matching, prompt_range[None, None, :], 0), -1)
    occupied = jnp.any(matching, -1)
    own_picks = lax.dynamic_index_in_dim(chosen_prompt, position, 0, keepdims=False)
    own_occupied = lax.dynamic_index_in_dim(occupied, position, 0, keepdims=False)
    page_rows = prompt_kv[0]
    outgoing = jnp.take(page_rows, chosen_prompt.T.reshape(-1), axis=0).reshape(
        MAXP, devices, 2, PAGE_TOKENS, key_value_width
    )
    outgoing = jnp.where(occupied.T[:, :, None, None, None], outgoing, 0)
    arrived = lax.all_to_all(outgoing, "expert", split_axis=1, concat_axis=1, tiled=True)
    lengths = jnp.take(prompt_pages, own_picks)
    new_keys = arrived[:, :, 0].reshape(MAXP, devices * PAGE_TOKENS, key_value_width)
    new_values = arrived[:, :, 1].reshape(MAXP, devices * PAGE_TOKENS, key_value_width)
    new_allowed = (jnp.arange(devices * PAGE_TOKENS, dtype=jnp.int32) // PAGE_TOKENS)[
        None, :
    ] < lengths[:, None]
    fresh_rows = attend(
        queries[:MAXP],
        new_keys,
        new_values,
        new_allowed,
        decode_key_value[:MAXP, 0],
        decode_key_value[:MAXP, 1],
    )
    fetched = local_kv[page_table]
    old_keys = fetched[:, :, 0].reshape(seq_dev, MAXB * PAGE_TOKENS, key_value_width)
    old_values = fetched[:, :, 1].reshape(seq_dev, MAXB * PAGE_TOKENS, key_value_width)
    old_allowed = (jnp.arange(MAXB * PAGE_TOKENS, dtype=jnp.int32) // PAGE_TOKENS)[
        None, :
    ] < seq_blocks[:, None]
    old_out = attend(
        queries, old_keys, old_values, old_allowed, decode_key_value[:, 0], decode_key_value[:, 1]
    )
    new_count = jnp.sum(own_occupied.astype(jnp.int32))
    is_new = jnp.arange(MAXP, dtype=jnp.int32) < new_count
    attention = jnp.concatenate(
        [jnp.where(is_new[:, None], fresh_rows, old_out[:MAXP]), old_out[MAXP:]], 0
    )
    residual = (hidden_in.astype(jnp.float32) + attention.astype(jnp.float32)).astype(jnp.bfloat16)
    resid_wide = residual.astype(jnp.float32)
    normed = (
        resid_wide
        * lax.rsqrt(jnp.mean(resid_wide * resid_wide, -1, keepdims=True) + norm_eps)
        * norm_gain
    ).astype(jnp.bfloat16)
    logits = jnp.dot(normed, router, preferred_element_type=jnp.float32)
    expert_onehot = route_ids[:, :, None] == jnp.arange(experts, dtype=jnp.int32)[None, None, :]
    selected = jnp.sum(jnp.where(expert_onehot, logits[:, None, :], 0.0), -1)
    gate_weights = jax.nn.softmax(selected, -1)
    assigned = seq_dev * TOPK
    expert_ids = route_ids.reshape(assigned)
    chosen = (expert_ids[:, None] == jnp.arange(experts, dtype=jnp.int32)[None, :]).astype(
        jnp.int32
    )
    before = jnp.cumsum(chosen, 0) - chosen
    slot_rank = jnp.sum(before * chosen, 1)
    slot_index = expert_ids * capacity + slot_rank
    placing = slot_index[None, :] == jnp.arange(experts * capacity, dtype=jnp.int32)[:, None]
    selector = jnp.any(placing.reshape(experts * capacity, seq_dev, TOPK), -1).astype(jnp.bfloat16)
    gathered_rows = jnp.dot(selector, normed, preferred_element_type=jnp.float32).astype(
        jnp.bfloat16
    )
    outgoing_half = gathered_rows.reshape(devices, half_cap, D)
    own_half = lax.all_to_all(outgoing_half, "expert", split_axis=0, concat_axis=0, tiled=True)
    partner_half = partner(own_half, "expert", 0)
    received = jnp.where(
        even_core,
        jnp.concatenate([own_half, partner_half], 1),
        jnp.concatenate([partner_half, own_half], 1),
    )
    flattened = received.reshape(devices * capacity, D)
    gate_proj = jnp.dot(flattened, w_gate[0], preferred_element_type=jnp.float32)
    up_proj = jnp.dot(flattened, w_up[0], preferred_element_type=jnp.float32)
    activated = (jax.nn.silu(gate_proj) * up_proj).astype(jnp.bfloat16)
    partial_value = jnp.dot(activated, w_down[0], preferred_element_type=jnp.float32).reshape(
        devices, capacity, D
    )
    kept = jnp.where(even_core, partial_value[:, :half_cap], partial_value[:, half_cap:])
    handed = jnp.where(even_core, partial_value[:, half_cap:], partial_value[:, :half_cap])
    partner_part = partner(handed, "expert", 0)
    finished = (kept + partner_part).astype(jnp.bfloat16)
    returned = lax.all_to_all(finished, "expert", split_axis=0, concat_axis=0, tiled=True)
    expert_sum = returned.reshape(experts * capacity, D)
    picked = jnp.take(expert_sum, slot_index, axis=0).astype(jnp.float32).reshape(seq_dev, TOPK, D)
    expert_mix = jnp.sum(picked * gate_weights[:, :, None], 1)
    return (resid_wide + expert_mix).astype(jnp.bfloat16)


def layer_kernel(
    devices,
    owners_hbm,
    lengths_hbm,
    blocks_hbm,
    pages_hbm,
    q_hbm,
    dkv_hbm,
    table_hbm,
    kv_hbm,
    hidden_hbm,
    gain_hbm,
    router_hbm,
    ids_hbm,
    gate_hbm,
    up_hbm,
    down_hbm,
    out_ref,
    owners,
    prompt_lengths,
    blocks,
    pages_ref,
    q_ref,
    dkv_ref,
    table_ref,
    kv_ref,
    hidden_ref,
    gain_ref,
    router_ref,
    ids_ref,
    w_in,
    w_down,
    other_pages,
    q_send,
    q_recv,
    o_send,
    o_recv,
    lse_send,
    lse_recv,
    attn,
    x_a,
    gates_a,
    x_b,
    gates_b,
    part_a,
    core_a,
    y_send,
    y_recv,
    z_send,
    z_recv,
    kept,
    part_b,
    core_b,
    sum_b,
    recv_b,
    in_sem,
    w_sem,
    page_sem,
    q_sem,
    o_sem,
    lse_sem,
    xa_ssem,
    xa_rsem,
    xb_ssem,
    xb_rsem,
    c_ssem,
    c_rsem,
    y_ssem,
    y_rsem,
    z_sem,
    cb_ssem,
    cb_rsem,
    rb_sem,
):
    f32, bf16 = jnp.float32, jnp.bfloat16
    me = lax.axis_index("expert")
    lines = devices // 4
    chips = devices // 2
    core, row, line = lax.rem(me, 2), lax.rem(me // 2, 2), me // 4
    unit = row * lines + line
    seqs = hidden_ref.shape[0]
    group = QUERY_HEADS // KEY_VALUE_HEADS
    scale = 1.0 / math.sqrt(HEAD_SIZE)
    old_rows = pl.ds(MAXP, seqs - MAXP)
    new_rows = pl.ds(0, MAXP)

    def device(at_line, at_row, at_core):
        return (at_line * 2 + at_row) * 2 + at_core

    def device_of(at_unit, at_core):
        return device(lax.rem(at_unit, lines), at_unit // lines, at_core)

    def place(at_line, at_row, at_core):
        return (at_core * 2 + at_row) * lines + at_line

    low = line * 2 < lines

    def far_line(j):
        return jnp.where(low, lines - 1 - j, j)

    def far_other_line(j):
        down = lines - 1 - j
        return jnp.where(
            low, jnp.where(down > line, down, down - 1), jnp.where(j < line, j, j + 1)
        )

    def other_units():
        for j in range(lines):
            yield (1 - row) * lines + far_line(j)
            if j < lines - 1:
                yield row * lines + far_other_line(j)

    def remote(src, dst, ssem, rsem, to):
        return pltpu.make_async_remote_copy(
            src_ref=src,
            dst_ref=dst,
            send_sem=ssem,
            recv_sem=rsem,
            device_id={"expert": to},
            device_id_type=pl.DeviceIdType.MESH,
        )

    other_row = device(line, 1 - row, core)
    other_core = device(line, row, 1 - core)
    mine = place(line, row, core)

    loads = [
        pltpu.make_async_copy(a, b, in_sem.at[i])
        for i, (a, b) in enumerate(
            (
                (q_hbm, q_ref),
                (pages_hbm, pages_ref),
                (dkv_hbm, dkv_ref),
                (table_hbm, table_ref),
                (kv_hbm, kv_ref),
                (hidden_hbm, hidden_ref),
                (gain_hbm, gain_ref),
                (router_hbm, router_ref),
                (ids_hbm, ids_ref),
                (blocks_hbm, blocks),
                (owners_hbm, owners),
                (lengths_hbm, prompt_lengths),
            )
        )
    ]
    hidden = w_down.shape[0]
    weights = [
        pltpu.make_async_copy(gate_hbm.at[0], w_in.at[:, pl.ds(0, hidden)], w_sem.at[0]),
        pltpu.make_async_copy(up_hbm.at[0], w_in.at[:, pl.ds(hidden, hidden)], w_sem.at[1]),
        pltpu.make_async_copy(down_hbm.at[0], w_down, w_sem.at[2]),
    ]
    barrier = pltpu.get_barrier_semaphore()

    def greet(k, carry):
        pl.semaphore_signal(
            barrier,
            inc=1,
            device_id={"expert": lax.rem(me + k, devices)},
            device_id_type=pl.DeviceIdType.MESH,
        )
        return carry

    lax.fori_loop(1, devices, greet, 0)
    for copy in loads + weights:
        copy.start()

    fold = seqs // MAXP
    lane_heads = QUERY_HEADS // fold
    packed = lane_heads * HEAD_SIZE
    per_kv = lane_heads // KEY_VALUE_HEADS
    sub = lax.broadcasted_iota(jnp.int32, (seqs, packed), 0) // MAXP

    def head_cols(h):
        return slice(h * HEAD_SIZE, (h + 1) * HEAD_SIZE)

    def turn(x, by):
        by = by % seqs
        return x if by == 0 else pltpu.roll(x, by, 0)

    def pack(rows):
        out = None
        for f in range(fold):
            wide = turn(
                jnp.concatenate([rows[:, head_cols(fold * hh + f)] for hh in range(lane_heads)], 1),
                MAXP * f,
            )
            out = wide if f == 0 else jnp.where(sub == f, wide, out)
        return out

    def spread_rows(rows):
        out = rows
        at = lax.broadcasted_iota(jnp.int32, rows.shape, 0) // MAXP
        for f in range(1, fold):
            out = jnp.where(at == f, turn(rows, MAXP * f), out)
        return out

    def dot_t(a, b):
        return lax.dot_general(a, b, (((1,), (1,)), ((), ())), preferred_element_type=f32)

    loads[0].wait()
    q_packed = pack(q_ref[...].astype(f32))
    q_send[...] = q_packed.astype(bf16)
    pl.semaphore_wait(barrier, devices - 1)

    def q_copy(to):
        return remote(q_send, q_recv.at[unit], q_sem.at[0], q_sem.at[1], device_of(to, core))

    for to in other_units():
        q_copy(to).start()
    q_recv[unit] = q_packed.astype(bf16)
    loads[1].wait()
    page_copy = remote(pages_ref, other_pages, page_sem.at[0], page_sem.at[1], other_core)
    page_copy.start()

    for copy in loads[2:]:
        copy.wait()

    def per_seq(values, shape):
        at = lax.broadcasted_iota(jnp.int32, shape, 0)
        return sum(jnp.where(at == s, v, 0) for s, v in enumerate(values))

    tokens = kv_ref.shape[0] * PAGE_TOKENS
    limit = per_seq([blocks[s] for s in range(seqs)], (seqs, tokens))
    page_of = lax.broadcasted_iota(jnp.int32, (seqs, tokens), 1) // PAGE_TOKENS
    held = jnp.zeros((seqs, tokens), f32)
    for b in range(table_ref.shape[1]):
        hit = (page_of == table_ref[:, b : b + 1]) & (limit > b)
        held = held + jnp.where(hit, 1.0, 0.0)
    held = jnp.concatenate([held] * group, 0)

    def heads(h):
        rows = q_ref[...].astype(f32)
        return jnp.concatenate([rows[:, head_cols(h * group + g)] for g in range(group)], 0)

    def own(h, at):
        both = dkv_ref[...].astype(f32)
        return jnp.concatenate([both[:, at, head_cols(h)]] * group, 0)

    def weigh(scores, times, own_score):
        scores = jnp.where(times > 0, scores, masked_score)
        peak = jnp.maximum(jnp.max(scores, -1, keepdims=True), own_score)
        weight = times * jnp.exp(scores - peak)
        own_weight = jnp.exp(own_score - peak)
        total = jnp.sum(weight, -1, keepdims=True) + own_weight
        return (weight / total).astype(bf16), (own_weight / total).astype(bf16).astype(f32)

    for h in range(KEY_VALUE_HEADS):
        at = head_cols(h)
        queries = heads(h)
        own_score = jnp.sum(queries * own(h, 0), -1, keepdims=True) * scale
        keys = kv_ref[:, 0, :, at].reshape(tokens, HEAD_SIZE)
        values = kv_ref[:, 1, :, at].reshape(tokens, HEAD_SIZE)
        probs, own_prob = weigh(dot_t(queries.astype(bf16), keys) * scale, held, own_score)
        mixed = jnp.dot(probs, values, preferred_element_type=f32) + own_prob * own(h, 1)
        for g in range(group):
            attn[:, head_cols(h * group + g)] = mixed[g * seqs : (g + 1) * seqs]

    def residual_of(attention):
        rounded = attention.astype(bf16).astype(f32)
        return (hidden_ref[...].astype(f32) + rounded).astype(bf16).astype(f32)

    def norm_of(wide):
        mean = jnp.mean(wide * wide, -1, keepdims=True)
        return (wide * lax.rsqrt(mean + norm_eps) * gain_ref[...]).astype(bf16)

    def gate_of(normed):
        logits = dot_t(normed, router_ref[...])
        experts = logits.shape[1]
        expert_of = lax.broadcasted_iota(jnp.int32, (seqs, experts), 1)
        times = jnp.zeros((seqs, experts), f32)
        for k in range(ids_ref.shape[1]):
            times = times + jnp.where(ids_ref[:, k : k + 1] == expert_of, 1.0, 0.0)
        picked = jnp.where(times > 0, logits, masked_score)
        gate = times * jnp.exp(picked - jnp.max(picked, -1, keepdims=True))
        gate = gate / jnp.sum(gate, -1, keepdims=True)
        return jnp.concatenate([gate] * (128 // experts), 1)

    normed = norm_of(residual_of(attn[...]))
    x_a[mine] = normed

    def pass_on(pool, spot, count, at, to):
        buffer, rows, n = pool
        ref = buffer.at[pl.ds(spot, count), rows]
        return remote(ref, ref, xa_ssem.at[n], xa_rsem.at[n, at], to)

    at_y, at_core = lines - 1, (lines, lines + 1)
    row_spots = [(core * 2 + at_row) * lines for at_row in (row, 1 - row)]

    def z_copy(pool, k):
        return pass_on(pool, mine, 1, k - 1, device(lax.rem(line + k, lines), row, core))

    def z_arrive(pool, k):
        spot = place(lax.rem(line + lines - k, lines), row, core)
        pass_on(pool, spot, 1, k - 1, other_row).wait_recv()
        pass_on(pool, spot, 1, at_y, other_row).start()

    def over_core(pool, n):
        pass_on(pool, row_spots[n], lines, at_core[n], other_core).start()

    def first_hops(pool):
        for k in range(1, lines):
            z_copy(pool, k).start()
        pass_on(pool, mine, 1, at_y, other_row).start()

    pools = [(x_a, old_rows, 0), (gates_a, pl.ds(0, seqs), 1)]
    first_hops(pools[0])
    gates_a[mine] = gate_of(normed)
    first_hops(pools[1])

    prompts = owners.shape[0]
    shape = (1, prompts * PAGE_TOKENS)
    prompt_of = lax.broadcasted_iota(jnp.int32, shape, 1) // PAGE_TOKENS
    owner_of, length_of = jnp.zeros(shape, jnp.int32), jnp.zeros(shape, jnp.int32)
    for p in range(prompts):
        owner_of = jnp.where(prompt_of == p, owners[p], owner_of)
        length_of = jnp.where(prompt_of == p, prompt_lengths[p], length_of)
    rank_of = jnp.zeros(shape, jnp.int32)
    for p in range(prompts):
        rank_of = rank_of + jnp.where((owner_of == owners[p]) & (prompt_of > p), 1, 0)
    slots = chips * seqs
    at_row = lax.broadcasted_iota(jnp.int32, (slots, 1), 0)
    row_unit = at_row // seqs
    row_owner = device_of(row_unit, core)
    match = (owner_of == row_owner) & (rank_of == lax.rem(at_row, MAXP))

    def allowed_at(position):
        ok = match & (length_of > position)
        return jnp.concatenate([jnp.where(ok, 1.0, 0.0)] * per_kv, 0)

    allowed = (allowed_at(me), allowed_at(other_core))
    page_copy.wait_recv()

    few = pl.ds(0, chips - 1)
    q_all = remote(q_recv.at[few], q_recv.at[few], q_sem.at[0], q_sem.at[1], other_core)
    q_all.wait_recv()
    lane_of = lax.broadcasted_iota(jnp.int32, (slots, 128), 1)
    lse_all = jnp.zeros((slots, 128), f32)
    for h in range(KEY_VALUE_HEADS):
        at = head_cols(h)
        lanes = [h * per_kv + j for j in range(per_kv)]
        queries = jnp.concatenate(
            [q_recv[:, :, head_cols(hh)].reshape(slots, HEAD_SIZE) for hh in lanes], 0
        )
        scores = []
        for ref, ok in zip((pages_ref, other_pages), allowed):
            keys = ref[:, 0, :, at].reshape(prompts * PAGE_TOKENS, HEAD_SIZE)
            scores.append(jnp.where(ok > 0, dot_t(queries, keys) * scale, masked_score))
        peak = jnp.maximum(
            jnp.max(scores[0], -1, keepdims=True), jnp.max(scores[1], -1, keepdims=True)
        )
        total = jnp.zeros((slots * per_kv, 1), f32)
        mixed = jnp.zeros((slots * per_kv, HEAD_SIZE), f32)
        for ref, ok, score in zip((pages_ref, other_pages), allowed, scores):
            weight = ok * jnp.exp(score - peak)
            total = total + jnp.sum(weight, -1, keepdims=True)
            values = ref[:, 1, :, at].reshape(prompts * PAGE_TOKENS, HEAD_SIZE)
            mixed = mixed + jnp.dot(weight.astype(bf16), values, preferred_element_type=f32)
        some = total > 0
        safe = jnp.where(some, total, 1.0)
        mixed = mixed / safe
        lse = jnp.where(some, peak + jnp.log(safe), masked_score)
        for j, hh in enumerate(lanes):
            rows = slice(j * slots, (j + 1) * slots)
            o_send[:, :, head_cols(hh)] = mixed[rows].astype(bf16).reshape(chips, seqs, HEAD_SIZE)
            lse_all = jnp.where(lane_of == hh, lse[rows], lse_all)
    lse_send[...] = lse_all.reshape(chips, seqs, 128)

    def o_copy(to):
        at = device_of(to, core)
        return (
            remote(o_send.at[to], o_recv.at[unit], o_sem.at[0], o_sem.at[1], at),
            remote(lse_send.at[to], lse_recv.at[unit], lse_sem.at[0], lse_sem.at[1], at),
        )

    for to in other_units():
        for copy in o_copy(to):
            copy.start()
    o_recv[unit] = o_send[unit]
    lse_recv[unit] = lse_send[unit]

    for k in range(1, lines):
        for pool in pools:
            z_arrive(pool, k)
    for pool in pools:
        over_core(pool, 0)

    own_both = dkv_ref[...].astype(f32)
    own_key = spread_rows(own_both[:, 0])
    own_value = spread_rows(own_both[:, 1])
    lane = lax.broadcasted_iota(jnp.int32, (seqs, 128), 1)
    own_score = jnp.zeros((seqs, 128), f32)
    for hh in range(lane_heads):
        score = jnp.sum(
            q_packed[:, head_cols(hh)] * own_key[:, head_cols(hh // per_kv)], -1, keepdims=True
        )
        own_score = jnp.where(lane == hh, score * scale, own_score)
    new_count = jnp.int32(0)
    for p in range(prompts):
        new_count = new_count + (owners[p] == me).astype(jnp.int32)
    is_new = lax.broadcasted_iota(jnp.int32, (seqs, HEAD_SIZE), 0) < new_count

    o_all = (
        remote(o_recv.at[few], o_recv.at[few], o_sem.at[0], o_sem.at[1], other_core),
        remote(lse_recv.at[few], lse_recv.at[few], lse_sem.at[0], lse_sem.at[1], other_core),
    )
    for copy in o_all:
        copy.wait_recv()
    peak = own_score
    for u in range(chips):
        peak = jnp.maximum(peak, lse_recv[u])
    shares = [jnp.exp(lse_recv[u] - peak) for u in range(chips)]
    own_share = jnp.exp(own_score - peak)
    total = own_share
    for share in shares:
        total = total + share
    inverse = 1.0 / total
    shares = [share * inverse for share in shares]
    own_share = own_share * inverse
    for hh in range(lane_heads):
        at = head_cols(hh)
        mixed = own_share[:, hh : hh + 1] * own_value[:, head_cols(hh // per_kv)]
        for u in range(chips):
            mixed = mixed + shares[u][:, hh : hh + 1] * o_recv[u, :, at].astype(f32)
        for f in range(fold):
            cols = head_cols(fold * hh + f)
            attn[:, cols] = jnp.where(is_new, turn(mixed, -MAXP * f), attn[:, cols])
    wide = residual_of(attn[...])
    attn[...] = wide
    normed = norm_of(wide)
    x_b[mine] = normed

    b_pools = [(x_b, new_rows, 0), (gates_b, pl.ds(0, seqs), 1)]

    def b_copy(pool, to):
        buffer, rows, n = pool
        ref = buffer.at[mine, rows]
        return remote(ref, ref, xb_ssem.at[n], xb_rsem.at[n, 0], device_of(to, core))

    def b_spots(pool, count, at):
        buffer, rows, n = pool
        ref = buffer.at[pl.ds(core * chips, count), rows]
        return remote(ref, ref, xb_ssem.at[n], xb_rsem.at[n, at], other_core)

    def b_first(pool):
        for to in other_units():
            b_copy(pool, to).start()

    b_first(b_pools[0])
    gates_b[mine] = gate_of(normed)
    b_first(b_pools[1])

    for pool in pools:
        pass_on(pool, row_spots[1], lines, at_y, other_row).wait_recv()
        over_core(pool, 1)
    for pool in pools:
        for n in range(2):
            pass_on(pool, row_spots[n], lines, at_core[n], other_core).wait_recv()
    for copy in weights:
        copy.wait()
    total = devices * seqs
    lanes_of = lax.broadcasted_iota(jnp.int32, (total, 128), 1)

    def activate(x_ref, gates_ref):
        both = jnp.dot(x_ref[...].reshape(total, D), w_in[...], preferred_element_type=f32)
        gate_proj, up_proj = both[:, :hidden], both[:, hidden:]
        scaled = jnp.sum(
            jnp.where(lanes_of == me // 2, gates_ref[...].reshape(total, 128), 0.0),
            -1,
            keepdims=True,
        )
        return (gate_proj / (1.0 + jnp.exp(-gate_proj)) * up_proj * scaled).astype(bf16)

    chunks = c_rsem.shape[0]
    width = D // chunks

    def cut(i):
        return slice(i * width, (i + 1) * width)

    def core_copy(i):
        return remote(
            part_a.at[1 - core, :, :, old_rows, cut(i)],
            core_a.at[:, :, old_rows, cut(i)],
            c_ssem,
            c_rsem.at[i],
            other_core,
        )

    def row_copy(i):
        return remote(
            y_send.at[:, old_rows, cut(i)],
            y_recv.at[:, old_rows, cut(i)],
            y_ssem,
            y_rsem.at[i],
            other_row,
        )

    def line_copy(i, k):
        to = lax.rem(line + k, lines)
        return remote(
            z_send.at[k, old_rows, cut(i)],
            z_recv.at[k, old_rows, cut(i)],
            z_sem.at[0],
            z_sem.at[1],
            device(to, row, core),
        )

    activated = activate(x_a, gates_a)
    for i in range(chunks):
        rows = jnp.dot(activated, w_down[:, cut(i)], preferred_element_type=f32)
        part_a[:, :, :, :, cut(i)] = rows.astype(bf16).reshape(2, 2, lines, seqs, width)
        core_copy(i).start()

    for pool in b_pools:
        b_spots(pool, chips - 1, 0).wait_recv()
        b_spots(pool, chips, 1).start()

    for i in range(chunks):
        core_copy(i).wait_recv()
        y_send[:, :, cut(i)] = (
            part_a[core, 1 - row, :, :, cut(i)].astype(f32)
            + core_a[1 - row, :, :, cut(i)].astype(f32)
        ).astype(bf16)
        row_copy(i).start()

    for pool in b_pools:
        b_spots(pool, chips, 1).wait_recv()
    activated = activate(x_b, gates_b)
    b_chunks = cb_rsem.shape[0]
    b_width = D // b_chunks

    def b_core(i):
        at = slice(i * b_width, (i + 1) * b_width)
        return remote(
            part_b.at[1 - core, :, new_rows, at],
            core_b.at[:, new_rows, at],
            cb_ssem,
            cb_rsem.at[i],
            other_core,
        )

    for i in range(b_chunks):
        at = slice(i * b_width, (i + 1) * b_width)
        rows = jnp.dot(activated, w_down[:, at], preferred_element_type=f32)
        part_b[:, :, :, at] = rows.astype(bf16).reshape(2, chips, seqs, b_width)
        b_core(i).start()

    def b_return(to):
        return remote(
            sum_b.at[to, new_rows],
            recv_b.at[unit, new_rows],
            rb_sem.at[0],
            rb_sem.at[1],
            device_of(to, core),
        )

    for i in range(chunks):
        row_copy(i).wait_recv()

        def summed(at_line):
            return (
                part_a[core, row, at_line, :, cut(i)].astype(f32)
                + core_a[row, at_line, :, cut(i)].astype(f32)
                + y_recv[at_line, :, cut(i)].astype(f32)
            )

        for k in range(1, lines):
            z_send[k, :, cut(i)] = summed(lax.rem(line + k, lines)).astype(bf16)
            line_copy(i, k).start()
        kept[:, cut(i)] = attn[:, cut(i)] + summed(line)

    for i in range(b_chunks):
        b_core(i).wait_recv()
    for to in other_units():
        sum_b[to] = (part_b[core, to].astype(f32) + core_b[to].astype(f32)).astype(bf16)
        b_return(to).start()
    last = attn[...] + part_b[core, unit].astype(f32) + core_b[unit].astype(f32)

    rest = pl.ds(1, lines - 1)
    z_all = remote(
        z_recv.at[rest, old_rows], z_recv.at[rest, old_rows], z_sem.at[0], z_sem.at[1], other_core
    )
    z_all.wait_recv()
    answer = kept[...]
    for k in range(1, lines):
        answer = answer + z_recv[k].astype(f32)

    b_all = remote(
        recv_b.at[few, new_rows], recv_b.at[few, new_rows], rb_sem.at[0], rb_sem.at[1], other_core
    )
    b_all.wait_recv()
    for k in range(1, chips):
        last = last + recv_b[lax.rem(unit + k, chips)].astype(f32)
    is_b = lax.broadcasted_iota(jnp.int32, (seqs, D), 0) < MAXP
    out_ref[...] = jnp.where(is_b, last, answer).astype(bf16)

    for copy in (page_copy, q_all, z_all, b_all) + o_all:
        copy.wait_send()
    for n, (buffer, rows) in enumerate(((x_a, old_rows), (gates_a, pl.ds(0, seqs)))):
        ref = buffer.at[pl.ds(0, 4 * lines - 1), rows]
        remote(ref, ref, xa_ssem.at[n], xa_rsem.at[n, 0], other_core).wait_send()
    for n, (buffer, rows) in enumerate(((x_b, new_rows), (gates_b, pl.ds(0, seqs)))):
        ref = buffer.at[pl.ds(0, 2 * chips - 1), rows]
        remote(ref, ref, xb_ssem.at[n], xb_rsem.at[n, 0], other_core).wait_send()
    for ref, ssem, rsem in (
        (part_a.at[0, :, :, old_rows], c_ssem, c_rsem.at[0]),
        (y_send.at[:, old_rows], y_ssem, y_rsem.at[0]),
        (part_b.at[0, :, new_rows], cb_ssem, cb_rsem.at[0]),
    ):
        remote(ref, ref, ssem, rsem, other_core).wait_send()


def dense(
    hidden_in,
    queries,
    decode_key_value,
    local_kv,
    page_table,
    seq_blocks,
    prompt_kv,
    prompt_owner,
    prompt_pages,
    norm_gain,
    router,
    w_gate,
    w_up,
    w_down,
    route_ids,
):
    devices = lax.axis_size("expert")
    seqs = hidden_in.shape[0]
    hidden = w_gate.shape[2]
    lines = devices // 4
    chips = devices // 2
    bf16, f32 = jnp.bfloat16, jnp.float32
    chunks = 4
    b_chunks = 2
    packed = D * MAXP // seqs
    loaded = (
        prompt_kv[0],
        queries,
        decode_key_value,
        page_table,
        local_kv,
        hidden_in,
        norm_gain[None, :],
        router.T,
        route_ids,
    )
    scalars = (prompt_owner, prompt_pages, seq_blocks)
    hbm = pl.BlockSpec(memory_space=pltpu.HBM)
    dma = pltpu.SemaphoreType.DMA
    return pl.pallas_call(
        functools.partial(layer_kernel, devices),
        out_shape=pltpu.VMEM((seqs, D), bf16),
        in_specs=[hbm] * (len(loaded) + 6),
        out_specs=pl.BlockSpec(memory_space=pltpu.VMEM),
        scratch_shapes=[pltpu.SMEM(a.shape, a.dtype) for a in scalars]
        + [pltpu.VMEM(a.shape, a.dtype) for a in loaded]
        + [
            pltpu.VMEM((D, 2 * hidden), bf16),
            pltpu.VMEM((hidden, D), bf16),
            pltpu.VMEM(loaded[0].shape, bf16),
            pltpu.VMEM((seqs, packed), bf16),
            pltpu.VMEM((chips, seqs, packed), bf16),
            pltpu.VMEM((chips, seqs, packed), bf16),
            pltpu.VMEM((chips, seqs, packed), bf16),
            pltpu.VMEM((chips, seqs, 128), f32),
            pltpu.VMEM((chips, seqs, 128), f32),
            pltpu.VMEM((seqs, D), f32),
            pltpu.VMEM((devices, seqs, D), bf16),
            pltpu.VMEM((devices, seqs, 128), f32),
            pltpu.VMEM((devices, seqs, D), bf16),
            pltpu.VMEM((devices, seqs, 128), f32),
            pltpu.VMEM((2, 2, lines, seqs, D), bf16),
            pltpu.VMEM((2, lines, seqs, D), bf16),
            pltpu.VMEM((lines, seqs, D), bf16),
            pltpu.VMEM((lines, seqs, D), bf16),
            pltpu.VMEM((lines, seqs, D), bf16),
            pltpu.VMEM((lines, seqs, D), bf16),
            pltpu.VMEM((seqs, D), f32),
            pltpu.VMEM((2, chips, seqs, D), bf16),
            pltpu.VMEM((chips, seqs, D), bf16),
            pltpu.VMEM((chips, seqs, D), bf16),
            pltpu.VMEM((chips, seqs, D), bf16),
            dma((len(loaded) + len(scalars),)),
            dma((3,)),
            dma((2,)),
            dma((2,)),
            dma((2,)),
            dma((2,)),
            dma((2,)),
            dma((2, lines + 2)),
            dma((2,)),
            dma((2, 2)),
            dma(()),
            dma((chunks,)),
            dma(()),
            dma((chunks,)),
            dma((2,)),
            dma(()),
            dma((b_chunks,)),
            dma((2,)),
        ],
        compiler_params=pltpu.CompilerParams(
            collective_id=0, has_side_effects=True, vmem_limit_bytes=58 * 2**20
        ),
    )(*scalars, *loaded, w_gate, w_up, w_down)


def local(*arrays):
    devices = lax.axis_size("expert")
    experts = arrays[10].shape[1]
    if experts == TOPK and devices == 2 * experts and devices % 4 == 0:
        return dense(*arrays)
    return routed(*arrays)


def solution(mesh):
    return jax.shard_map(
        local,
        mesh=mesh,
        in_specs=(
            P(("groups", "expert"), None),
            P(("groups", "expert"), None),
            P(("groups", "expert"), None, None),
            P(("groups", "expert"), None, None, None),
            P(("groups", "expert"), None),
            P(("groups", "expert")),
            P(("groups", "expert"), None, None, None, None),
            P("groups"),
            P("groups"),
            P(),
            P(),
            P("expert", None, None),
            P("expert", None, None),
            P("expert", None, None),
            P(("groups", "expert"), None),
        ),
        out_specs=P(("groups", "expert"), None),
        check_vma=False,
    )
```

```python
import functools
import math

import jax
import jax.numpy as jnp
from jax import lax
from jax.experimental import pallas as pl
from jax.experimental.pallas import tpu as pltpu
from jax.sharding import PartitionSpec as P

D = 4096
QUERY_HEADS = 32
KEY_VALUE_HEADS = 2
HEAD_SIZE = 128
PAGE_TOKENS = 16
TOPK = 8
MAXB = 16
MAXP = 2


norm_eps = 1e-06
masked_score = -1e30


def partner(x, axis, apart):
    return lax.ppermute(x, axis, [(i, i ^ 1 << apart) for i in range(lax.axis_size(axis))])


def attend(rows_of_queries, rows_of_keys, rows_of_values, allowed, token_own_key, token_own_value):
    decode_tokens = rows_of_queries.shape[0]
    heads_of_queries = rows_of_queries.reshape(
        decode_tokens, KEY_VALUE_HEADS, QUERY_HEADS // KEY_VALUE_HEADS, HEAD_SIZE
    )
    heads_of_keys = rows_of_keys.reshape(decode_tokens, -1, KEY_VALUE_HEADS, HEAD_SIZE)
    heads_of_values = rows_of_values.reshape(decode_tokens, -1, KEY_VALUE_HEADS, HEAD_SIZE)
    scale_for_scores = 1.0 / math.sqrt(HEAD_SIZE)
    allowed_mask = allowed[:, None, None, :]
    scores = (
        jnp.einsum(
            "tkgd,tlkd->tkgl", heads_of_queries, heads_of_keys, preferred_element_type=jnp.float32
        )
        * scale_for_scores
    )
    scores = jnp.where(allowed_mask, scores, masked_score)
    token_own_score = (
        jnp.einsum(
            "xejp,xep->xej",
            heads_of_queries,
            token_own_key.reshape(decode_tokens, KEY_VALUE_HEADS, HEAD_SIZE),
            preferred_element_type=jnp.float32,
        )
        * scale_for_scores
    )
    peak = jnp.maximum(jnp.max(scores, -1), token_own_score)
    weights = jnp.where(allowed_mask, jnp.exp(scores - peak[..., None]), 0.0)
    own_weight = jnp.exp(token_own_score - peak)
    denominator = jnp.sum(weights, -1) + own_weight
    probs = (weights / denominator[..., None]).astype(jnp.bfloat16)
    token_own_probability = (own_weight / denominator).astype(jnp.bfloat16)
    blended_noise = jnp.einsum(
        "tkgl,tlkd->tkgd", probs, heads_of_values, preferred_element_type=jnp.float32
    )
    blended_noise = blended_noise + token_own_probability.astype(jnp.float32)[
        ..., None
    ] * token_own_value.reshape(decode_tokens, KEY_VALUE_HEADS, 1, HEAD_SIZE).astype(jnp.float32)
    return blended_noise.reshape(decode_tokens, QUERY_HEADS * HEAD_SIZE).astype(jnp.bfloat16)


def routed(
    hidden_in,
    queries,
    decode_key_value,
    local_kv,
    page_table,
    seq_blocks,
    prompt_kv,
    prompt_owner,
    prompt_pages,
    norm_gain,
    router,
    w_gate,
    w_up,
    w_down,
    route_ids,
):
    devices = lax.axis_size("expert")
    position = lax.axis_index("expert")
    experts = devices // 2
    seq_dev = hidden_in.shape[0]
    key_value_width = KEY_VALUE_HEADS * HEAD_SIZE
    capacity = min(seq_dev, max(2, 2 * ((3 * seq_dev * TOPK + 2 * devices - 1) // (2 * devices))))
    half_cap = capacity // 2
    even_core = position % 2 == 0
    prompt_count = prompt_owner.shape[0]
    prompt_range = jnp.arange(prompt_count, dtype=jnp.int32)
    same_owner = prompt_owner[:, None] == prompt_owner[None, :]
    earlier = prompt_range[None, :] < prompt_range[:, None]
    arrival = jnp.sum((same_owner & earlier).astype(jnp.int32), 1)
    matching = (
        prompt_owner[None, None, :] == jnp.arange(devices, dtype=jnp.int32)[:, None, None]
    ) & (arrival[None, None, :] == jnp.arange(MAXP, dtype=jnp.int32)[None, :, None])
    chosen_prompt = jnp.sum(jnp.where(matching, prompt_range[None, None, :], 0), -1)
    occupied = jnp.any(matching, -1)
    own_picks = lax.dynamic_index_in_dim(chosen_prompt, position, 0, keepdims=False)
    own_occupied = lax.dynamic_index_in_dim(occupied, position, 0, keepdims=False)
    page_rows = prompt_kv[0]
    outgoing = jnp.take(page_rows, chosen_prompt.T.reshape(-1), axis=0).reshape(
        MAXP, devices, 2, PAGE_TOKENS, key_value_width
    )
    outgoing = jnp.where(occupied.T[:, :, None, None, None], outgoing, 0)
    arrived = lax.all_to_all(outgoing, "expert", split_axis=1, concat_axis=1, tiled=True)
    lengths = jnp.take(prompt_pages, own_picks)
    new_keys = arrived[:, :, 0].reshape(MAXP, devices * PAGE_TOKENS, key_value_width)
    new_values = arrived[:, :, 1].reshape(MAXP, devices * PAGE_TOKENS, key_value_width)
    new_allowed = (jnp.arange(devices * PAGE_TOKENS, dtype=jnp.int32) // PAGE_TOKENS)[
        None, :
    ] < lengths[:, None]
    fresh_rows = attend(
        queries[:MAXP],
        new_keys,
        new_values,
        new_allowed,
        decode_key_value[:MAXP, 0],
        decode_key_value[:MAXP, 1],
    )
    fetched = local_kv[page_table]
    old_keys = fetched[:, :, 0].reshape(seq_dev, MAXB * PAGE_TOKENS, key_value_width)
    old_values = fetched[:, :, 1].reshape(seq_dev, MAXB * PAGE_TOKENS, key_value_width)
    old_allowed = (jnp.arange(MAXB * PAGE_TOKENS, dtype=jnp.int32) // PAGE_TOKENS)[
        None, :
    ] < seq_blocks[:, None]
    old_out = attend(
        queries, old_keys, old_values, old_allowed, decode_key_value[:, 0], decode_key_value[:, 1]
    )
    new_count = jnp.sum(own_occupied.astype(jnp.int32))
    is_new = jnp.arange(MAXP, dtype=jnp.int32) < new_count
    attention = jnp.concatenate(
        [jnp.where(is_new[:, None], fresh_rows, old_out[:MAXP]), old_out[MAXP:]], 0
    )
    residual = (hidden_in.astype(jnp.float32) + attention.astype(jnp.float32)).astype(jnp.bfloat16)
    resid_wide = residual.astype(jnp.float32)
    normed = (
        resid_wide
        * lax.rsqrt(jnp.mean(resid_wide * resid_wide, -1, keepdims=True) + norm_eps)
        * norm_gain
    ).astype(jnp.bfloat16)
    logits = jnp.dot(normed, router, preferred_element_type=jnp.float32)
    expert_onehot = route_ids[:, :, None] == jnp.arange(experts, dtype=jnp.int32)[None, None, :]
    selected = jnp.sum(jnp.where(expert_onehot, logits[:, None, :], 0.0), -1)
    gate_weights = jax.nn.softmax(selected, -1)
    assigned = seq_dev * TOPK
    expert_ids = route_ids.reshape(assigned)
    chosen = (expert_ids[:, None] == jnp.arange(experts, dtype=jnp.int32)[None, :]).astype(
        jnp.int32
    )
    before = jnp.cumsum(chosen, 0) - chosen
    slot_rank = jnp.sum(before * chosen, 1)
    slot_index = expert_ids * capacity + slot_rank
    placing = slot_index[None, :] == jnp.arange(experts * capacity, dtype=jnp.int32)[:, None]
    selector = jnp.any(placing.reshape(experts * capacity, seq_dev, TOPK), -1).astype(jnp.bfloat16)
    gathered_rows = jnp.dot(selector, normed, preferred_element_type=jnp.float32).astype(
        jnp.bfloat16
    )
    outgoing_half = gathered_rows.reshape(devices, half_cap, D)
    own_half = lax.all_to_all(outgoing_half, "expert", split_axis=0, concat_axis=0, tiled=True)
    partner_half = partner(own_half, "expert", 0)
    received = jnp.where(
        even_core,
        jnp.concatenate([own_half, partner_half], 1),
        jnp.concatenate([partner_half, own_half], 1),
    )
    flattened = received.reshape(devices * capacity, D)
    gate_proj = jnp.dot(flattened, w_gate[0], preferred_element_type=jnp.float32)
    up_proj = jnp.dot(flattened, w_up[0], preferred_element_type=jnp.float32)
    activated = (jax.nn.silu(gate_proj) * up_proj).astype(jnp.bfloat16)
    partial_value = jnp.dot(activated, w_down[0], preferred_element_type=jnp.float32).reshape(
        devices, capacity, D
    )
    kept = jnp.where(even_core, partial_value[:, :half_cap], partial_value[:, half_cap:])
    handed = jnp.where(even_core, partial_value[:, half_cap:], partial_value[:, :half_cap])
    partner_part = partner(handed, "expert", 0)
    finished = (kept + partner_part).astype(jnp.bfloat16)
    returned = lax.all_to_all(finished, "expert", split_axis=0, concat_axis=0, tiled=True)
    expert_sum = returned.reshape(experts * capacity, D)
    picked = jnp.take(expert_sum, slot_index, axis=0).astype(jnp.float32).reshape(seq_dev, TOPK, D)
    expert_mix = jnp.sum(picked * gate_weights[:, :, None], 1)
    return (resid_wide + expert_mix).astype(jnp.bfloat16)


def layer_kernel(
    devices,
    owners_hbm,
    lengths_hbm,
    blocks_hbm,
    pages_hbm,
    q_hbm,
    dkv_hbm,
    table_hbm,
    kv_hbm,
    hidden_hbm,
    gain_hbm,
    router_hbm,
    ids_hbm,
    gate_hbm,
    up_hbm,
    down_hbm,
    out_ref,
    owners,
    prompt_lengths,
    blocks,
    pages_ref,
    q_ref,
    dkv_ref,
    table_ref,
    kv_ref,
    hidden_ref,
    gain_ref,
    router_ref,
    ids_ref,
    w_in,
    w_down,
    other_pages,
    q_send,
    q_recv,
    o_send,
    o_recv,
    lse_send,
    lse_recv,
    attn,
    x_a,
    gates_a,
    x_b,
    gates_b,
    part_a,
    core_a,
    y_send,
    y_recv,
    z_send,
    z_recv,
    zf_send,
    zf_recv,
    yf_send,
    yf_recv,
    kept,
    part_b,
    core_b,
    sum_b,
    recv_b,
    in_sem,
    w_sem,
    page_sem,
    q_sem,
    o_sem,
    lse_sem,
    xa_ssem,
    xa_rsem,
    xb_ssem,
    xb_rsem,
    c_ssem,
    c_rsem,
    y_ssem,
    y_rsem,
    z_sem,
    zf_ssem,
    zf_rsem,
    yf_sem,
    cb_ssem,
    cb_rsem,
    rb_sem,
):
    f32, bf16 = jnp.float32, jnp.bfloat16
    me = lax.axis_index("expert")
    lines = devices // 4
    chips = devices // 2
    core, row, line = lax.rem(me, 2), lax.rem(me // 2, 2), me // 4
    unit = row * lines + line
    seqs = hidden_ref.shape[0]
    group = QUERY_HEADS // KEY_VALUE_HEADS
    scale = 1.0 / math.sqrt(HEAD_SIZE)
    old_rows = pl.ds(MAXP, seqs - MAXP)
    new_rows = pl.ds(0, MAXP)

    def device(at_line, at_row, at_core):
        return (at_line * 2 + at_row) * 2 + at_core

    def device_of(at_unit, at_core):
        return device(lax.rem(at_unit, lines), at_unit // lines, at_core)

    def place(at_line, at_row, at_core):
        return (at_core * 2 + at_row) * lines + at_line

    low = line * 2 < lines

    def far_line(j):
        return jnp.where(low, lines - 1 - j, j)

    def far_other_line(j):
        down = lines - 1 - j
        return jnp.where(
            low, jnp.where(down > line, down, down - 1), jnp.where(j < line, j, j + 1)
        )

    def all_units():
        yield from other_units()
        yield unit

    def other_units():
        for j in range(lines):
            yield (1 - row) * lines + far_line(j)
            if j < lines - 1:
                yield row * lines + far_other_line(j)

    def remote(src, dst, ssem, rsem, to):
        return pltpu.make_async_remote_copy(
            src_ref=src,
            dst_ref=dst,
            send_sem=ssem,
            recv_sem=rsem,
            device_id={"expert": to},
            device_id_type=pl.DeviceIdType.MESH,
        )

    other_row = device(line, 1 - row, core)
    other_core = device(line, row, 1 - core)
    mine = place(line, row, core)

    loads = [
        pltpu.make_async_copy(a, b, in_sem.at[i])
        for i, (a, b) in enumerate(
            (
                (q_hbm, q_ref),
                (pages_hbm, pages_ref),
                (dkv_hbm, dkv_ref),
                (table_hbm, table_ref),
                (kv_hbm, kv_ref),
                (hidden_hbm, hidden_ref),
                (gain_hbm, gain_ref),
                (router_hbm, router_ref),
                (ids_hbm, ids_ref),
                (blocks_hbm, blocks),
                (owners_hbm, owners),
                (lengths_hbm, prompt_lengths),
            )
        )
    ]
    hidden = w_down.shape[0]
    weights = [
        pltpu.make_async_copy(gate_hbm.at[0], w_in.at[:, pl.ds(0, hidden)], w_sem.at[0]),
        pltpu.make_async_copy(up_hbm.at[0], w_in.at[:, pl.ds(hidden, hidden)], w_sem.at[1]),
        pltpu.make_async_copy(down_hbm.at[0], w_down, w_sem.at[2]),
    ]
    barrier = pltpu.get_barrier_semaphore()

    def greet(k, carry):
        pl.semaphore_signal(
            barrier,
            inc=1,
            device_id={"expert": lax.rem(me + k, devices)},
            device_id_type=pl.DeviceIdType.MESH,
        )
        return carry

    lax.fori_loop(1, devices, greet, 0)
    for copy in loads + weights:
        copy.start()

    fold = seqs // MAXP
    lane_heads = QUERY_HEADS // fold
    packed = lane_heads * HEAD_SIZE
    per_kv = lane_heads // KEY_VALUE_HEADS
    sub = lax.broadcasted_iota(jnp.int32, (seqs, packed), 0) // MAXP

    def head_cols(h):
        return slice(h * HEAD_SIZE, (h + 1) * HEAD_SIZE)

    def turn(x, by):
        by = by % seqs
        return x if by == 0 else pltpu.roll(x, by, 0)

    def pack(rows):
        out = None
        for f in range(fold):
            wide = turn(
                jnp.concatenate([rows[:, head_cols(fold * hh + f)] for hh in range(lane_heads)], 1),
                MAXP * f,
            )
            out = wide if f == 0 else jnp.where(sub == f, wide, out)
        return out

    def spread_rows(rows):
        out = rows
        at = lax.broadcasted_iota(jnp.int32, rows.shape, 0) // MAXP
        for f in range(1, fold):
            out = jnp.where(at == f, turn(rows, MAXP * f), out)
        return out

    def dot_t(a, b):
        return lax.dot_general(a, b, (((1,), (1,)), ((), ())), preferred_element_type=f32)

    loads[0].wait()
    q_packed = pack(q_ref[...].astype(f32))
    q_send[...] = q_packed.astype(bf16)
    for copy in loads[2:]:
        copy.wait()

    def per_seq(values, shape):
        at = lax.broadcasted_iota(jnp.int32, shape, 0)
        return sum(jnp.where(at == s, v, 0) for s, v in enumerate(values))

    tokens = kv_ref.shape[0] * PAGE_TOKENS
    limit = per_seq([blocks[s] for s in range(seqs)], (seqs, tokens))
    page_of = lax.broadcasted_iota(jnp.int32, (seqs, tokens), 1) // PAGE_TOKENS
    held = jnp.zeros((seqs, tokens), f32)
    for b in range(table_ref.shape[1]):
        hit = (page_of == table_ref[:, b : b + 1]) & (limit > b)
        held = held + jnp.where(hit, 1.0, 0.0)
    held = jnp.concatenate([held] * group, 0)

    def heads(h):
        rows = q_ref[...].astype(f32)
        return jnp.concatenate([rows[:, head_cols(h * group + g)] for g in range(group)], 0)

    def own(h, at):
        both = dkv_ref[...].astype(f32)
        return jnp.concatenate([both[:, at, head_cols(h)]] * group, 0)

    def weigh(scores, times, own_score):
        scores = jnp.where(times > 0, scores, masked_score)
        peak = jnp.maximum(jnp.max(scores, -1, keepdims=True), own_score)
        weight = times * jnp.exp(scores - peak)
        own_weight = jnp.exp(own_score - peak)
        total = jnp.sum(weight, -1, keepdims=True) + own_weight
        return (weight / total).astype(bf16), (own_weight / total).astype(bf16).astype(f32)

    for h in range(KEY_VALUE_HEADS):
        at = head_cols(h)
        queries = heads(h)
        own_score = jnp.sum(queries * own(h, 0), -1, keepdims=True) * scale
        keys = kv_ref[:, 0, :, at].reshape(tokens, HEAD_SIZE)
        values = kv_ref[:, 1, :, at].reshape(tokens, HEAD_SIZE)
        probs, own_prob = weigh(dot_t(queries.astype(bf16), keys) * scale, held, own_score)
        mixed = jnp.dot(probs, values, preferred_element_type=f32) + own_prob * own(h, 1)
        for g in range(group):
            attn[:, head_cols(h * group + g)] = mixed[g * seqs : (g + 1) * seqs]

    def residual_of(attention):
        rounded = attention.astype(bf16).astype(f32)
        return (hidden_ref[...].astype(f32) + rounded).astype(bf16).astype(f32)

    def norm_of(wide):
        mean = jnp.mean(wide * wide, -1, keepdims=True)
        return (wide * lax.rsqrt(mean + norm_eps) * gain_ref[...]).astype(bf16)

    def gate_of(normed):
        logits = dot_t(normed, router_ref[...])
        experts = logits.shape[1]
        expert_of = lax.broadcasted_iota(jnp.int32, (seqs, experts), 1)
        times = jnp.zeros((seqs, experts), f32)
        for k in range(ids_ref.shape[1]):
            times = times + jnp.where(ids_ref[:, k : k + 1] == expert_of, 1.0, 0.0)
        picked = jnp.where(times > 0, logits, masked_score)
        gate = times * jnp.exp(picked - jnp.max(picked, -1, keepdims=True))
        gate = gate / jnp.sum(gate, -1, keepdims=True)
        return jnp.concatenate([gate] * (128 // experts), 1)

    normed = norm_of(residual_of(attn[...]))
    x_a[mine] = normed
    pl.semaphore_wait(barrier, devices - 1)

    def q_copy(to):
        return remote(q_send, q_recv.at[unit], q_sem.at[0], q_sem.at[1], device_of(to, 1 - core))

    for to in all_units():
        q_copy(to).start()
    loads[1].wait()
    page_copy = remote(pages_ref, other_pages, page_sem.at[0], page_sem.at[1], other_core)
    page_copy.start()


    def pass_on(pool, spot, count, at, to):
        buffer, rows, n = pool
        ref = buffer.at[pl.ds(spot, count), rows]
        return remote(ref, ref, xa_ssem.at[n], xa_rsem.at[n, at], to)

    far, near = lax.rem(line + 2, lines), line + 1 - 2 * lax.rem(line, 2)
    far_device, near_device = device(far, row, 1 - core), device(near, row, 1 - core)
    row_device = device(line, 1 - row, 1 - core)
    at_far, at_near, at_relay, at_core = 0, 1, 2, 7
    sources = (far, near, lax.rem(near + 2, lines), line)
    z_cores, y_cores = (1 - core, 1 - core, core), (core, core, 1 - core, 1 - core)

    def at_y(n):
        return 3 + n

    def cross(pool, spot, n):
        pass_on(pool, spot, 1, at_y(n), row_device).start()
        pass_on(pool, spot, 1, at_core, other_core).start()

    def z_arrive(pool, n):
        spot = place(sources[n], row, z_cores[n])
        pass_on(pool, spot, 1, n, other_row).wait_recv()
        if n == at_far:
            pass_on(pool, spot, 1, at_relay, near_device).start()
        cross(pool, spot, n)

    def y_arrive(pool, n):
        spot = place(sources[n], 1 - row, y_cores[n])
        pass_on(pool, spot, 1, at_y(n), other_row).wait_recv()
        pass_on(pool, spot, 1, at_core, other_core).start()

    def first_hops(pool):
        pass_on(pool, mine, 1, at_far, far_device).start()
        pass_on(pool, mine, 1, at_near, near_device).start()
        cross(pool, mine, 3)

    pools = [(x_a, old_rows, 0), (gates_a, pl.ds(0, seqs), 1)]
    first_hops(pools[0])
    gates_a[mine] = gate_of(normed)
    first_hops(pools[1])

    prompts = owners.shape[0]
    shape = (1, prompts * PAGE_TOKENS)
    prompt_of = lax.broadcasted_iota(jnp.int32, shape, 1) // PAGE_TOKENS
    owner_of, length_of = jnp.zeros(shape, jnp.int32), jnp.zeros(shape, jnp.int32)
    for p in range(prompts):
        owner_of = jnp.where(prompt_of == p, owners[p], owner_of)
        length_of = jnp.where(prompt_of == p, prompt_lengths[p], length_of)
    rank_of = jnp.zeros(shape, jnp.int32)
    for p in range(prompts):
        rank_of = rank_of + jnp.where((owner_of == owners[p]) & (prompt_of > p), 1, 0)
    slots = chips * seqs
    at_row = lax.broadcasted_iota(jnp.int32, (slots, 1), 0)
    row_unit = at_row // seqs
    row_owner = device_of(row_unit, 1 - core)
    match = (owner_of == row_owner) & (rank_of == lax.rem(at_row, MAXP))

    def allowed_at(position):
        ok = match & (length_of > position)
        return jnp.concatenate([jnp.where(ok, 1.0, 0.0)] * per_kv, 0)

    allowed = (allowed_at(me), allowed_at(other_core))
    page_copy.wait_recv()

    q_all = remote(q_recv, q_recv, q_sem.at[0], q_sem.at[1], other_core)
    q_all.wait_recv()
    lane_of = lax.broadcasted_iota(jnp.int32, (slots, 128), 1)
    lse_all = jnp.zeros((slots, 128), f32)
    for h in range(KEY_VALUE_HEADS):
        at = head_cols(h)
        lanes = [h * per_kv + j for j in range(per_kv)]
        queries = jnp.concatenate(
            [q_recv[:, :, head_cols(hh)].reshape(slots, HEAD_SIZE) for hh in lanes], 0
        )
        scores = []
        for ref, ok in zip((pages_ref, other_pages), allowed):
            keys = ref[:, 0, :, at].reshape(prompts * PAGE_TOKENS, HEAD_SIZE)
            scores.append(jnp.where(ok > 0, dot_t(queries, keys) * scale, masked_score))
        peak = jnp.maximum(
            jnp.max(scores[0], -1, keepdims=True), jnp.max(scores[1], -1, keepdims=True)
        )
        total = jnp.zeros((slots * per_kv, 1), f32)
        mixed = jnp.zeros((slots * per_kv, HEAD_SIZE), f32)
        for ref, score in zip((pages_ref, other_pages), scores):
            weight = jnp.exp(score - peak)
            total = total + jnp.sum(weight, -1, keepdims=True)
            values = ref[:, 1, :, at].reshape(prompts * PAGE_TOKENS, HEAD_SIZE)
            mixed = mixed + jnp.dot(weight.astype(bf16), values, preferred_element_type=f32)
        mixed = mixed / total
        lse = jnp.where(peak > masked_score, peak + jnp.log(total), masked_score)
        for j, hh in enumerate(lanes):
            rows = slice(j * slots, (j + 1) * slots)
            o_send[:, :, head_cols(hh)] = mixed[rows].astype(bf16).reshape(chips, seqs, HEAD_SIZE)
            lse_all = jnp.where(lane_of == hh, lse[rows], lse_all)
    lse_send[...] = lse_all.reshape(chips, seqs, 128)

    def o_copy(to):
        at = device_of(to, 1 - core)
        return (
            remote(o_send.at[to], o_recv.at[unit], o_sem.at[0], o_sem.at[1], at),
            remote(lse_send.at[to], lse_recv.at[unit], lse_sem.at[0], lse_sem.at[1], at),
        )

    for to in all_units():
        for copy in o_copy(to):
            copy.start()

    for pool in pools:
        z_arrive(pool, at_far)
    for pool in pools:
        z_arrive(pool, at_near)
    for pool in pools:
        y_arrive(pool, 3)
    for pool in pools:
        z_arrive(pool, at_relay)

    own_both = dkv_ref[...].astype(f32)
    own_key = spread_rows(own_both[:, 0])
    own_value = spread_rows(own_both[:, 1])
    lane = lax.broadcasted_iota(jnp.int32, (seqs, 128), 1)
    own_score = jnp.zeros((seqs, 128), f32)
    for hh in range(lane_heads):
        score = jnp.sum(
            q_packed[:, head_cols(hh)] * own_key[:, head_cols(hh // per_kv)], -1, keepdims=True
        )
        own_score = jnp.where(lane == hh, score * scale, own_score)
    new_count = jnp.int32(0)
    for p in range(prompts):
        new_count = new_count + (owners[p] == me).astype(jnp.int32)
    is_new = lax.broadcasted_iota(jnp.int32, (seqs, HEAD_SIZE), 0) < new_count

    o_all = (
        remote(o_recv, o_recv, o_sem.at[0], o_sem.at[1], other_core),
        remote(lse_recv, lse_recv, lse_sem.at[0], lse_sem.at[1], other_core),
    )
    for copy in o_all:
        copy.wait_recv()
    peak = own_score
    for u in range(chips):
        peak = jnp.maximum(peak, lse_recv[u])
    shares = [jnp.exp(lse_recv[u] - peak) for u in range(chips)]
    own_share = jnp.exp(own_score - peak)
    total = own_share
    for share in shares:
        total = total + share
    inverse = 1.0 / total
    shares = [share * inverse for share in shares]
    own_share = own_share * inverse
    for hh in range(lane_heads):
        at = head_cols(hh)
        mixed = own_share[:, hh : hh + 1] * own_value[:, head_cols(hh // per_kv)]
        for u in range(chips):
            mixed = mixed + shares[u][:, hh : hh + 1] * o_recv[u, :, at].astype(f32)
        for f in range(fold):
            cols = head_cols(fold * hh + f)
            attn[:, cols] = jnp.where(is_new, turn(mixed, -MAXP * f), attn[:, cols])
    wide = residual_of(attn[...])
    attn[...] = wide
    normed = norm_of(wide)
    x_b[mine] = normed

    b_pools = [(x_b, new_rows, 0), (gates_b, pl.ds(0, seqs), 1)]

    def b_copy(pool, to):
        buffer, rows, n = pool
        ref = buffer.at[mine, rows]
        return remote(ref, ref, xb_ssem.at[n], xb_rsem.at[n, 0], device_of(to, 1 - core))

    def b_core_copy(pool, spot, count):
        buffer, rows, n = pool
        ref = buffer.at[pl.ds(spot, count), rows]
        return remote(ref, ref, xb_ssem.at[n], xb_rsem.at[n, 1], other_core)

    def b_first(pool):
        for to in other_units():
            b_copy(pool, to).start()
        b_core_copy(pool, mine, 1).start()

    def b_pass(pool):
        buffer, rows, n = pool
        ref = buffer.at[pl.ds(0, chips - 1), rows]
        remote(ref, ref, xb_ssem.at[n], xb_rsem.at[n, 0], other_core).wait_recv()
        for source in other_units():
            b_core_copy(pool, (1 - core) * chips + source, 1).start()

    b_first(b_pools[0])
    gates_b[mine] = gate_of(normed)
    b_first(b_pools[1])

    for copy in weights:
        copy.wait()

    def activate(x, gate):
        total = x.shape[0]
        lanes_of = lax.broadcasted_iota(jnp.int32, (total, 128), 1)
        both = jnp.dot(x, w_in[...], preferred_element_type=f32)
        gate_proj, up_proj = both[:, :hidden], both[:, hidden:]
        scaled = jnp.sum(jnp.where(lanes_of == me // 2, gate, 0.0), -1, keepdims=True)
        return (gate_proj / (1.0 + jnp.exp(-gate_proj)) * up_proj * scaled).astype(bf16)

    total = devices * seqs

    def rows_of(ref):
        return ref[...].reshape(total, ref.shape[2])

    chunks = c_rsem.shape[0]
    ends = (0, D // 4, D // 2, 3 * D // 4, D)
    z_chunks = zf_rsem.shape[0]
    half = ends[z_chunks]

    def late(i):
        return slice(ends[i] - half, ends[i + 1] - half)

    def cut(i):
        return slice(ends[i], ends[i + 1])

    def core_copy(i):
        return remote(
            part_a.at[1 - core, :, :, old_rows, cut(i)],
            core_a.at[:, :, old_rows, cut(i)],
            c_ssem,
            c_rsem.at[i],
            other_core,
        )

    def row_copy(i):
        return remote(
            y_send.at[:, old_rows, late(i)],
            y_recv.at[:, old_rows, late(i)],
            y_ssem,
            y_rsem.at[i - z_chunks],
            other_row,
        )

    def line_copy(i, k):
        to = lax.rem(line + k, lines)
        return remote(
            z_send.at[k, old_rows, late(i)],
            z_recv.at[k, old_rows, late(i)],
            z_sem.at[0],
            z_sem.at[1],
            device(to, row, core),
        )

    for n in range(3):
        for pool in pools:
            y_arrive(pool, n)
    for pool in pools:
        pass_on(pool, (1 - core) * chips, chips, at_core, other_core).wait_recv()
    activated = activate(rows_of(x_a), rows_of(gates_a))

    def zf_copy(i, k):
        to = lax.rem(line + k, lines)
        return remote(
            zf_send.at[k, :, old_rows, cut(i)],
            zf_recv.at[k, :, old_rows, cut(i)],
            zf_ssem,
            zf_rsem.at[i],
            device(to, row, core),
        )

    def held_by(at_row, at_line, i):
        return part_a[core, at_row, at_line, :, cut(i)].astype(f32) + core_a[
            at_row, at_line, :, cut(i)
        ].astype(f32)

    def zf_step(i):
        core_copy(i).wait_recv()
        for k in (2, 1, 3):
            for at_row in range(2):
                zf_send[k, at_row, :, cut(i)] = held_by(
                    at_row, lax.rem(line + k, lines), i
                ).astype(bf16)
            zf_copy(i, k).start()

    def yf_copy():
        return remote(
            yf_send.at[old_rows], yf_recv.at[old_rows], yf_sem.at[0], yf_sem.at[1], other_row
        )

    def yf_step(i):
        ref = zf_recv.at[pl.ds(1, lines - 1), :, old_rows, cut(i)]
        remote(ref, ref, zf_ssem, zf_rsem.at[i], other_core).wait_recv()

        def summed(at_row):
            total = held_by(at_row, line, i)
            for k in range(1, lines):
                total = total + zf_recv[k, at_row, :, cut(i)].astype(f32)
            return total

        yf_send[:, cut(i)] = summed(1 - row).astype(bf16)
        kept[:, cut(i)] = attn[:, cut(i)] + summed(row)

    def row_step(i):
        if i < z_chunks:
            zf_step(i)
            return
        core_copy(i).wait_recv()
        y_send[:, :, late(i)] = (
            part_a[core, 1 - row, :, :, cut(i)].astype(f32)
            + core_a[1 - row, :, :, cut(i)].astype(f32)
        ).astype(bf16)
        row_copy(i).start()

    behind = 3
    for i in range(chunks):
        rows = jnp.dot(activated, w_down[:, cut(i)], preferred_element_type=f32)
        part_a[:, :, :, :, cut(i)] = rows.astype(bf16).reshape(
            2, 2, lines, seqs, ends[i + 1] - ends[i]
        )
        core_copy(i).start()
        if i == 1:
            for pool in b_pools:
                b_pass(pool)
        if i >= behind:
            row_step(i - behind)
    for i in range(chunks - behind, chunks):
        row_step(i)

    for pool in b_pools:
        b_core_copy(pool, 0, chips).wait_recv()
    activated = activate(rows_of(x_b), rows_of(gates_b))
    b_chunks = cb_rsem.shape[0]
    b_width = D // b_chunks

    def b_core(i):
        at = slice(i * b_width, (i + 1) * b_width)
        return remote(
            part_b.at[core, :, new_rows, at],
            core_b.at[:, new_rows, at],
            cb_ssem,
            cb_rsem.at[i],
            other_core,
        )

    for i in range(b_chunks):
        at = slice(i * b_width, (i + 1) * b_width)
        rows = jnp.dot(activated, w_down[:, at], preferred_element_type=f32)
        part_b[:, :, :, at] = rows.astype(bf16).reshape(2, chips, seqs, b_width)
        b_core(i).start()

    def b_return(to):
        return remote(
            sum_b.at[to, new_rows],
            recv_b.at[unit, new_rows],
            rb_sem.at[0],
            rb_sem.at[1],
            device_of(to, 1 - core),
        )

    def line_step(i):
        row_copy(i).wait_recv()

        def summed(at_line):
            return (
                part_a[core, row, at_line, :, cut(i)].astype(f32)
                + core_a[row, at_line, :, cut(i)].astype(f32)
                + y_recv[at_line, :, late(i)].astype(f32)
            )

        for k in range(1, lines):
            z_send[k, :, late(i)] = summed(lax.rem(line + k, lines)).astype(bf16)
            line_copy(i, k).start()
        kept[:, cut(i)] = attn[:, cut(i)] + summed(line)

    early = chunks - 1
    for i in range(z_chunks, early):
        line_step(i)
    for i in range(b_chunks):
        b_core(i).wait_recv()
    for to in all_units():
        sum_b[to] = (part_b[1 - core, to].astype(f32) + core_b[to].astype(f32)).astype(bf16)
        b_return(to).start()
    for i in range(early, chunks):
        line_step(i)
    for i in range(z_chunks):
        yf_step(i)
    yf_copy().start()

    rest = pl.ds(1, lines - 1)
    z_all = remote(
        z_recv.at[rest, old_rows], z_recv.at[rest, old_rows], z_sem.at[0], z_sem.at[1], other_core
    )
    z_all.wait_recv()
    answer = kept[:, half:]
    for k in range(1, lines):
        answer = answer + z_recv[k].astype(f32)
    yf_copy().wait_recv()
    answer = jnp.concatenate([kept[:, :half] + yf_recv[...].astype(f32), answer], 1)

    b_all = remote(
        recv_b.at[:, new_rows], recv_b.at[:, new_rows], rb_sem.at[0], rb_sem.at[1], other_core
    )
    b_all.wait_recv()
    last = attn[...]
    for u in range(chips):
        last = last + recv_b[u].astype(f32)
    is_b = lax.broadcasted_iota(jnp.int32, (seqs, D), 0) < MAXP
    out_ref[...] = jnp.where(is_b, last, answer).astype(bf16)

    for copy in (page_copy, q_all, z_all, b_all, yf_copy()) + o_all:
        copy.wait_send()
    for n, (buffer, rows) in enumerate(((x_a, old_rows), (gates_a, pl.ds(0, seqs)))):
        ref = buffer.at[pl.ds(0, 4 * lines - 1), rows]
        remote(ref, ref, xa_ssem.at[n], xa_rsem.at[n, 0], other_core).wait_send()
    for n, (buffer, rows) in enumerate(((x_b, new_rows), (gates_b, pl.ds(0, seqs)))):
        ref = buffer.at[pl.ds(0, 2 * chips - 1), rows]
        remote(ref, ref, xb_ssem.at[n], xb_rsem.at[n, 0], other_core).wait_send()
    for ref, ssem, rsem in (
        (part_a.at[0, :, :, old_rows], c_ssem, c_rsem.at[0]),
        (y_send.at[:, old_rows], y_ssem, y_rsem.at[0]),
        (zf_send.at[pl.ds(1, lines - 1), :, old_rows], zf_ssem, zf_rsem.at[0]),
        (part_b.at[0, :, new_rows], cb_ssem, cb_rsem.at[0]),
    ):
        remote(ref, ref, ssem, rsem, other_core).wait_send()


def dense(
    hidden_in,
    queries,
    decode_key_value,
    local_kv,
    page_table,
    seq_blocks,
    prompt_kv,
    prompt_owner,
    prompt_pages,
    norm_gain,
    router,
    w_gate,
    w_up,
    w_down,
    route_ids,
):
    devices = lax.axis_size("expert")
    seqs = hidden_in.shape[0]
    hidden = w_gate.shape[2]
    lines = devices // 4
    chips = devices // 2
    bf16, f32 = jnp.bfloat16, jnp.float32
    chunks, z_chunks = 4, 2
    b_chunks = 2
    packed = D * MAXP // seqs
    loaded = (
        prompt_kv[0],
        queries,
        decode_key_value,
        page_table,
        local_kv,
        hidden_in,
        norm_gain[None, :],
        router.T,
        route_ids,
    )
    scalars = (prompt_owner, prompt_pages, seq_blocks)
    hbm = pl.BlockSpec(memory_space=pltpu.HBM)
    dma = pltpu.SemaphoreType.DMA
    return pl.pallas_call(
        functools.partial(layer_kernel, devices),
        out_shape=pltpu.VMEM((seqs, D), bf16),
        in_specs=[hbm] * (len(loaded) + 6),
        out_specs=pl.BlockSpec(memory_space=pltpu.VMEM),
        scratch_shapes=[pltpu.SMEM(a.shape, a.dtype) for a in scalars]
        + [pltpu.VMEM(a.shape, a.dtype) for a in loaded]
        + [
            pltpu.VMEM((D, 2 * hidden), bf16),
            pltpu.VMEM((hidden, D), bf16),
            pltpu.VMEM(loaded[0].shape, bf16),
            pltpu.VMEM((seqs, packed), bf16),
            pltpu.VMEM((chips, seqs, packed), bf16),
            pltpu.VMEM((chips, seqs, packed), bf16),
            pltpu.VMEM((chips, seqs, packed), bf16),
            pltpu.VMEM((chips, seqs, 128), f32),
            pltpu.VMEM((chips, seqs, 128), f32),
            pltpu.VMEM((seqs, D), f32),
            pltpu.VMEM((devices, seqs, D), bf16),
            pltpu.VMEM((devices, seqs, 128), f32),
            pltpu.VMEM((devices, seqs, D), bf16),
            pltpu.VMEM((devices, seqs, 128), f32),
            pltpu.VMEM((2, 2, lines, seqs, D), bf16),
            pltpu.VMEM((2, lines, seqs, D), bf16),
            pltpu.VMEM((lines, seqs, D // 2), bf16),
            pltpu.VMEM((lines, seqs, D // 2), bf16),
            pltpu.VMEM((lines, seqs, D // 2), bf16),
            pltpu.VMEM((lines, seqs, D // 2), bf16),
            pltpu.VMEM((lines, 2, seqs, D // 2), bf16),
            pltpu.VMEM((lines, 2, seqs, D // 2), bf16),
            pltpu.VMEM((seqs, D // 2), bf16),
            pltpu.VMEM((seqs, D // 2), bf16),
            pltpu.VMEM((seqs, D), f32),
            pltpu.VMEM((2, chips, seqs, D), bf16),
            pltpu.VMEM((chips, seqs, D), bf16),
            pltpu.VMEM((chips, seqs, D), bf16),
            pltpu.VMEM((chips, seqs, D), bf16),
            dma((len(loaded) + len(scalars),)),
            dma((3,)),
            dma((2,)),
            dma((2,)),
            dma((2,)),
            dma((2,)),
            dma((2,)),
            dma((2, 2 * lines)),
            dma((2,)),
            dma((2, 2)),
            dma(()),
            dma((chunks,)),
            dma(()),
            dma((chunks - z_chunks,)),
            dma((2,)),
            dma(()),
            dma((z_chunks,)),
            dma((2,)),
            dma(()),
            dma((b_chunks,)),
            dma((2,)),
        ],
        compiler_params=pltpu.CompilerParams(
            collective_id=0, has_side_effects=True, vmem_limit_bytes=58 * 2**20
        ),
    )(*scalars, *loaded, w_gate, w_up, w_down)


def local(*arrays):
    devices = lax.axis_size("expert")
    experts = arrays[10].shape[1]
    if experts == TOPK and devices == 2 * experts and devices % 4 == 0:
        return dense(*arrays)
    return routed(*arrays)


def solution(mesh):
    return jax.shard_map(
        local,
        mesh=mesh,
        in_specs=(
            P(("groups", "expert"), None),
            P(("groups", "expert"), None),
            P(("groups", "expert"), None, None),
            P(("groups", "expert"), None, None, None),
            P(("groups", "expert"), None),
            P(("groups", "expert")),
            P(("groups", "expert"), None, None, None, None),
            P("groups"),
            P("groups"),
            P(),
            P(),
            P("expert", None, None),
            P("expert", None, None),
            P("expert", None, None),
            P(("groups", "expert"), None),
        ),
        out_specs=P(("groups", "expert"), None),
        check_vma=False,
    )
```

```python
import functools
import math

import jax
import jax.numpy as jnp
from jax import lax
from jax.experimental import pallas as pl
from jax.experimental.pallas import tpu as pltpu
from jax.sharding import PartitionSpec as P

D = 4096
QUERY_HEADS = 32
KEY_VALUE_HEADS = 2
HEAD_SIZE = 128
PAGE_TOKENS = 16
TOPK = 8
MAXB = 16
MAXP = 2


norm_eps = 1e-06
masked_score = -1e30


def partner(x, axis, apart):
    return lax.ppermute(x, axis, [(i, i ^ 1 << apart) for i in range(lax.axis_size(axis))])


def attend(rows_of_queries, rows_of_keys, rows_of_values, allowed, token_own_key, token_own_value):
    decode_tokens = rows_of_queries.shape[0]
    heads_of_queries = rows_of_queries.reshape(
        decode_tokens, KEY_VALUE_HEADS, QUERY_HEADS // KEY_VALUE_HEADS, HEAD_SIZE
    )
    heads_of_keys = rows_of_keys.reshape(decode_tokens, -1, KEY_VALUE_HEADS, HEAD_SIZE)
    heads_of_values = rows_of_values.reshape(decode_tokens, -1, KEY_VALUE_HEADS, HEAD_SIZE)
    scale_for_scores = 1.0 / math.sqrt(HEAD_SIZE)
    allowed_mask = allowed[:, None, None, :]
    scores = (
        jnp.einsum(
            "tkgd,tlkd->tkgl", heads_of_queries, heads_of_keys, preferred_element_type=jnp.float32
        )
        * scale_for_scores
    )
    scores = jnp.where(allowed_mask, scores, masked_score)
    token_own_score = (
        jnp.einsum(
            "xejp,xep->xej",
            heads_of_queries,
            token_own_key.reshape(decode_tokens, KEY_VALUE_HEADS, HEAD_SIZE),
            preferred_element_type=jnp.float32,
        )
        * scale_for_scores
    )
    peak = jnp.maximum(jnp.max(scores, -1), token_own_score)
    weights = jnp.where(allowed_mask, jnp.exp(scores - peak[..., None]), 0.0)
    own_weight = jnp.exp(token_own_score - peak)
    denominator = jnp.sum(weights, -1) + own_weight
    probs = (weights / denominator[..., None]).astype(jnp.bfloat16)
    token_own_probability = (own_weight / denominator).astype(jnp.bfloat16)
    blended_noise = jnp.einsum(
        "tkgl,tlkd->tkgd", probs, heads_of_values, preferred_element_type=jnp.float32
    )
    blended_noise = blended_noise + token_own_probability.astype(jnp.float32)[
        ..., None
    ] * token_own_value.reshape(decode_tokens, KEY_VALUE_HEADS, 1, HEAD_SIZE).astype(jnp.float32)
    return blended_noise.reshape(decode_tokens, QUERY_HEADS * HEAD_SIZE).astype(jnp.bfloat16)


def routed(
    hidden_in,
    queries,
    decode_key_value,
    local_kv,
    page_table,
    seq_blocks,
    prompt_kv,
    prompt_owner,
    prompt_pages,
    norm_gain,
    router,
    w_gate,
    w_up,
    w_down,
    route_ids,
):
    devices = lax.axis_size("expert")
    position = lax.axis_index("expert")
    experts = devices // 2
    seq_dev = hidden_in.shape[0]
    key_value_width = KEY_VALUE_HEADS * HEAD_SIZE
    capacity = min(seq_dev, max(2, 2 * ((3 * seq_dev * TOPK + 2 * devices - 1) // (2 * devices))))
    half_cap = capacity // 2
    even_core = position % 2 == 0
    prompt_count = prompt_owner.shape[0]
    prompt_range = jnp.arange(prompt_count, dtype=jnp.int32)
    same_owner = prompt_owner[:, None] == prompt_owner[None, :]
    earlier = prompt_range[None, :] < prompt_range[:, None]
    arrival = jnp.sum((same_owner & earlier).astype(jnp.int32), 1)
    matching = (
        prompt_owner[None, None, :] == jnp.arange(devices, dtype=jnp.int32)[:, None, None]
    ) & (arrival[None, None, :] == jnp.arange(MAXP, dtype=jnp.int32)[None, :, None])
    chosen_prompt = jnp.sum(jnp.where(matching, prompt_range[None, None, :], 0), -1)
    occupied = jnp.any(matching, -1)
    own_picks = lax.dynamic_index_in_dim(chosen_prompt, position, 0, keepdims=False)
    own_occupied = lax.dynamic_index_in_dim(occupied, position, 0, keepdims=False)
    page_rows = prompt_kv[0]
    outgoing = jnp.take(page_rows, chosen_prompt.T.reshape(-1), axis=0).reshape(
        MAXP, devices, 2, PAGE_TOKENS, key_value_width
    )
    outgoing = jnp.where(occupied.T[:, :, None, None, None], outgoing, 0)
    arrived = lax.all_to_all(outgoing, "expert", split_axis=1, concat_axis=1, tiled=True)
    lengths = jnp.take(prompt_pages, own_picks)
    new_keys = arrived[:, :, 0].reshape(MAXP, devices * PAGE_TOKENS, key_value_width)
    new_values = arrived[:, :, 1].reshape(MAXP, devices * PAGE_TOKENS, key_value_width)
    new_allowed = (jnp.arange(devices * PAGE_TOKENS, dtype=jnp.int32) // PAGE_TOKENS)[
        None, :
    ] < lengths[:, None]
    fresh_rows = attend(
        queries[:MAXP],
        new_keys,
        new_values,
        new_allowed,
        decode_key_value[:MAXP, 0],
        decode_key_value[:MAXP, 1],
    )
    fetched = local_kv[page_table]
    old_keys = fetched[:, :, 0].reshape(seq_dev, MAXB * PAGE_TOKENS, key_value_width)
    old_values = fetched[:, :, 1].reshape(seq_dev, MAXB * PAGE_TOKENS, key_value_width)
    old_allowed = (jnp.arange(MAXB * PAGE_TOKENS, dtype=jnp.int32) // PAGE_TOKENS)[
        None, :
    ] < seq_blocks[:, None]
    old_out = attend(
        queries, old_keys, old_values, old_allowed, decode_key_value[:, 0], decode_key_value[:, 1]
    )
    new_count = jnp.sum(own_occupied.astype(jnp.int32))
    is_new = jnp.arange(MAXP, dtype=jnp.int32) < new_count
    attention = jnp.concatenate(
        [jnp.where(is_new[:, None], fresh_rows, old_out[:MAXP]), old_out[MAXP:]], 0
    )
    residual = (hidden_in.astype(jnp.float32) + attention.astype(jnp.float32)).astype(jnp.bfloat16)
    resid_wide = residual.astype(jnp.float32)
    normed = (
        resid_wide
        * lax.rsqrt(jnp.mean(resid_wide * resid_wide, -1, keepdims=True) + norm_eps)
        * norm_gain
    ).astype(jnp.bfloat16)
    logits = jnp.dot(normed, router, preferred_element_type=jnp.float32)
    expert_onehot = route_ids[:, :, None] == jnp.arange(experts, dtype=jnp.int32)[None, None, :]
    selected = jnp.sum(jnp.where(expert_onehot, logits[:, None, :], 0.0), -1)
    gate_weights = jax.nn.softmax(selected, -1)
    assigned = seq_dev * TOPK
    expert_ids = route_ids.reshape(assigned)
    chosen = (expert_ids[:, None] == jnp.arange(experts, dtype=jnp.int32)[None, :]).astype(
        jnp.int32
    )
    before = jnp.cumsum(chosen, 0) - chosen
    slot_rank = jnp.sum(before * chosen, 1)
    slot_index = expert_ids * capacity + slot_rank
    placing = slot_index[None, :] == jnp.arange(experts * capacity, dtype=jnp.int32)[:, None]
    selector = jnp.any(placing.reshape(experts * capacity, seq_dev, TOPK), -1).astype(jnp.bfloat16)
    gathered_rows = jnp.dot(selector, normed, preferred_element_type=jnp.float32).astype(
        jnp.bfloat16
    )
    outgoing_half = gathered_rows.reshape(devices, half_cap, D)
    own_half = lax.all_to_all(outgoing_half, "expert", split_axis=0, concat_axis=0, tiled=True)
    partner_half = partner(own_half, "expert", 0)
    received = jnp.where(
        even_core,
        jnp.concatenate([own_half, partner_half], 1),
        jnp.concatenate([partner_half, own_half], 1),
    )
    flattened = received.reshape(devices * capacity, D)
    gate_proj = jnp.dot(flattened, w_gate[0], preferred_element_type=jnp.float32)
    up_proj = jnp.dot(flattened, w_up[0], preferred_element_type=jnp.float32)
    activated = (jax.nn.silu(gate_proj) * up_proj).astype(jnp.bfloat16)
    partial_value = jnp.dot(activated, w_down[0], preferred_element_type=jnp.float32).reshape(
        devices, capacity, D
    )
    kept = jnp.where(even_core, partial_value[:, :half_cap], partial_value[:, half_cap:])
    handed = jnp.where(even_core, partial_value[:, half_cap:], partial_value[:, :half_cap])
    partner_part = partner(handed, "expert", 0)
    finished = (kept + partner_part).astype(jnp.bfloat16)
    returned = lax.all_to_all(finished, "expert", split_axis=0, concat_axis=0, tiled=True)
    expert_sum = returned.reshape(experts * capacity, D)
    picked = jnp.take(expert_sum, slot_index, axis=0).astype(jnp.float32).reshape(seq_dev, TOPK, D)
    expert_mix = jnp.sum(picked * gate_weights[:, :, None], 1)
    return (resid_wide + expert_mix).astype(jnp.bfloat16)


def layer_kernel(
    devices,
    owners_hbm,
    lengths_hbm,
    blocks_hbm,
    pages_hbm,
    q_hbm,
    dkv_hbm,
    table_hbm,
    kv_hbm,
    hidden_hbm,
    gain_hbm,
    router_hbm,
    ids_hbm,
    gate_hbm,
    up_hbm,
    down_hbm,
    out_ref,
    owners,
    prompt_lengths,
    blocks,
    pages_ref,
    q_ref,
    dkv_ref,
    table_ref,
    kv_ref,
    hidden_ref,
    gain_ref,
    router_ref,
    ids_ref,
    w_in,
    w_down,
    other_pages,
    q_send,
    q_recv,
    o_send,
    o_recv,
    lse_send,
    lse_recv,
    attn,
    x_a,
    x_b,
    gates_b,
    part_a,
    core_a,
    y_send,
    y_recv,
    z_send,
    z_recv,
    zf_send,
    zf_recv,
    yf_send,
    yf_recv,
    kept,
    part_b,
    core_b,
    sum_b,
    recv_b,
    in_sem,
    w_sem,
    page_sem,
    q_sem,
    o_sem,
    lse_sem,
    xa_ssem,
    xa_rsem,
    xb_ssem,
    xb_rsem,
    c_ssem,
    c_rsem,
    y_ssem,
    y_rsem,
    z_sem,
    zf_ssem,
    zf_rsem,
    yf_sem,
    cb_ssem,
    cb_rsem,
    rb_sem,
):
    f32, bf16 = jnp.float32, jnp.bfloat16
    me = lax.axis_index("expert")
    lines = devices // 4
    chips = devices // 2
    core, row, line = lax.rem(me, 2), lax.rem(me // 2, 2), me // 4
    unit = row * lines + line
    seqs = hidden_ref.shape[0]
    group = QUERY_HEADS // KEY_VALUE_HEADS
    scale = 1.0 / math.sqrt(HEAD_SIZE)
    old_rows = pl.ds(MAXP, seqs - MAXP)
    new_rows = pl.ds(0, MAXP)

    def device(at_line, at_row, at_core):
        return (at_line * 2 + at_row) * 2 + at_core

    def device_of(at_unit, at_core):
        return device(lax.rem(at_unit, lines), at_unit // lines, at_core)

    def place(at_line, at_row, at_core):
        return (at_core * 2 + at_row) * lines + at_line

    low = line * 2 < lines

    def far_line(j):
        return jnp.where(low, lines - 1 - j, j)

    def far_other_line(j):
        down = lines - 1 - j
        return jnp.where(
            low, jnp.where(down > line, down, down - 1), jnp.where(j < line, j, j + 1)
        )

    def all_units():
        yield from other_units()
        yield unit

    def other_units():
        for j in range(lines):
            yield (1 - row) * lines + far_line(j)
            if j < lines - 1:
                yield row * lines + far_other_line(j)

    def remote(src, dst, ssem, rsem, to):
        return pltpu.make_async_remote_copy(
            src_ref=src,
            dst_ref=dst,
            send_sem=ssem,
            recv_sem=rsem,
            device_id={"expert": to},
            device_id_type=pl.DeviceIdType.MESH,
        )

    other_row = device(line, 1 - row, core)
    other_core = device(line, row, 1 - core)
    mine = place(line, row, core)

    loads = [
        pltpu.make_async_copy(a, b, in_sem.at[i])
        for i, (a, b) in enumerate(
            (
                (q_hbm, q_ref),
                (pages_hbm, pages_ref),
                (dkv_hbm, dkv_ref),
                (table_hbm, table_ref),
                (kv_hbm, kv_ref),
                (hidden_hbm, hidden_ref),
                (gain_hbm, gain_ref),
                (router_hbm, router_ref),
                (ids_hbm, ids_ref),
                (blocks_hbm, blocks),
                (owners_hbm, owners),
                (lengths_hbm, prompt_lengths),
            )
        )
    ]
    hidden = w_down.shape[0]
    weights = [
        pltpu.make_async_copy(gate_hbm.at[0], w_in.at[:, pl.ds(0, hidden)], w_sem.at[0]),
        pltpu.make_async_copy(up_hbm.at[0], w_in.at[:, pl.ds(hidden, hidden)], w_sem.at[1]),
        pltpu.make_async_copy(down_hbm.at[0], w_down, w_sem.at[2]),
    ]
    barrier = pltpu.get_barrier_semaphore()

    def greet(k, carry):
        pl.semaphore_signal(
            barrier,
            inc=1,
            device_id={"expert": lax.rem(me + k, devices)},
            device_id_type=pl.DeviceIdType.MESH,
        )
        return carry

    lax.fori_loop(1, devices, greet, 0)
    for copy in loads + weights:
        copy.start()

    fold = seqs // MAXP
    lane_heads = QUERY_HEADS // fold
    packed = lane_heads * HEAD_SIZE
    per_kv = lane_heads // KEY_VALUE_HEADS
    sub = lax.broadcasted_iota(jnp.int32, (seqs, packed), 0) // MAXP

    def head_cols(h):
        return slice(h * HEAD_SIZE, (h + 1) * HEAD_SIZE)

    def turn(x, by):
        by = by % seqs
        return x if by == 0 else pltpu.roll(x, by, 0)

    def pack(rows):
        out = None
        for f in range(fold):
            wide = turn(
                jnp.concatenate([rows[:, head_cols(fold * hh + f)] for hh in range(lane_heads)], 1),
                MAXP * f,
            )
            out = wide if f == 0 else jnp.where(sub == f, wide, out)
        return out

    def spread_rows(rows):
        out = rows
        at = lax.broadcasted_iota(jnp.int32, rows.shape, 0) // MAXP
        for f in range(1, fold):
            out = jnp.where(at == f, turn(rows, MAXP * f), out)
        return out

    def dot_t(a, b):
        return lax.dot_general(a, b, (((1,), (1,)), ((), ())), preferred_element_type=f32)

    loads[0].wait()
    q_packed = pack(q_ref[...].astype(f32))
    q_send[...] = q_packed.astype(bf16)
    for copy in loads[2:]:
        copy.wait()

    def per_seq(values, shape):
        at = lax.broadcasted_iota(jnp.int32, shape, 0)
        return sum(jnp.where(at == s, v, 0) for s, v in enumerate(values))

    tokens = kv_ref.shape[0] * PAGE_TOKENS
    limit = per_seq([blocks[s] for s in range(seqs)], (seqs, tokens))
    page_of = lax.broadcasted_iota(jnp.int32, (seqs, tokens), 1) // PAGE_TOKENS
    held = jnp.zeros((seqs, tokens), f32)
    for b in range(table_ref.shape[1]):
        hit = (page_of == table_ref[:, b : b + 1]) & (limit > b)
        held = held + jnp.where(hit, 1.0, 0.0)
    held = jnp.concatenate([held] * group, 0)

    def heads(h):
        rows = q_ref[...].astype(f32)
        return jnp.concatenate([rows[:, head_cols(h * group + g)] for g in range(group)], 0)

    def own(h, at):
        both = dkv_ref[...].astype(f32)
        return jnp.concatenate([both[:, at, head_cols(h)]] * group, 0)

    def weigh(scores, times, own_score):
        scores = jnp.where(times > 0, scores, masked_score)
        peak = jnp.maximum(jnp.max(scores, -1, keepdims=True), own_score)
        weight = times * jnp.exp(scores - peak)
        own_weight = jnp.exp(own_score - peak)
        total = jnp.sum(weight, -1, keepdims=True) + own_weight
        return (weight / total).astype(bf16), (own_weight / total).astype(bf16).astype(f32)

    for h in range(KEY_VALUE_HEADS):
        at = head_cols(h)
        queries = heads(h)
        own_score = jnp.sum(queries * own(h, 0), -1, keepdims=True) * scale
        keys = kv_ref[:, 0, :, at].reshape(tokens, HEAD_SIZE)
        values = kv_ref[:, 1, :, at].reshape(tokens, HEAD_SIZE)
        probs, own_prob = weigh(dot_t(queries.astype(bf16), keys) * scale, held, own_score)
        mixed = jnp.dot(probs, values, preferred_element_type=f32) + own_prob * own(h, 1)
        for g in range(group):
            attn[:, head_cols(h * group + g)] = mixed[g * seqs : (g + 1) * seqs]

    def residual_of(attention):
        rounded = attention.astype(bf16).astype(f32)
        return (hidden_ref[...].astype(f32) + rounded).astype(bf16).astype(f32)

    def norm_of(wide):
        mean = jnp.mean(wide * wide, -1, keepdims=True)
        return (wide * lax.rsqrt(mean + norm_eps) * gain_ref[...]).astype(bf16)

    def gate_of(normed):
        logits = dot_t(normed, router_ref[...])
        experts = logits.shape[1]
        expert_of = lax.broadcasted_iota(jnp.int32, (seqs, experts), 1)
        times = jnp.zeros((seqs, experts), f32)
        for k in range(ids_ref.shape[1]):
            times = times + jnp.where(ids_ref[:, k : k + 1] == expert_of, 1.0, 0.0)
        picked = jnp.where(times > 0, logits, masked_score)
        gate = times * jnp.exp(picked - jnp.max(picked, -1, keepdims=True))
        gate = gate / jnp.sum(gate, -1, keepdims=True)
        return jnp.concatenate([gate] * (128 // experts), 1)

    normed = norm_of(residual_of(attn[...]))
    x_a[mine, :, :D] = normed
    pl.semaphore_wait(barrier, devices - 1)

    def q_copy(to):
        return remote(q_send, q_recv.at[unit], q_sem.at[0], q_sem.at[1], device_of(to, 1 - core))

    for to in all_units():
        q_copy(to).start()
    loads[1].wait()
    page_copy = remote(pages_ref, other_pages, page_sem.at[0], page_sem.at[1], other_core)
    page_copy.start()


    def pass_on(pool, spot, count, at, to):
        buffer, rows, cols, n = pool
        ref = buffer.at[pl.ds(spot, count), rows, cols]
        return remote(ref, ref, xa_ssem.at[n], xa_rsem.at[n, at], to)

    far, near = lax.rem(line + 2, lines), line + 1 - 2 * lax.rem(line, 2)
    far_device, near_device = device(far, row, 1 - core), device(near, row, 1 - core)
    row_device = device(line, 1 - row, 1 - core)
    at_far, at_near, at_relay, at_core = 0, 1, 2, 7
    sources = (far, near, lax.rem(near + 2, lines), line)
    z_cores, y_cores = (1 - core, 1 - core, core), (core, core, 1 - core, 1 - core)

    def at_y(n):
        return 3 + n

    def cross(pool, spot, n):
        pass_on(pool, spot, 1, at_y(n), row_device).start()
        pass_on(pool, spot, 1, at_core, other_core).start()

    def z_arrive(pool, n):
        spot = place(sources[n], row, z_cores[n])
        pass_on(pool, spot, 1, n, other_row).wait_recv()
        if n == at_far:
            pass_on(pool, spot, 1, at_relay, near_device).start()
        cross(pool, spot, n)

    def y_arrive(pool, n):
        spot = place(sources[n], 1 - row, y_cores[n])
        pass_on(pool, spot, 1, at_y(n), other_row).wait_recv()
        pass_on(pool, spot, 1, at_core, other_core).start()

    def first_hops(pool):
        pass_on(pool, mine, 1, at_far, far_device).start()
        pass_on(pool, mine, 1, at_near, near_device).start()
        cross(pool, mine, 3)

    pieces = xa_ssem.shape[0]
    piece = D // pieces
    sizes = [piece] * (pieces - 1) + [piece + 128]
    pools = [(x_a, old_rows, pl.ds(n * piece, sizes[n]), n) for n in range(pieces)]
    for pool in pools[:-1]:
        first_hops(pool)
    gate = gate_of(normed)
    high = gate.astype(bf16)
    x_a[mine, :, D:] = jnp.where(
        lax.broadcasted_iota(jnp.int32, (seqs, 128), 1) < 128 // 2,
        high.astype(f32),
        gate - high.astype(f32),
    ).astype(bf16)
    first_hops(pools[-1])

    prompts = owners.shape[0]
    shape = (1, prompts * PAGE_TOKENS)
    prompt_of = lax.broadcasted_iota(jnp.int32, shape, 1) // PAGE_TOKENS
    owner_of, length_of = jnp.zeros(shape, jnp.int32), jnp.zeros(shape, jnp.int32)
    for p in range(prompts):
        owner_of = jnp.where(prompt_of == p, owners[p], owner_of)
        length_of = jnp.where(prompt_of == p, prompt_lengths[p], length_of)
    rank_of = jnp.zeros(shape, jnp.int32)
    for p in range(prompts):
        rank_of = rank_of + jnp.where((owner_of == owners[p]) & (prompt_of > p), 1, 0)
    slots = chips * seqs
    at_row = lax.broadcasted_iota(jnp.int32, (slots, 1), 0)
    row_unit = at_row // seqs
    row_owner = device_of(row_unit, 1 - core)
    match = (owner_of == row_owner) & (rank_of == lax.rem(at_row, MAXP))

    def allowed_at(position):
        ok = match & (length_of > position)
        return jnp.concatenate([jnp.where(ok, 1.0, 0.0)] * per_kv, 0)

    allowed = (allowed_at(me), allowed_at(other_core))
    page_copy.wait_recv()

    q_all = remote(q_recv, q_recv, q_sem.at[0], q_sem.at[1], other_core)
    q_all.wait_recv()
    wide_kv = per_kv * HEAD_SIZE

    def o_copy(to, h):
        cols = pl.ds(h * wide_kv, wide_kv)
        return remote(
            o_send.at[to, :, cols],
            o_recv.at[unit, :, cols],
            o_sem.at[0],
            o_sem.at[1],
            device_of(to, 1 - core),
        )

    def lse_copy(to):
        at = device_of(to, 1 - core)
        return remote(lse_send.at[to], lse_recv.at[unit], lse_sem.at[0], lse_sem.at[1], at)

    lane_of = lax.broadcasted_iota(jnp.int32, (slots, 128), 1)
    lse_all = jnp.zeros((slots, 128), f32)
    for h in range(KEY_VALUE_HEADS):
        at = head_cols(h)
        lanes = [h * per_kv + j for j in range(per_kv)]
        queries = jnp.concatenate(
            [q_recv[:, :, head_cols(hh)].reshape(slots, HEAD_SIZE) for hh in lanes], 0
        )
        scores = []
        for ref, ok in zip((pages_ref, other_pages), allowed):
            keys = ref[:, 0, :, at].reshape(prompts * PAGE_TOKENS, HEAD_SIZE)
            scores.append(jnp.where(ok > 0, dot_t(queries, keys) * scale, masked_score))
        peak = jnp.maximum(
            jnp.max(scores[0], -1, keepdims=True), jnp.max(scores[1], -1, keepdims=True)
        )
        total = jnp.zeros((slots * per_kv, 1), f32)
        mixed = jnp.zeros((slots * per_kv, HEAD_SIZE), f32)
        for ref, score in zip((pages_ref, other_pages), scores):
            weight = jnp.exp(score - peak)
            total = total + jnp.sum(weight, -1, keepdims=True)
            values = ref[:, 1, :, at].reshape(prompts * PAGE_TOKENS, HEAD_SIZE)
            mixed = mixed + jnp.dot(weight.astype(bf16), values, preferred_element_type=f32)
        mixed = mixed / total
        lse = jnp.where(peak > masked_score, peak + jnp.log(total), masked_score)
        for j, hh in enumerate(lanes):
            rows = slice(j * slots, (j + 1) * slots)
            o_send[:, :, head_cols(hh)] = mixed[rows].astype(bf16).reshape(chips, seqs, HEAD_SIZE)
            lse_all = jnp.where(lane_of == hh, lse[rows], lse_all)
        for to in all_units():
            o_copy(to, h).start()
    lse_send[...] = lse_all.reshape(chips, seqs, 128)

    for to in all_units():
        lse_copy(to).start()

    for pool in pools:
        z_arrive(pool, at_far)
    for pool in pools:
        z_arrive(pool, at_near)
    for pool in pools:
        y_arrive(pool, 3)
    for pool in pools:
        z_arrive(pool, at_relay)

    own_both = dkv_ref[...].astype(f32)
    own_key = spread_rows(own_both[:, 0])
    own_value = spread_rows(own_both[:, 1])
    lane = lax.broadcasted_iota(jnp.int32, (seqs, 128), 1)
    own_score = jnp.zeros((seqs, 128), f32)
    for hh in range(lane_heads):
        score = jnp.sum(
            q_packed[:, head_cols(hh)] * own_key[:, head_cols(hh // per_kv)], -1, keepdims=True
        )
        own_score = jnp.where(lane == hh, score * scale, own_score)
    new_count = jnp.int32(0)
    for p in range(prompts):
        new_count = new_count + (owners[p] == me).astype(jnp.int32)
    is_new = lax.broadcasted_iota(jnp.int32, (seqs, HEAD_SIZE), 0) < new_count

    o_all = (
        remote(o_recv, o_recv, o_sem.at[0], o_sem.at[1], other_core),
        remote(lse_recv, lse_recv, lse_sem.at[0], lse_sem.at[1], other_core),
    )
    for copy in o_all:
        copy.wait_recv()
    peak = own_score
    for u in range(chips):
        peak = jnp.maximum(peak, lse_recv[u])
    shares = [jnp.exp(lse_recv[u] - peak) for u in range(chips)]
    own_share = jnp.exp(own_score - peak)
    total = own_share
    for share in shares:
        total = total + share
    inverse = 1.0 / total
    shares = [share * inverse for share in shares]
    own_share = own_share * inverse
    for hh in range(lane_heads):
        at = head_cols(hh)
        mixed = own_share[:, hh : hh + 1] * own_value[:, head_cols(hh // per_kv)]
        for u in range(chips):
            mixed = mixed + shares[u][:, hh : hh + 1] * o_recv[u, :, at].astype(f32)
        for f in range(fold):
            cols = head_cols(fold * hh + f)
            attn[:, cols] = jnp.where(is_new, turn(mixed, -MAXP * f), attn[:, cols])
    wide = residual_of(attn[...])
    attn[...] = wide
    normed = norm_of(wide)
    x_b[mine] = normed

    b_pools = [(x_b, new_rows, 0), (gates_b, pl.ds(0, seqs), 1)]

    def b_copy(pool, to):
        buffer, rows, n = pool
        ref = buffer.at[mine, rows]
        return remote(ref, ref, xb_ssem.at[n], xb_rsem.at[n, 0], device_of(to, 1 - core))

    def b_core_copy(pool, spot, count):
        buffer, rows, n = pool
        ref = buffer.at[pl.ds(spot, count), rows]
        return remote(ref, ref, xb_ssem.at[n], xb_rsem.at[n, 1], other_core)

    def b_first(pool):
        for to in other_units():
            b_copy(pool, to).start()
        b_core_copy(pool, mine, 1).start()

    def b_pass(pool):
        buffer, rows, n = pool
        ref = buffer.at[pl.ds(0, chips - 1), rows]
        remote(ref, ref, xb_ssem.at[n], xb_rsem.at[n, 0], other_core).wait_recv()
        for source in other_units():
            b_core_copy(pool, (1 - core) * chips + source, 1).start()

    b_first(b_pools[0])
    gates_b[mine] = gate_of(normed)
    b_first(b_pools[1])

    for copy in weights:
        copy.wait()

    def activate(both, gate, parts):
        lanes_of = lax.broadcasted_iota(jnp.int32, (total, 128), 1)
        gate_proj, up_proj = both[:, :hidden], both[:, hidden:]
        kept_lanes = lanes_of == me // 2
        if parts == 2:
            kept_lanes = kept_lanes | (lanes_of == 128 // 2 + me // 2)
        scaled = jnp.sum(jnp.where(kept_lanes, gate, 0.0), -1, keepdims=True)
        return (gate_proj / (1.0 + jnp.exp(-gate_proj)) * up_proj * scaled).astype(bf16)

    total = devices * seqs

    def rows_of(ref):
        return ref[...].reshape(total, ref.shape[2])

    chunks = c_rsem.shape[0]
    ends = (0, D // 4, D // 2, 3 * D // 4, D)
    z_chunks = zf_rsem.shape[0]
    half = ends[z_chunks]

    def late(i):
        return slice(ends[i] - half, ends[i + 1] - half)

    def cut(i):
        return slice(ends[i], ends[i + 1])

    def core_copy(i):
        return remote(
            part_a.at[1 - core, :, :, old_rows, cut(i)],
            core_a.at[:, :, old_rows, cut(i)],
            c_ssem,
            c_rsem.at[i],
            other_core,
        )

    def row_copy(i):
        return remote(
            y_send.at[:, old_rows, late(i)],
            y_recv.at[:, old_rows, late(i)],
            y_ssem,
            y_rsem.at[i - z_chunks],
            other_row,
        )

    def line_copy(i, k):
        to = lax.rem(line + k, lines)
        return remote(
            z_send.at[k, old_rows, late(i)],
            z_recv.at[k, old_rows, late(i)],
            z_sem.at[0],
            z_sem.at[1],
            device(to, row, core),
        )

    for n in range(2):
        for pool in pools:
            y_arrive(pool, n)
    for pool in pools:
        y_arrive(pool, 2)

    def core_arrive(pool):
        pass_on(pool, (1 - core) * chips, chips, at_core, other_core).wait_recv()

    both = jnp.zeros((total, 2 * hidden), f32)
    for n in range(pieces):
        core_arrive(pools[n])
        cols = slice(n * piece, (n + 1) * piece)
        x = x_a[:, :, cols].reshape(total, piece)
        both = both + jnp.dot(x, w_in[cols], preferred_element_type=f32)
    activated = activate(both, x_a[:, :, D:].reshape(total, 128).astype(f32), 2)

    def zf_copy(i, k):
        to = lax.rem(line + k, lines)
        return remote(
            zf_send.at[k, :, old_rows, cut(i)],
            zf_recv.at[k, :, old_rows, cut(i)],
            zf_ssem,
            zf_rsem.at[i],
            device(to, row, core),
        )

    def held_by(at_row, at_line, i):
        return part_a[core, at_row, at_line, :, cut(i)].astype(f32) + core_a[
            at_row, at_line, :, cut(i)
        ].astype(f32)

    def zf_step(i):
        core_copy(i).wait_recv()
        for k in (2, 1, 3):
            for at_row in range(2):
                zf_send[k, at_row, :, cut(i)] = held_by(
                    at_row, lax.rem(line + k, lines), i
                ).astype(bf16)
            zf_copy(i, k).start()

    def yf_copy():
        return remote(
            yf_send.at[old_rows], yf_recv.at[old_rows], yf_sem.at[0], yf_sem.at[1], other_row
        )

    def yf_step(i):
        ref = zf_recv.at[pl.ds(1, lines - 1), :, old_rows, cut(i)]
        remote(ref, ref, zf_ssem, zf_rsem.at[i], other_core).wait_recv()

        def summed(at_row):
            total = held_by(at_row, line, i)
            for k in range(1, lines):
                total = total + zf_recv[k, at_row, :, cut(i)].astype(f32)
            return total

        yf_send[:, cut(i)] = summed(1 - row).astype(bf16)
        kept[:, cut(i)] = attn[:, cut(i)] + summed(row)

    def row_step(i):
        if i < z_chunks:
            zf_step(i)
            return
        core_copy(i).wait_recv()
        y_send[:, :, late(i)] = (
            part_a[core, 1 - row, :, :, cut(i)].astype(f32)
            + core_a[1 - row, :, :, cut(i)].astype(f32)
        ).astype(bf16)
        row_copy(i).start()

    behind = 2
    for i in range(chunks):
        rows = jnp.dot(activated, w_down[:, cut(i)], preferred_element_type=f32)
        part_a[:, :, :, :, cut(i)] = rows.astype(bf16).reshape(
            2, 2, lines, seqs, ends[i + 1] - ends[i]
        )
        core_copy(i).start()
        if i == 1:
            for pool in b_pools:
                b_pass(pool)
        if i >= behind:
            row_step(i - behind)
    for i in range(chunks - behind, chunks):
        row_step(i)

    for pool in b_pools:
        b_core_copy(pool, 0, chips).wait_recv()
    both = jnp.dot(rows_of(x_b), w_in[...], preferred_element_type=f32)
    activated = activate(both, rows_of(gates_b), 1)
    b_chunks = cb_rsem.shape[0]
    b_width = D // b_chunks

    def b_core(i):
        at = slice(i * b_width, (i + 1) * b_width)
        return remote(
            part_b.at[core, :, new_rows, at],
            core_b.at[:, new_rows, at],
            cb_ssem,
            cb_rsem.at[i],
            other_core,
        )

    for i in range(b_chunks):
        at = slice(i * b_width, (i + 1) * b_width)
        rows = jnp.dot(activated, w_down[:, at], preferred_element_type=f32)
        part_b[:, :, :, at] = rows.astype(bf16).reshape(2, chips, seqs, b_width)
        b_core(i).start()

    def b_return(to):
        return remote(
            sum_b.at[to, new_rows],
            recv_b.at[unit, new_rows],
            rb_sem.at[0],
            rb_sem.at[1],
            device_of(to, 1 - core),
        )

    def line_step(i):
        row_copy(i).wait_recv()

        def summed(at_line):
            return (
                part_a[core, row, at_line, :, cut(i)].astype(f32)
                + core_a[row, at_line, :, cut(i)].astype(f32)
                + y_recv[at_line, :, late(i)].astype(f32)
            )

        for k in range(1, lines):
            z_send[k, :, late(i)] = summed(lax.rem(line + k, lines)).astype(bf16)
            line_copy(i, k).start()
        kept[:, cut(i)] = attn[:, cut(i)] + summed(line)

    early = chunks - 1
    for i in range(z_chunks, early):
        line_step(i)
    for i in range(b_chunks):
        b_core(i).wait_recv()
    for to in all_units():
        sum_b[to] = (part_b[1 - core, to].astype(f32) + core_b[to].astype(f32)).astype(bf16)
        b_return(to).start()
    for i in range(early, chunks):
        line_step(i)
    for i in range(z_chunks):
        yf_step(i)
    yf_copy().start()

    rest = pl.ds(1, lines - 1)
    z_all = remote(
        z_recv.at[rest, old_rows], z_recv.at[rest, old_rows], z_sem.at[0], z_sem.at[1], other_core
    )
    z_all.wait_recv()
    answer = kept[:, half:]
    for k in range(1, lines):
        answer = answer + z_recv[k].astype(f32)
    yf_copy().wait_recv()
    answer = jnp.concatenate([kept[:, :half] + yf_recv[...].astype(f32), answer], 1)

    b_all = remote(
        recv_b.at[:, new_rows], recv_b.at[:, new_rows], rb_sem.at[0], rb_sem.at[1], other_core
    )
    b_all.wait_recv()
    last = attn[...]
    for u in range(chips):
        last = last + recv_b[u].astype(f32)
    is_b = lax.broadcasted_iota(jnp.int32, (seqs, D), 0) < MAXP
    out_ref[...] = jnp.where(is_b, last, answer).astype(bf16)

    for copy in (page_copy, q_all, z_all, b_all, yf_copy()) + o_all:
        copy.wait_send()
    for pool in pools:
        pass_on(pool, 0, 4 * lines - 1, 0, other_core).wait_send()
    for n, (buffer, rows) in enumerate(((x_b, new_rows), (gates_b, pl.ds(0, seqs)))):
        ref = buffer.at[pl.ds(0, 2 * chips - 1), rows]
        remote(ref, ref, xb_ssem.at[n], xb_rsem.at[n, 0], other_core).wait_send()
    for ref, ssem, rsem in (
        (part_a.at[0, :, :, old_rows], c_ssem, c_rsem.at[0]),
        (y_send.at[:, old_rows], y_ssem, y_rsem.at[0]),
        (zf_send.at[pl.ds(1, lines - 1), :, old_rows], zf_ssem, zf_rsem.at[0]),
        (part_b.at[0, :, new_rows], cb_ssem, cb_rsem.at[0]),
    ):
        remote(ref, ref, ssem, rsem, other_core).wait_send()


def dense(
    hidden_in,
    queries,
    decode_key_value,
    local_kv,
    page_table,
    seq_blocks,
    prompt_kv,
    prompt_owner,
    prompt_pages,
    norm_gain,
    router,
    w_gate,
    w_up,
    w_down,
    route_ids,
):
    devices = lax.axis_size("expert")
    seqs = hidden_in.shape[0]
    hidden = w_gate.shape[2]
    lines = devices // 4
    chips = devices // 2
    bf16, f32 = jnp.bfloat16, jnp.float32
    chunks, z_chunks = 4, 2
    pieces = 2
    b_chunks = 2
    packed = D * MAXP // seqs
    loaded = (
        prompt_kv[0],
        queries,
        decode_key_value,
        page_table,
        local_kv,
        hidden_in,
        norm_gain[None, :],
        router.T,
        route_ids,
    )
    scalars = (prompt_owner, prompt_pages, seq_blocks)
    hbm = pl.BlockSpec(memory_space=pltpu.HBM)
    dma = pltpu.SemaphoreType.DMA
    return pl.pallas_call(
        functools.partial(layer_kernel, devices),
        out_shape=pltpu.VMEM((seqs, D), bf16),
        in_specs=[hbm] * (len(loaded) + 6),
        out_specs=pl.BlockSpec(memory_space=pltpu.VMEM),
        scratch_shapes=[pltpu.SMEM(a.shape, a.dtype) for a in scalars]
        + [pltpu.VMEM(a.shape, a.dtype) for a in loaded]
        + [
            pltpu.VMEM((D, 2 * hidden), bf16),
            pltpu.VMEM((hidden, D), bf16),
            pltpu.VMEM(loaded[0].shape, bf16),
            pltpu.VMEM((seqs, packed), bf16),
            pltpu.VMEM((chips, seqs, packed), bf16),
            pltpu.VMEM((chips, seqs, packed), bf16),
            pltpu.VMEM((chips, seqs, packed), bf16),
            pltpu.VMEM((chips, seqs, 128), f32),
            pltpu.VMEM((chips, seqs, 128), f32),
            pltpu.VMEM((seqs, D), f32),
            pltpu.VMEM((devices, seqs, D + 128), bf16),
            pltpu.VMEM((devices, seqs, D), bf16),
            pltpu.VMEM((devices, seqs, 128), f32),
            pltpu.VMEM((2, 2, lines, seqs, D), bf16),
            pltpu.VMEM((2, lines, seqs, D), bf16),
            pltpu.VMEM((lines, seqs, D // 2), bf16),
            pltpu.VMEM((lines, seqs, D // 2), bf16),
            pltpu.VMEM((lines, seqs, D // 2), bf16),
            pltpu.VMEM((lines, seqs, D // 2), bf16),
            pltpu.VMEM((lines, 2, seqs, D // 2), bf16),
            pltpu.VMEM((lines, 2, seqs, D // 2), bf16),
            pltpu.VMEM((seqs, D // 2), bf16),
            pltpu.VMEM((seqs, D // 2), bf16),
            pltpu.VMEM((seqs, D), f32),
            pltpu.VMEM((2, chips, seqs, D), bf16),
            pltpu.VMEM((chips, seqs, D), bf16),
            pltpu.VMEM((chips, seqs, D), bf16),
            pltpu.VMEM((chips, seqs, D), bf16),
            dma((len(loaded) + len(scalars),)),
            dma((3,)),
            dma((2,)),
            dma((2,)),
            dma((2,)),
            dma((2,)),
            dma((pieces,)),
            dma((pieces, 2 * lines)),
            dma((2,)),
            dma((2, 2)),
            dma(()),
            dma((chunks,)),
            dma(()),
            dma((chunks - z_chunks,)),
            dma((2,)),
            dma(()),
            dma((z_chunks,)),
            dma((2,)),
            dma(()),
            dma((b_chunks,)),
            dma((2,)),
        ],
        compiler_params=pltpu.CompilerParams(
            collective_id=0, has_side_effects=True, vmem_limit_bytes=58 * 2**20
        ),
    )(*scalars, *loaded, w_gate, w_up, w_down)


def local(*arrays):
    devices = lax.axis_size("expert")
    experts = arrays[10].shape[1]
    if experts == TOPK and devices == 2 * experts and devices % 4 == 0:
        return dense(*arrays)
    return routed(*arrays)


def solution(mesh):
    return jax.shard_map(
        local,
        mesh=mesh,
        in_specs=(
            P(("groups", "expert"), None),
            P(("groups", "expert"), None),
            P(("groups", "expert"), None, None),
            P(("groups", "expert"), None, None, None),
            P(("groups", "expert"), None),
            P(("groups", "expert")),
            P(("groups", "expert"), None, None, None, None),
            P("groups"),
            P("groups"),
            P(),
            P(),
            P("expert", None, None),
            P("expert", None, None),
            P("expert", None, None),
            P(("groups", "expert"), None),
        ),
        out_specs=P(("groups", "expert"), None),
        check_vma=False,
    )
```

```python
import functools
import math

import jax
import jax.numpy as jnp
from jax import lax
from jax.experimental import pallas as pl
from jax.experimental.pallas import tpu as pltpu
from jax.sharding import PartitionSpec as P

D = 4096
QUERY_HEADS = 32
KEY_VALUE_HEADS = 2
HEAD_SIZE = 128
PAGE_TOKENS = 16
TOPK = 8
MAXB = 16
MAXP = 2


norm_eps = 1e-06
masked_score = -1e30


def partner(x, axis, apart):
    return lax.ppermute(x, axis, [(i, i ^ 1 << apart) for i in range(lax.axis_size(axis))])


def attend(rows_of_queries, rows_of_keys, rows_of_values, allowed, token_own_key, token_own_value):
    decode_tokens = rows_of_queries.shape[0]
    heads_of_queries = rows_of_queries.reshape(
        decode_tokens, KEY_VALUE_HEADS, QUERY_HEADS // KEY_VALUE_HEADS, HEAD_SIZE
    )
    heads_of_keys = rows_of_keys.reshape(decode_tokens, -1, KEY_VALUE_HEADS, HEAD_SIZE)
    heads_of_values = rows_of_values.reshape(decode_tokens, -1, KEY_VALUE_HEADS, HEAD_SIZE)
    scale_for_scores = 1.0 / math.sqrt(HEAD_SIZE)
    allowed_mask = allowed[:, None, None, :]
    scores = (
        jnp.einsum(
            "tkgd,tlkd->tkgl", heads_of_queries, heads_of_keys, preferred_element_type=jnp.float32
        )
        * scale_for_scores
    )
    scores = jnp.where(allowed_mask, scores, masked_score)
    token_own_score = (
        jnp.einsum(
            "xejp,xep->xej",
            heads_of_queries,
            token_own_key.reshape(decode_tokens, KEY_VALUE_HEADS, HEAD_SIZE),
            preferred_element_type=jnp.float32,
        )
        * scale_for_scores
    )
    peak = jnp.maximum(jnp.max(scores, -1), token_own_score)
    weights = jnp.where(allowed_mask, jnp.exp(scores - peak[..., None]), 0.0)
    own_weight = jnp.exp(token_own_score - peak)
    denominator = jnp.sum(weights, -1) + own_weight
    probs = (weights / denominator[..., None]).astype(jnp.bfloat16)
    token_own_probability = (own_weight / denominator).astype(jnp.bfloat16)
    blended_noise = jnp.einsum(
        "tkgl,tlkd->tkgd", probs, heads_of_values, preferred_element_type=jnp.float32
    )
    blended_noise = blended_noise + token_own_probability.astype(jnp.float32)[
        ..., None
    ] * token_own_value.reshape(decode_tokens, KEY_VALUE_HEADS, 1, HEAD_SIZE).astype(jnp.float32)
    return blended_noise.reshape(decode_tokens, QUERY_HEADS * HEAD_SIZE).astype(jnp.bfloat16)


def routed(
    hidden_in,
    queries,
    decode_key_value,
    local_kv,
    page_table,
    seq_blocks,
    prompt_kv,
    prompt_owner,
    prompt_pages,
    norm_gain,
    router,
    w_gate,
    w_up,
    w_down,
    route_ids,
):
    devices = lax.axis_size("expert")
    position = lax.axis_index("expert")
    experts = devices // 2
    seq_dev = hidden_in.shape[0]
    key_value_width = KEY_VALUE_HEADS * HEAD_SIZE
    capacity = min(seq_dev, max(2, 2 * ((3 * seq_dev * TOPK + 2 * devices - 1) // (2 * devices))))
    half_cap = capacity // 2
    even_core = position % 2 == 0
    prompt_count = prompt_owner.shape[0]
    prompt_range = jnp.arange(prompt_count, dtype=jnp.int32)
    same_owner = prompt_owner[:, None] == prompt_owner[None, :]
    earlier = prompt_range[None, :] < prompt_range[:, None]
    arrival = jnp.sum((same_owner & earlier).astype(jnp.int32), 1)
    matching = (
        prompt_owner[None, None, :] == jnp.arange(devices, dtype=jnp.int32)[:, None, None]
    ) & (arrival[None, None, :] == jnp.arange(MAXP, dtype=jnp.int32)[None, :, None])
    chosen_prompt = jnp.sum(jnp.where(matching, prompt_range[None, None, :], 0), -1)
    occupied = jnp.any(matching, -1)
    own_picks = lax.dynamic_index_in_dim(chosen_prompt, position, 0, keepdims=False)
    own_occupied = lax.dynamic_index_in_dim(occupied, position, 0, keepdims=False)
    page_rows = prompt_kv[0]
    outgoing = jnp.take(page_rows, chosen_prompt.T.reshape(-1), axis=0).reshape(
        MAXP, devices, 2, PAGE_TOKENS, key_value_width
    )
    outgoing = jnp.where(occupied.T[:, :, None, None, None], outgoing, 0)
    arrived = lax.all_to_all(outgoing, "expert", split_axis=1, concat_axis=1, tiled=True)
    lengths = jnp.take(prompt_pages, own_picks)
    new_keys = arrived[:, :, 0].reshape(MAXP, devices * PAGE_TOKENS, key_value_width)
    new_values = arrived[:, :, 1].reshape(MAXP, devices * PAGE_TOKENS, key_value_width)
    new_allowed = (jnp.arange(devices * PAGE_TOKENS, dtype=jnp.int32) // PAGE_TOKENS)[
        None, :
    ] < lengths[:, None]
    fresh_rows = attend(
        queries[:MAXP],
        new_keys,
        new_values,
        new_allowed,
        decode_key_value[:MAXP, 0],
        decode_key_value[:MAXP, 1],
    )
    fetched = local_kv[page_table]
    old_keys = fetched[:, :, 0].reshape(seq_dev, MAXB * PAGE_TOKENS, key_value_width)
    old_values = fetched[:, :, 1].reshape(seq_dev, MAXB * PAGE_TOKENS, key_value_width)
    old_allowed = (jnp.arange(MAXB * PAGE_TOKENS, dtype=jnp.int32) // PAGE_TOKENS)[
        None, :
    ] < seq_blocks[:, None]
    old_out = attend(
        queries, old_keys, old_values, old_allowed, decode_key_value[:, 0], decode_key_value[:, 1]
    )
    new_count = jnp.sum(own_occupied.astype(jnp.int32))
    is_new = jnp.arange(MAXP, dtype=jnp.int32) < new_count
    attention = jnp.concatenate(
        [jnp.where(is_new[:, None], fresh_rows, old_out[:MAXP]), old_out[MAXP:]], 0
    )
    residual = (hidden_in.astype(jnp.float32) + attention.astype(jnp.float32)).astype(jnp.bfloat16)
    resid_wide = residual.astype(jnp.float32)
    normed = (
        resid_wide
        * lax.rsqrt(jnp.mean(resid_wide * resid_wide, -1, keepdims=True) + norm_eps)
        * norm_gain
    ).astype(jnp.bfloat16)
    logits = jnp.dot(normed, router, preferred_element_type=jnp.float32)
    expert_onehot = route_ids[:, :, None] == jnp.arange(experts, dtype=jnp.int32)[None, None, :]
    selected = jnp.sum(jnp.where(expert_onehot, logits[:, None, :], 0.0), -1)
    gate_weights = jax.nn.softmax(selected, -1)
    assigned = seq_dev * TOPK
    expert_ids = route_ids.reshape(assigned)
    chosen = (expert_ids[:, None] == jnp.arange(experts, dtype=jnp.int32)[None, :]).astype(
        jnp.int32
    )
    before = jnp.cumsum(chosen, 0) - chosen
    slot_rank = jnp.sum(before * chosen, 1)
    slot_index = expert_ids * capacity + slot_rank
    placing = slot_index[None, :] == jnp.arange(experts * capacity, dtype=jnp.int32)[:, None]
    selector = jnp.any(placing.reshape(experts * capacity, seq_dev, TOPK), -1).astype(jnp.bfloat16)
    gathered_rows = jnp.dot(selector, normed, preferred_element_type=jnp.float32).astype(
        jnp.bfloat16
    )
    outgoing_half = gathered_rows.reshape(devices, half_cap, D)
    own_half = lax.all_to_all(outgoing_half, "expert", split_axis=0, concat_axis=0, tiled=True)
    partner_half = partner(own_half, "expert", 0)
    received = jnp.where(
        even_core,
        jnp.concatenate([own_half, partner_half], 1),
        jnp.concatenate([partner_half, own_half], 1),
    )
    flattened = received.reshape(devices * capacity, D)
    gate_proj = jnp.dot(flattened, w_gate[0], preferred_element_type=jnp.float32)
    up_proj = jnp.dot(flattened, w_up[0], preferred_element_type=jnp.float32)
    activated = (jax.nn.silu(gate_proj) * up_proj).astype(jnp.bfloat16)
    partial_value = jnp.dot(activated, w_down[0], preferred_element_type=jnp.float32).reshape(
        devices, capacity, D
    )
    kept = jnp.where(even_core, partial_value[:, :half_cap], partial_value[:, half_cap:])
    handed = jnp.where(even_core, partial_value[:, half_cap:], partial_value[:, :half_cap])
    partner_part = partner(handed, "expert", 0)
    finished = (kept + partner_part).astype(jnp.bfloat16)
    returned = lax.all_to_all(finished, "expert", split_axis=0, concat_axis=0, tiled=True)
    expert_sum = returned.reshape(experts * capacity, D)
    picked = jnp.take(expert_sum, slot_index, axis=0).astype(jnp.float32).reshape(seq_dev, TOPK, D)
    expert_mix = jnp.sum(picked * gate_weights[:, :, None], 1)
    return (resid_wide + expert_mix).astype(jnp.bfloat16)


def layer_kernel(
    devices,
    owners_hbm,
    lengths_hbm,
    blocks_hbm,
    pages_hbm,
    q_hbm,
    dkv_hbm,
    table_hbm,
    kv_hbm,
    hidden_hbm,
    gain_hbm,
    router_hbm,
    ids_hbm,
    gate_hbm,
    up_hbm,
    down_hbm,
    out_ref,
    owners,
    prompt_lengths,
    blocks,
    pages_ref,
    q_ref,
    dkv_ref,
    table_ref,
    kv_ref,
    hidden_ref,
    gain_ref,
    router_ref,
    ids_ref,
    w_in,
    w_down,
    other_pages,
    q_send,
    q_recv,
    o_send,
    o_recv,
    lse_send,
    lse_recv,
    attn,
    x_a,
    x_b,
    gates_b,
    part_a,
    core_a,
    z_send,
    z_recv,
    y_send,
    y_recv,
    kept,
    part_b,
    core_b,
    sum_b,
    recv_b,
    in_sem,
    w_sem,
    page_sem,
    q_sem,
    o_sem,
    lse_sem,
    xa_ssem,
    xa_rsem,
    xb_ssem,
    xb_rsem,
    c_ssem,
    c_rsem,
    z_ssem,
    z_rsem,
    y_ssem,
    y_rsem,
    cb_ssem,
    cb_rsem,
    rb_sem,
):
    f32, bf16 = jnp.float32, jnp.bfloat16
    me = lax.axis_index("expert")
    lines = devices // 4
    chips = devices // 2
    core, row, line = lax.rem(me, 2), lax.rem(me // 2, 2), me // 4
    unit = row * lines + line
    seqs = hidden_ref.shape[0]
    group = QUERY_HEADS // KEY_VALUE_HEADS
    scale = 1.0 / math.sqrt(HEAD_SIZE)
    old_rows = pl.ds(MAXP, seqs - MAXP)
    new_rows = pl.ds(0, MAXP)

    def device(at_line, at_row, at_core):
        return (at_line * 2 + at_row) * 2 + at_core

    def device_of(at_unit, at_core):
        return device(lax.rem(at_unit, lines), at_unit // lines, at_core)

    def place(at_line, at_row, at_core):
        return (at_core * 2 + at_row) * lines + at_line

    low = line * 2 < lines

    def far_line(j):
        return jnp.where(low, lines - 1 - j, j)

    def far_other_line(j):
        down = lines - 1 - j
        return jnp.where(
            low, jnp.where(down > line, down, down - 1), jnp.where(j < line, j, j + 1)
        )

    def all_units():
        yield from other_units()
        yield unit

    def other_units():
        for j in range(lines):
            yield (1 - row) * lines + far_line(j)
            if j < lines - 1:
                yield row * lines + far_other_line(j)

    def remote(src, dst, ssem, rsem, to):
        return pltpu.make_async_remote_copy(
            src_ref=src,
            dst_ref=dst,
            send_sem=ssem,
            recv_sem=rsem,
            device_id={"expert": to},
            device_id_type=pl.DeviceIdType.MESH,
        )

    other_row = device(line, 1 - row, core)
    other_core = device(line, row, 1 - core)
    mine = place(line, row, core)

    loads = [
        pltpu.make_async_copy(a, b, in_sem.at[i])
        for i, (a, b) in enumerate(
            (
                (q_hbm, q_ref),
                (pages_hbm, pages_ref),
                (dkv_hbm, dkv_ref),
                (table_hbm, table_ref),
                (kv_hbm, kv_ref),
                (hidden_hbm, hidden_ref),
                (gain_hbm, gain_ref),
                (router_hbm, router_ref),
                (ids_hbm, ids_ref),
                (blocks_hbm, blocks),
                (owners_hbm, owners),
                (lengths_hbm, prompt_lengths),
            )
        )
    ]
    hidden = w_down.shape[0]
    weights = [
        pltpu.make_async_copy(gate_hbm.at[0], w_in.at[:, pl.ds(0, hidden)], w_sem.at[0]),
        pltpu.make_async_copy(up_hbm.at[0], w_in.at[:, pl.ds(hidden, hidden)], w_sem.at[1]),
        pltpu.make_async_copy(down_hbm.at[0], w_down, w_sem.at[2]),
    ]
    barrier = pltpu.get_barrier_semaphore()

    def greet(k, carry):
        pl.semaphore_signal(
            barrier,
            inc=1,
            device_id={"expert": lax.rem(me + k, devices)},
            device_id_type=pl.DeviceIdType.MESH,
        )
        return carry

    lax.fori_loop(1, devices, greet, 0)
    for copy in loads + weights:
        copy.start()

    fold = seqs // MAXP
    lane_heads = QUERY_HEADS // fold
    packed = lane_heads * HEAD_SIZE
    per_kv = lane_heads // KEY_VALUE_HEADS
    sub = lax.broadcasted_iota(jnp.int32, (seqs, packed), 0) // MAXP

    def head_cols(h):
        return slice(h * HEAD_SIZE, (h + 1) * HEAD_SIZE)

    def turn(x, by):
        by = by % seqs
        return x if by == 0 else pltpu.roll(x, by, 0)

    def pack(rows):
        out = None
        for f in range(fold):
            wide = turn(
                jnp.concatenate([rows[:, head_cols(fold * hh + f)] for hh in range(lane_heads)], 1),
                MAXP * f,
            )
            out = wide if f == 0 else jnp.where(sub == f, wide, out)
        return out

    def spread_rows(rows):
        out = rows
        at = lax.broadcasted_iota(jnp.int32, rows.shape, 0) // MAXP
        for f in range(1, fold):
            out = jnp.where(at == f, turn(rows, MAXP * f), out)
        return out

    def dot_t(a, b):
        return lax.dot_general(a, b, (((1,), (1,)), ((), ())), preferred_element_type=f32)

    loads[0].wait()
    q_packed = pack(q_ref[...].astype(f32))
    q_send[...] = q_packed.astype(bf16)
    for copy in loads[2:]:
        copy.wait()

    def per_seq(values, shape):
        at = lax.broadcasted_iota(jnp.int32, shape, 0)
        return sum(jnp.where(at == s, v, 0) for s, v in enumerate(values))

    tokens = kv_ref.shape[0] * PAGE_TOKENS
    limit = per_seq([blocks[s] for s in range(seqs)], (seqs, tokens))
    page_of = lax.broadcasted_iota(jnp.int32, (seqs, tokens), 1) // PAGE_TOKENS
    held = jnp.zeros((seqs, tokens), f32)
    for b in range(table_ref.shape[1]):
        hit = (page_of == table_ref[:, b : b + 1]) & (limit > b)
        held = held + jnp.where(hit, 1.0, 0.0)
    held = jnp.concatenate([held] * group, 0)

    def heads(h):
        rows = q_ref[...].astype(f32)
        return jnp.concatenate([rows[:, head_cols(h * group + g)] for g in range(group)], 0)

    def own(h, at):
        both = dkv_ref[...].astype(f32)
        return jnp.concatenate([both[:, at, head_cols(h)]] * group, 0)

    def weigh(scores, times, own_score):
        scores = jnp.where(times > 0, scores, masked_score)
        peak = jnp.maximum(jnp.max(scores, -1, keepdims=True), own_score)
        weight = times * jnp.exp(scores - peak)
        own_weight = jnp.exp(own_score - peak)
        total = jnp.sum(weight, -1, keepdims=True) + own_weight
        return (weight / total).astype(bf16), (own_weight / total).astype(bf16).astype(f32)

    for h in range(KEY_VALUE_HEADS):
        at = head_cols(h)
        queries = heads(h)
        own_score = jnp.sum(queries * own(h, 0), -1, keepdims=True) * scale
        keys = kv_ref[:, 0, :, at].reshape(tokens, HEAD_SIZE)
        values = kv_ref[:, 1, :, at].reshape(tokens, HEAD_SIZE)
        probs, own_prob = weigh(dot_t(queries.astype(bf16), keys) * scale, held, own_score)
        mixed = jnp.dot(probs, values, preferred_element_type=f32) + own_prob * own(h, 1)
        for g in range(group):
            attn[:, head_cols(h * group + g)] = mixed[g * seqs : (g + 1) * seqs]

    def residual_of(attention):
        rounded = attention.astype(bf16).astype(f32)
        return (hidden_ref[...].astype(f32) + rounded).astype(bf16).astype(f32)

    def norm_of(wide):
        mean = jnp.mean(wide * wide, -1, keepdims=True)
        return (wide * lax.rsqrt(mean + norm_eps) * gain_ref[...]).astype(bf16)

    def gate_of(normed):
        logits = dot_t(normed, router_ref[...])
        experts = logits.shape[1]
        expert_of = lax.broadcasted_iota(jnp.int32, (seqs, experts), 1)
        times = jnp.zeros((seqs, experts), f32)
        for k in range(ids_ref.shape[1]):
            times = times + jnp.where(ids_ref[:, k : k + 1] == expert_of, 1.0, 0.0)
        picked = jnp.where(times > 0, logits, masked_score)
        gate = times * jnp.exp(picked - jnp.max(picked, -1, keepdims=True))
        gate = gate / jnp.sum(gate, -1, keepdims=True)
        return jnp.concatenate([gate] * (128 // experts), 1)

    normed = norm_of(residual_of(attn[...]))
    x_a[mine, :, :D] = normed
    pl.semaphore_wait(barrier, devices - 1)

    def q_copy(to):
        return remote(q_send, q_recv.at[unit], q_sem.at[0], q_sem.at[1], device_of(to, 1 - core))

    for to in all_units():
        q_copy(to).start()
    loads[1].wait()
    page_copy = remote(pages_ref, other_pages, page_sem.at[0], page_sem.at[1], other_core)
    page_copy.start()


    def pass_on(pool, spot, count, at, to):
        buffer, rows, cols, n = pool
        ref = buffer.at[pl.ds(spot, count), rows, cols]
        return remote(ref, ref, xa_ssem.at[n], xa_rsem.at[n, at], to)

    far, near = lax.rem(line + 2, lines), line + 1 - 2 * lax.rem(line, 2)
    far_device, near_device = device(far, row, 1 - core), device(near, row, 1 - core)
    row_device = device(line, 1 - row, 1 - core)
    at_far, at_near, at_relay, at_core = 0, 1, 2, (7, 8)
    sources = (far, near, lax.rem(near + 2, lines), line)
    z_cores, y_cores = (1 - core, 1 - core, core), (core, core, 1 - core, 1 - core)

    def at_y(n):
        return 3 + n

    def cross(pool, spot, n):
        pass_on(pool, spot, 1, at_y(n), row_device).start()
        pass_on(pool, spot, 1, at_core[0], other_core).start()

    def z_arrive(pool, n):
        spot = place(sources[n], row, z_cores[n])
        pass_on(pool, spot, 1, n, other_row).wait_recv()
        if n == at_far:
            pass_on(pool, spot, 1, at_relay, near_device).start()
        cross(pool, spot, n)

    def y_arrive(pool, n):
        spot = place(sources[n], 1 - row, y_cores[n])
        pass_on(pool, spot, 1, at_y(n), other_row).wait_recv()
        pass_on(pool, spot, 1, at_core[1], other_core).start()

    def first_hops(pool):
        pass_on(pool, mine, 1, at_far, far_device).start()
        pass_on(pool, mine, 1, at_near, near_device).start()
        cross(pool, mine, 3)

    pieces = xa_ssem.shape[0]
    piece = D // pieces
    sizes = [piece] * (pieces - 1) + [piece + 128]
    pools = [(x_a, old_rows, pl.ds(n * piece, sizes[n]), n) for n in range(pieces)]
    for pool in pools[:-1]:
        first_hops(pool)
    gate = gate_of(normed)
    high = gate.astype(bf16)
    x_a[mine, :, D:] = jnp.where(
        lax.broadcasted_iota(jnp.int32, (seqs, 128), 1) < 128 // 2,
        high.astype(f32),
        gate - high.astype(f32),
    ).astype(bf16)
    first_hops(pools[-1])

    prompts = owners.shape[0]
    shape = (1, prompts * PAGE_TOKENS)
    prompt_of = lax.broadcasted_iota(jnp.int32, shape, 1) // PAGE_TOKENS
    owner_of, length_of = jnp.zeros(shape, jnp.int32), jnp.zeros(shape, jnp.int32)
    for p in range(prompts):
        owner_of = jnp.where(prompt_of == p, owners[p], owner_of)
        length_of = jnp.where(prompt_of == p, prompt_lengths[p], length_of)
    rank_of = jnp.zeros(shape, jnp.int32)
    for p in range(prompts):
        rank_of = rank_of + jnp.where((owner_of == owners[p]) & (prompt_of > p), 1, 0)
    slots = chips * seqs
    at_row = lax.broadcasted_iota(jnp.int32, (slots, 1), 0)
    row_unit = at_row // seqs
    row_owner = device_of(row_unit, 1 - core)
    match = (owner_of == row_owner) & (rank_of == lax.rem(at_row, MAXP))

    def allowed_at(position):
        ok = match & (length_of > position)
        return jnp.concatenate([jnp.where(ok, 1.0, 0.0)] * per_kv, 0)

    allowed = (allowed_at(me), allowed_at(other_core))
    page_copy.wait_recv()

    q_all = remote(q_recv, q_recv, q_sem.at[0], q_sem.at[1], other_core)
    q_all.wait_recv()
    wide_kv = per_kv * HEAD_SIZE

    def o_copy(to, h):
        cols = pl.ds(h * wide_kv, wide_kv)
        return remote(
            o_send.at[to, :, cols],
            o_recv.at[unit, :, cols],
            o_sem.at[0],
            o_sem.at[1],
            device_of(to, 1 - core),
        )

    def lse_copy(to):
        at = device_of(to, 1 - core)
        return remote(lse_send.at[to], lse_recv.at[unit], lse_sem.at[0], lse_sem.at[1], at)

    lane_of = lax.broadcasted_iota(jnp.int32, (slots, 128), 1)
    lse_all = jnp.zeros((slots, 128), f32)
    for h in range(KEY_VALUE_HEADS):
        at = head_cols(h)
        lanes = [h * per_kv + j for j in range(per_kv)]
        queries = jnp.concatenate(
            [q_recv[:, :, head_cols(hh)].reshape(slots, HEAD_SIZE) for hh in lanes], 0
        )
        scores = []
        for ref, ok in zip((pages_ref, other_pages), allowed):
            keys = ref[:, 0, :, at].reshape(prompts * PAGE_TOKENS, HEAD_SIZE)
            scores.append(jnp.where(ok > 0, dot_t(queries, keys) * scale, masked_score))
        peak = jnp.maximum(
            jnp.max(scores[0], -1, keepdims=True), jnp.max(scores[1], -1, keepdims=True)
        )
        total = jnp.zeros((slots * per_kv, 1), f32)
        mixed = jnp.zeros((slots * per_kv, HEAD_SIZE), f32)
        for ref, score in zip((pages_ref, other_pages), scores):
            weight = jnp.exp(score - peak)
            total = total + jnp.sum(weight, -1, keepdims=True)
            values = ref[:, 1, :, at].reshape(prompts * PAGE_TOKENS, HEAD_SIZE)
            mixed = mixed + jnp.dot(weight.astype(bf16), values, preferred_element_type=f32)
        mixed = mixed / total
        lse = jnp.where(peak > masked_score, peak + jnp.log(total), masked_score)
        for j, hh in enumerate(lanes):
            rows = slice(j * slots, (j + 1) * slots)
            o_send[:, :, head_cols(hh)] = mixed[rows].astype(bf16).reshape(chips, seqs, HEAD_SIZE)
            lse_all = jnp.where(lane_of == hh, lse[rows], lse_all)
        for to in all_units():
            o_copy(to, h).start()
    lse_send[...] = lse_all.reshape(chips, seqs, 128)

    for to in all_units():
        lse_copy(to).start()

    for pool in pools:
        z_arrive(pool, at_far)
    for pool in pools:
        z_arrive(pool, at_near)
    for pool in pools:
        y_arrive(pool, 3)
    for pool in pools:
        z_arrive(pool, at_relay)

    own_both = dkv_ref[...].astype(f32)
    own_key = spread_rows(own_both[:, 0])
    own_value = spread_rows(own_both[:, 1])
    lane = lax.broadcasted_iota(jnp.int32, (seqs, 128), 1)
    own_score = jnp.zeros((seqs, 128), f32)
    for hh in range(lane_heads):
        score = jnp.sum(
            q_packed[:, head_cols(hh)] * own_key[:, head_cols(hh // per_kv)], -1, keepdims=True
        )
        own_score = jnp.where(lane == hh, score * scale, own_score)
    new_count = jnp.int32(0)
    for p in range(prompts):
        new_count = new_count + (owners[p] == me).astype(jnp.int32)
    is_new = lax.broadcasted_iota(jnp.int32, (seqs, HEAD_SIZE), 0) < new_count

    o_all = (
        remote(o_recv, o_recv, o_sem.at[0], o_sem.at[1], other_core),
        remote(lse_recv, lse_recv, lse_sem.at[0], lse_sem.at[1], other_core),
    )
    for copy in o_all:
        copy.wait_recv()
    peak = own_score
    for u in range(chips):
        peak = jnp.maximum(peak, lse_recv[u])
    shares = [jnp.exp(lse_recv[u] - peak) for u in range(chips)]
    own_share = jnp.exp(own_score - peak)
    total = own_share
    for share in shares:
        total = total + share
    inverse = 1.0 / total
    shares = [share * inverse for share in shares]
    own_share = own_share * inverse
    for hh in range(lane_heads):
        at = head_cols(hh)
        mixed = own_share[:, hh : hh + 1] * own_value[:, head_cols(hh // per_kv)]
        for u in range(chips):
            mixed = mixed + shares[u][:, hh : hh + 1] * o_recv[u, :, at].astype(f32)
        for f in range(fold):
            cols = head_cols(fold * hh + f)
            attn[:, cols] = jnp.where(is_new, turn(mixed, -MAXP * f), attn[:, cols])
    wide = residual_of(attn[...])
    attn[...] = wide
    normed = norm_of(wide)
    x_b[mine] = normed

    b_pools = [(x_b, new_rows, 0), (gates_b, pl.ds(0, seqs), 1)]

    def b_copy(pool, to):
        buffer, rows, n = pool
        ref = buffer.at[mine, rows]
        return remote(ref, ref, xb_ssem.at[n], xb_rsem.at[n, 0], device_of(to, 1 - core))

    def b_core_copy(pool, spot, count):
        buffer, rows, n = pool
        ref = buffer.at[pl.ds(spot, count), rows]
        return remote(ref, ref, xb_ssem.at[n], xb_rsem.at[n, 1], other_core)

    def b_first(pool):
        for to in other_units():
            b_copy(pool, to).start()
        b_core_copy(pool, mine, 1).start()

    def b_pass(pool):
        buffer, rows, n = pool
        ref = buffer.at[pl.ds(0, chips - 1), rows]
        remote(ref, ref, xb_ssem.at[n], xb_rsem.at[n, 0], other_core).wait_recv()
        for source in other_units():
            b_core_copy(pool, (1 - core) * chips + source, 1).start()

    b_first(b_pools[0])
    gates_b[mine] = gate_of(normed)
    b_first(b_pools[1])

    for copy in weights:
        copy.wait()

    def activate(both, gate, parts):
        lanes_of = lax.broadcasted_iota(jnp.int32, gate.shape, 1)
        gate_proj, up_proj = both[:, :hidden], both[:, hidden:]
        kept_lanes = lanes_of == me // 2
        if parts == 2:
            kept_lanes = kept_lanes | (lanes_of == 128 // 2 + me // 2)
        scaled = jnp.sum(jnp.where(kept_lanes, gate, 0.0), -1, keepdims=True)
        return (gate_proj / (1.0 + jnp.exp(-gate_proj)) * up_proj * scaled).astype(bf16)

    total = devices * seqs

    def rows_of(ref):
        return ref[...].reshape(total, ref.shape[2])

    chunks = c_rsem.shape[1]
    ends = (0, D // 4, D // 2, 3 * D // 4, D)

    def cut(i):
        return slice(ends[i], ends[i + 1])

    def core_copy(n, i):
        return remote(
            part_a.at[1 - core, kinds[n], :, old_rows, cut(i)],
            core_a.at[kinds[n], :, old_rows, cut(i)],
            c_ssem,
            c_rsem.at[n, i],
            other_core,
        )

    for n in range(2):
        for pool in pools:
            y_arrive(pool, n)

    def core_arrive(n):
        for pool in pools:
            pass_on(pool, 0, lines, at_core[n], other_core).wait_recv()

    def row_activated(at_row):
        x = jnp.concatenate(
            [
                x_a[pl.ds((at * 2 + at_row) * lines, lines)].reshape(lines * seqs, D + 128)
                for at in range(2)
            ],
            0,
        )
        both = jnp.dot(x[:, :D], w_in[...], preferred_element_type=f32)
        return activate(both, x[:, D:].astype(f32), 2)

    kinds = (row, 1 - row)

    def z_sum_copy(n, i, k):
        to = lax.rem(line + k, lines)
        return remote(
            z_send.at[k, kinds[n], old_rows, cut(i)],
            z_recv.at[k, kinds[n], old_rows, cut(i)],
            z_ssem,
            z_rsem.at[n, i],
            device(to, row, core),
        )

    def y_sum_copy(i):
        return remote(
            y_send.at[old_rows, cut(i)],
            y_recv.at[old_rows, cut(i)],
            y_ssem,
            y_rsem.at[i],
            other_row,
        )

    def held_by(at_row, at_line, i):
        return part_a[core, at_row, at_line, :, cut(i)].astype(f32) + core_a[
            at_row, at_line, :, cut(i)
        ].astype(f32)

    def z_step(n, i):
        core_copy(n, i).wait_recv()
        for k in (2, 1, 3):
            z_send[k, kinds[n], :, cut(i)] = held_by(
                kinds[n], lax.rem(line + k, lines), i
            ).astype(bf16)
            z_sum_copy(n, i, k).start()

    def y_step(i):
        for n in range(2):
            ref = z_recv.at[pl.ds(1, lines - 1), kinds[n], old_rows, cut(i)]
            remote(ref, ref, z_ssem, z_rsem.at[n, i], other_core).wait_recv()

        def summed(at_row):
            value = held_by(at_row, line, i)
            for k in range(1, lines):
                value = value + z_recv[k, at_row, :, cut(i)].astype(f32)
            return value

        y_send[:, cut(i)] = summed(1 - row).astype(bf16)
        y_sum_copy(i).start()
        kept[:, cut(i)] = attn[:, cut(i)] + summed(row)

    def down(n, i, activated):
        rows = jnp.dot(activated, w_down[:, cut(i)], preferred_element_type=f32)
        part_a[:, kinds[n], :, :, cut(i)] = rows.astype(bf16).reshape(
            2, lines, seqs, ends[i + 1] - ends[i]
        )
        core_copy(n, i).start()

    def expert_rows(n, between):
        core_arrive(n)
        activated = row_activated(kinds[n])
        between[0]()
        for i in range(chunks):
            down(n, i, activated)
            if i == 1:
                between[1]()
            if i >= behind:
                z_step(n, i - behind)
        for i in range(chunks - behind, chunks):
            z_step(n, i)

    def finish_gather():
        for pool in pools:
            y_arrive(pool, 2)

    def pass_b():
        for pool in b_pools:
            b_pass(pool)

    def nothing():
        pass

    behind = 2
    expert_rows(0, (finish_gather, nothing))
    expert_rows(1, (nothing, pass_b))

    for pool in b_pools:
        b_core_copy(pool, 0, chips).wait_recv()
    both = jnp.dot(rows_of(x_b), w_in[...], preferred_element_type=f32)
    activated = activate(both, rows_of(gates_b), 1)
    b_chunks = cb_rsem.shape[0]
    b_width = D // b_chunks

    def b_core(i):
        at = slice(i * b_width, (i + 1) * b_width)
        return remote(
            part_b.at[core, :, new_rows, at],
            core_b.at[:, new_rows, at],
            cb_ssem,
            cb_rsem.at[i],
            other_core,
        )

    for i in range(b_chunks):
        at = slice(i * b_width, (i + 1) * b_width)
        rows = jnp.dot(activated, w_down[:, at], preferred_element_type=f32)
        part_b[:, :, :, at] = rows.astype(bf16).reshape(2, chips, seqs, b_width)
        b_core(i).start()

    def b_return(to):
        return remote(
            sum_b.at[to, new_rows],
            recv_b.at[unit, new_rows],
            rb_sem.at[0],
            rb_sem.at[1],
            device_of(to, 1 - core),
        )

    for i in range(b_chunks):
        b_core(i).wait_recv()
    for to in all_units():
        sum_b[to] = (part_b[1 - core, to].astype(f32) + core_b[to].astype(f32)).astype(bf16)
        b_return(to).start()
    for i in range(chunks):
        y_step(i)
    b_all = remote(
        recv_b.at[:, new_rows], recv_b.at[:, new_rows], rb_sem.at[0], rb_sem.at[1], other_core
    )
    b_all.wait_recv()
    last = attn[...]
    for u in range(chips):
        last = last + recv_b[u].astype(f32)
    for i in range(chunks):
        y_sum_copy(i).wait_recv()
    answer = kept[...] + y_recv[...].astype(f32)
    is_b = lax.broadcasted_iota(jnp.int32, (seqs, D), 0) < MAXP
    out_ref[...] = jnp.where(is_b, last, answer).astype(bf16)

    for copy in (page_copy, q_all, b_all) + o_all:
        copy.wait_send()
    for pool in pools:
        pass_on(pool, 0, 4 * lines - 1, 0, other_core).wait_send()
    for n, (buffer, rows) in enumerate(((x_b, new_rows), (gates_b, pl.ds(0, seqs)))):
        ref = buffer.at[pl.ds(0, 2 * chips - 1), rows]
        remote(ref, ref, xb_ssem.at[n], xb_rsem.at[n, 0], other_core).wait_send()
    for ref, ssem, rsem in (
        (part_a.at[0, :, :, old_rows], c_ssem, c_rsem.at[0, 0]),
        (z_send.at[pl.ds(1, lines - 1), :, old_rows], z_ssem, z_rsem.at[0, 0]),
        (y_send.at[old_rows], y_ssem, y_rsem.at[0]),
        (part_b.at[0, :, new_rows], cb_ssem, cb_rsem.at[0]),
    ):
        remote(ref, ref, ssem, rsem, other_core).wait_send()


def dense(
    hidden_in,
    queries,
    decode_key_value,
    local_kv,
    page_table,
    seq_blocks,
    prompt_kv,
    prompt_owner,
    prompt_pages,
    norm_gain,
    router,
    w_gate,
    w_up,
    w_down,
    route_ids,
):
    devices = lax.axis_size("expert")
    seqs = hidden_in.shape[0]
    hidden = w_gate.shape[2]
    lines = devices // 4
    chips = devices // 2
    bf16, f32 = jnp.bfloat16, jnp.float32
    chunks = 4
    pieces = 2
    b_chunks = 2
    packed = D * MAXP // seqs
    loaded = (
        prompt_kv[0],
        queries,
        decode_key_value,
        page_table,
        local_kv,
        hidden_in,
        norm_gain[None, :],
        router.T,
        route_ids,
    )
    scalars = (prompt_owner, prompt_pages, seq_blocks)
    hbm = pl.BlockSpec(memory_space=pltpu.HBM)
    dma = pltpu.SemaphoreType.DMA
    return pl.pallas_call(
        functools.partial(layer_kernel, devices),
        out_shape=pltpu.VMEM((seqs, D), bf16),
        in_specs=[hbm] * (len(loaded) + 6),
        out_specs=pl.BlockSpec(memory_space=pltpu.VMEM),
        scratch_shapes=[pltpu.SMEM(a.shape, a.dtype) for a in scalars]
        + [pltpu.VMEM(a.shape, a.dtype) for a in loaded]
        + [
            pltpu.VMEM((D, 2 * hidden), bf16),
            pltpu.VMEM((hidden, D), bf16),
            pltpu.VMEM(loaded[0].shape, bf16),
            pltpu.VMEM((seqs, packed), bf16),
            pltpu.VMEM((chips, seqs, packed), bf16),
            pltpu.VMEM((chips, seqs, packed), bf16),
            pltpu.VMEM((chips, seqs, packed), bf16),
            pltpu.VMEM((chips, seqs, 128), f32),
            pltpu.VMEM((chips, seqs, 128), f32),
            pltpu.VMEM((seqs, D), f32),
            pltpu.VMEM((devices, seqs, D + 128), bf16),
            pltpu.VMEM((devices, seqs, D), bf16),
            pltpu.VMEM((devices, seqs, 128), f32),
            pltpu.VMEM((2, 2, lines, seqs, D), bf16),
            pltpu.VMEM((2, lines, seqs, D), bf16),
            pltpu.VMEM((lines, 2, seqs, D), bf16),
            pltpu.VMEM((lines, 2, seqs, D), bf16),
            pltpu.VMEM((seqs, D), bf16),
            pltpu.VMEM((seqs, D), bf16),
            pltpu.VMEM((seqs, D), f32),
            pltpu.VMEM((2, chips, seqs, D), bf16),
            pltpu.VMEM((chips, seqs, D), bf16),
            pltpu.VMEM((chips, seqs, D), bf16),
            pltpu.VMEM((chips, seqs, D), bf16),
            dma((len(loaded) + len(scalars),)),
            dma((3,)),
            dma((2,)),
            dma((2,)),
            dma((2,)),
            dma((2,)),
            dma((pieces,)),
            dma((pieces, 2 * lines + 1)),
            dma((2,)),
            dma((2, 2)),
            dma(()),
            dma((2, chunks)),
            dma(()),
            dma((2, chunks)),
            dma(()),
            dma((chunks,)),
            dma(()),
            dma((b_chunks,)),
            dma((2,)),
        ],
        compiler_params=pltpu.CompilerParams(
            collective_id=0, has_side_effects=True, vmem_limit_bytes=58 * 2**20
        ),
    )(*scalars, *loaded, w_gate, w_up, w_down)


def local(*arrays):
    devices = lax.axis_size("expert")
    experts = arrays[10].shape[1]
    if experts == TOPK and devices == 2 * experts and devices % 4 == 0:
        return dense(*arrays)
    return routed(*arrays)


def solution(mesh):
    return jax.shard_map(
        local,
        mesh=mesh,
        in_specs=(
            P(("groups", "expert"), None),
            P(("groups", "expert"), None),
            P(("groups", "expert"), None, None),
            P(("groups", "expert"), None, None, None),
            P(("groups", "expert"), None),
            P(("groups", "expert")),
            P(("groups", "expert"), None, None, None, None),
            P("groups"),
            P("groups"),
            P(),
            P(),
            P("expert", None, None),
            P("expert", None, None),
            P("expert", None, None),
            P(("groups", "expert"), None),
        ),
        out_specs=P(("groups", "expert"), None),
        check_vma=False,
    )
```

```python
import functools
import math

import jax
import jax.numpy as jnp
from jax import lax
from jax.experimental import pallas as pl
from jax.experimental.pallas import tpu as pltpu
from jax.sharding import PartitionSpec as P

D = 4096
QUERY_HEADS = 32
KEY_VALUE_HEADS = 2
HEAD_SIZE = 128
PAGE_TOKENS = 16
TOPK = 8
MAXB = 16
MAXP = 2


norm_eps = 1e-06
masked_score = -1e30


def partner(x, axis, apart):
    return lax.ppermute(x, axis, [(i, i ^ 1 << apart) for i in range(lax.axis_size(axis))])


def attend(rows_of_queries, rows_of_keys, rows_of_values, allowed, token_own_key, token_own_value):
    decode_tokens = rows_of_queries.shape[0]
    heads_of_queries = rows_of_queries.reshape(
        decode_tokens, KEY_VALUE_HEADS, QUERY_HEADS // KEY_VALUE_HEADS, HEAD_SIZE
    )
    heads_of_keys = rows_of_keys.reshape(decode_tokens, -1, KEY_VALUE_HEADS, HEAD_SIZE)
    heads_of_values = rows_of_values.reshape(decode_tokens, -1, KEY_VALUE_HEADS, HEAD_SIZE)
    scale_for_scores = 1.0 / math.sqrt(HEAD_SIZE)
    allowed_mask = allowed[:, None, None, :]
    scores = (
        jnp.einsum(
            "tkgd,tlkd->tkgl", heads_of_queries, heads_of_keys, preferred_element_type=jnp.float32
        )
        * scale_for_scores
    )
    scores = jnp.where(allowed_mask, scores, masked_score)
    token_own_score = (
        jnp.einsum(
            "xejp,xep->xej",
            heads_of_queries,
            token_own_key.reshape(decode_tokens, KEY_VALUE_HEADS, HEAD_SIZE),
            preferred_element_type=jnp.float32,
        )
        * scale_for_scores
    )
    peak = jnp.maximum(jnp.max(scores, -1), token_own_score)
    weights = jnp.where(allowed_mask, jnp.exp(scores - peak[..., None]), 0.0)
    own_weight = jnp.exp(token_own_score - peak)
    denominator = jnp.sum(weights, -1) + own_weight
    probs = (weights / denominator[..., None]).astype(jnp.bfloat16)
    token_own_probability = (own_weight / denominator).astype(jnp.bfloat16)
    blended_noise = jnp.einsum(
        "tkgl,tlkd->tkgd", probs, heads_of_values, preferred_element_type=jnp.float32
    )
    blended_noise = blended_noise + token_own_probability.astype(jnp.float32)[
        ..., None
    ] * token_own_value.reshape(decode_tokens, KEY_VALUE_HEADS, 1, HEAD_SIZE).astype(jnp.float32)
    return blended_noise.reshape(decode_tokens, QUERY_HEADS * HEAD_SIZE).astype(jnp.bfloat16)


def routed(
    hidden_in,
    queries,
    decode_key_value,
    local_kv,
    page_table,
    seq_blocks,
    prompt_kv,
    prompt_owner,
    prompt_pages,
    norm_gain,
    router,
    w_gate,
    w_up,
    w_down,
    route_ids,
):
    devices = lax.axis_size("expert")
    position = lax.axis_index("expert")
    experts = devices // 2
    seq_dev = hidden_in.shape[0]
    key_value_width = KEY_VALUE_HEADS * HEAD_SIZE
    capacity = min(seq_dev, max(2, 2 * ((3 * seq_dev * TOPK + 2 * devices - 1) // (2 * devices))))
    half_cap = capacity // 2
    even_core = position % 2 == 0
    prompt_count = prompt_owner.shape[0]
    prompt_range = jnp.arange(prompt_count, dtype=jnp.int32)
    same_owner = prompt_owner[:, None] == prompt_owner[None, :]
    earlier = prompt_range[None, :] < prompt_range[:, None]
    arrival = jnp.sum((same_owner & earlier).astype(jnp.int32), 1)
    matching = (
        prompt_owner[None, None, :] == jnp.arange(devices, dtype=jnp.int32)[:, None, None]
    ) & (arrival[None, None, :] == jnp.arange(MAXP, dtype=jnp.int32)[None, :, None])
    chosen_prompt = jnp.sum(jnp.where(matching, prompt_range[None, None, :], 0), -1)
    occupied = jnp.any(matching, -1)
    own_picks = lax.dynamic_index_in_dim(chosen_prompt, position, 0, keepdims=False)
    own_occupied = lax.dynamic_index_in_dim(occupied, position, 0, keepdims=False)
    page_rows = prompt_kv[0]
    outgoing = jnp.take(page_rows, chosen_prompt.T.reshape(-1), axis=0).reshape(
        MAXP, devices, 2, PAGE_TOKENS, key_value_width
    )
    outgoing = jnp.where(occupied.T[:, :, None, None, None], outgoing, 0)
    arrived = lax.all_to_all(outgoing, "expert", split_axis=1, concat_axis=1, tiled=True)
    lengths = jnp.take(prompt_pages, own_picks)
    new_keys = arrived[:, :, 0].reshape(MAXP, devices * PAGE_TOKENS, key_value_width)
    new_values = arrived[:, :, 1].reshape(MAXP, devices * PAGE_TOKENS, key_value_width)
    new_allowed = (jnp.arange(devices * PAGE_TOKENS, dtype=jnp.int32) // PAGE_TOKENS)[
        None, :
    ] < lengths[:, None]
    fresh_rows = attend(
        queries[:MAXP],
        new_keys,
        new_values,
        new_allowed,
        decode_key_value[:MAXP, 0],
        decode_key_value[:MAXP, 1],
    )
    fetched = local_kv[page_table]
    old_keys = fetched[:, :, 0].reshape(seq_dev, MAXB * PAGE_TOKENS, key_value_width)
    old_values = fetched[:, :, 1].reshape(seq_dev, MAXB * PAGE_TOKENS, key_value_width)
    old_allowed = (jnp.arange(MAXB * PAGE_TOKENS, dtype=jnp.int32) // PAGE_TOKENS)[
        None, :
    ] < seq_blocks[:, None]
    old_out = attend(
        queries, old_keys, old_values, old_allowed, decode_key_value[:, 0], decode_key_value[:, 1]
    )
    new_count = jnp.sum(own_occupied.astype(jnp.int32))
    is_new = jnp.arange(MAXP, dtype=jnp.int32) < new_count
    attention = jnp.concatenate(
        [jnp.where(is_new[:, None], fresh_rows, old_out[:MAXP]), old_out[MAXP:]], 0
    )
    residual = (hidden_in.astype(jnp.float32) + attention.astype(jnp.float32)).astype(jnp.bfloat16)
    resid_wide = residual.astype(jnp.float32)
    normed = (
        resid_wide
        * lax.rsqrt(jnp.mean(resid_wide * resid_wide, -1, keepdims=True) + norm_eps)
        * norm_gain
    ).astype(jnp.bfloat16)
    logits = jnp.dot(normed, router, preferred_element_type=jnp.float32)
    expert_onehot = route_ids[:, :, None] == jnp.arange(experts, dtype=jnp.int32)[None, None, :]
    selected = jnp.sum(jnp.where(expert_onehot, logits[:, None, :], 0.0), -1)
    gate_weights = jax.nn.softmax(selected, -1)
    assigned = seq_dev * TOPK
    expert_ids = route_ids.reshape(assigned)
    chosen = (expert_ids[:, None] == jnp.arange(experts, dtype=jnp.int32)[None, :]).astype(
        jnp.int32
    )
    before = jnp.cumsum(chosen, 0) - chosen
    slot_rank = jnp.sum(before * chosen, 1)
    slot_index = expert_ids * capacity + slot_rank
    placing = slot_index[None, :] == jnp.arange(experts * capacity, dtype=jnp.int32)[:, None]
    selector = jnp.any(placing.reshape(experts * capacity, seq_dev, TOPK), -1).astype(jnp.bfloat16)
    gathered_rows = jnp.dot(selector, normed, preferred_element_type=jnp.float32).astype(
        jnp.bfloat16
    )
    outgoing_half = gathered_rows.reshape(devices, half_cap, D)
    own_half = lax.all_to_all(outgoing_half, "expert", split_axis=0, concat_axis=0, tiled=True)
    partner_half = partner(own_half, "expert", 0)
    received = jnp.where(
        even_core,
        jnp.concatenate([own_half, partner_half], 1),
        jnp.concatenate([partner_half, own_half], 1),
    )
    flattened = received.reshape(devices * capacity, D)
    gate_proj = jnp.dot(flattened, w_gate[0], preferred_element_type=jnp.float32)
    up_proj = jnp.dot(flattened, w_up[0], preferred_element_type=jnp.float32)
    activated = (jax.nn.silu(gate_proj) * up_proj).astype(jnp.bfloat16)
    partial_value = jnp.dot(activated, w_down[0], preferred_element_type=jnp.float32).reshape(
        devices, capacity, D
    )
    kept = jnp.where(even_core, partial_value[:, :half_cap], partial_value[:, half_cap:])
    handed = jnp.where(even_core, partial_value[:, half_cap:], partial_value[:, :half_cap])
    partner_part = partner(handed, "expert", 0)
    finished = (kept + partner_part).astype(jnp.bfloat16)
    returned = lax.all_to_all(finished, "expert", split_axis=0, concat_axis=0, tiled=True)
    expert_sum = returned.reshape(experts * capacity, D)
    picked = jnp.take(expert_sum, slot_index, axis=0).astype(jnp.float32).reshape(seq_dev, TOPK, D)
    expert_mix = jnp.sum(picked * gate_weights[:, :, None], 1)
    return (resid_wide + expert_mix).astype(jnp.bfloat16)


def layer_kernel(
    devices,
    owners_hbm,
    lengths_hbm,
    blocks_hbm,
    pages_hbm,
    q_hbm,
    dkv_hbm,
    table_hbm,
    kv_hbm,
    hidden_hbm,
    gain_hbm,
    router_hbm,
    ids_hbm,
    gate_hbm,
    up_hbm,
    down_hbm,
    out_ref,
    owners,
    prompt_lengths,
    blocks,
    pages_ref,
    q_ref,
    dkv_ref,
    table_ref,
    kv_ref,
    hidden_ref,
    gain_ref,
    router_ref,
    ids_ref,
    w_in,
    w_down,
    other_pages,
    q_send,
    q_recv,
    o_send,
    o_recv,
    lse_send,
    lse_recv,
    attn,
    x_a,
    x_b,
    gates_b,
    part_a,
    core_a,
    z_send,
    z_recv,
    y_send,
    y_recv,
    kept,
    part_b,
    core_b,
    sum_b,
    recv_b,
    in_sem,
    w_sem,
    page_sem,
    q_sem,
    o_sem,
    lse_sem,
    xa_ssem,
    xa_rsem,
    xb_ssem,
    xb_rsem,
    c_ssem,
    c_rsem,
    z_ssem,
    z_rsem,
    y_ssem,
    y_rsem,
    cb_ssem,
    cb_rsem,
    rb_sem,
):
    f32, bf16 = jnp.float32, jnp.bfloat16
    me = lax.axis_index("expert")
    lines = devices // 4
    chips = devices // 2
    core, row, line = lax.rem(me, 2), lax.rem(me // 2, 2), me // 4
    unit = row * lines + line
    seqs = hidden_ref.shape[0]
    group = QUERY_HEADS // KEY_VALUE_HEADS
    scale = 1.0 / math.sqrt(HEAD_SIZE)
    old_rows = pl.ds(MAXP, seqs - MAXP)
    new_rows = pl.ds(0, MAXP)

    def device(at_line, at_row, at_core):
        return (at_line * 2 + at_row) * 2 + at_core

    def device_of(at_unit, at_core):
        return device(lax.rem(at_unit, lines), at_unit // lines, at_core)

    def place(at_line, at_row, at_core):
        return (at_core * 2 + at_row) * lines + at_line

    low = line * 2 < lines

    def far_line(j):
        return jnp.where(low, lines - 1 - j, j)

    def far_other_line(j):
        down = lines - 1 - j
        return jnp.where(
            low, jnp.where(down > line, down, down - 1), jnp.where(j < line, j, j + 1)
        )

    def all_units():
        yield from other_units()
        yield unit

    def other_units():
        for j in range(lines):
            yield (1 - row) * lines + far_line(j)
            if j < lines - 1:
                yield row * lines + far_other_line(j)

    def remote(src, dst, ssem, rsem, to):
        return pltpu.make_async_remote_copy(
            src_ref=src,
            dst_ref=dst,
            send_sem=ssem,
            recv_sem=rsem,
            device_id={"expert": to},
            device_id_type=pl.DeviceIdType.MESH,
        )

    other_row = device(line, 1 - row, core)
    other_core = device(line, row, 1 - core)
    mine = place(line, row, core)

    loads = [
        pltpu.make_async_copy(a, b, in_sem.at[i])
        for i, (a, b) in enumerate(
            (
                (q_hbm, q_ref),
                (pages_hbm, pages_ref),
                (dkv_hbm, dkv_ref),
                (table_hbm, table_ref),
                (kv_hbm, kv_ref),
                (hidden_hbm, hidden_ref),
                (gain_hbm, gain_ref),
                (router_hbm, router_ref),
                (ids_hbm, ids_ref),
                (blocks_hbm, blocks),
                (owners_hbm, owners),
                (lengths_hbm, prompt_lengths),
            )
        )
    ]
    hidden = w_down.shape[0]
    weights = [
        pltpu.make_async_copy(gate_hbm.at[0], w_in.at[:, pl.ds(0, hidden)], w_sem.at[0]),
        pltpu.make_async_copy(up_hbm.at[0], w_in.at[:, pl.ds(hidden, hidden)], w_sem.at[1]),
        pltpu.make_async_copy(down_hbm.at[0], w_down, w_sem.at[2]),
    ]
    barrier = pltpu.get_barrier_semaphore()

    def greet(k, carry):
        pl.semaphore_signal(
            barrier,
            inc=1,
            device_id={"expert": lax.rem(me + k, devices)},
            device_id_type=pl.DeviceIdType.MESH,
        )
        return carry

    lax.fori_loop(1, devices, greet, 0)
    for copy in loads + weights:
        copy.start()

    fold = seqs // MAXP
    lane_heads = QUERY_HEADS // fold
    packed = lane_heads * HEAD_SIZE
    per_kv = lane_heads // KEY_VALUE_HEADS
    sub = lax.broadcasted_iota(jnp.int32, (seqs, packed), 0) // MAXP

    def head_cols(h):
        return slice(h * HEAD_SIZE, (h + 1) * HEAD_SIZE)

    def turn(x, by):
        by = by % seqs
        return x if by == 0 else pltpu.roll(x, by, 0)

    def pack(rows):
        out = None
        for f in range(fold):
            wide = turn(
                jnp.concatenate([rows[:, head_cols(fold * hh + f)] for hh in range(lane_heads)], 1),
                MAXP * f,
            )
            out = wide if f == 0 else jnp.where(sub == f, wide, out)
        return out

    def spread_rows(rows):
        out = rows
        at = lax.broadcasted_iota(jnp.int32, rows.shape, 0) // MAXP
        for f in range(1, fold):
            out = jnp.where(at == f, turn(rows, MAXP * f), out)
        return out

    def dot_t(a, b):
        return lax.dot_general(a, b, (((1,), (1,)), ((), ())), preferred_element_type=f32)

    loads[0].wait()
    q_packed = pack(q_ref[...].astype(f32))
    q_send[...] = q_packed.astype(bf16)
    for copy in loads[2:]:
        copy.wait()

    def per_seq(values, shape):
        at = lax.broadcasted_iota(jnp.int32, shape, 0)
        return sum(jnp.where(at == s, v, 0) for s, v in enumerate(values))

    tokens = kv_ref.shape[0] * PAGE_TOKENS
    limit = per_seq([blocks[s] for s in range(seqs)], (seqs, tokens))
    page_of = lax.broadcasted_iota(jnp.int32, (seqs, tokens), 1) // PAGE_TOKENS
    held = jnp.zeros((seqs, tokens), f32)
    for b in range(table_ref.shape[1]):
        hit = (page_of == table_ref[:, b : b + 1]) & (limit > b)
        held = held + jnp.where(hit, 1.0, 0.0)
    held = jnp.concatenate([held] * group, 0)

    def heads(h):
        rows = q_ref[...].astype(f32)
        return jnp.concatenate([rows[:, head_cols(h * group + g)] for g in range(group)], 0)

    def own(h, at):
        both = dkv_ref[...].astype(f32)
        return jnp.concatenate([both[:, at, head_cols(h)]] * group, 0)

    def weigh(scores, times, own_score):
        scores = jnp.where(times > 0, scores, masked_score)
        peak = jnp.maximum(jnp.max(scores, -1, keepdims=True), own_score)
        weight = times * jnp.exp(scores - peak)
        own_weight = jnp.exp(own_score - peak)
        total = jnp.sum(weight, -1, keepdims=True) + own_weight
        return (weight / total).astype(bf16), (own_weight / total).astype(bf16).astype(f32)

    for h in range(KEY_VALUE_HEADS):
        at = head_cols(h)
        queries = heads(h)
        own_score = jnp.sum(queries * own(h, 0), -1, keepdims=True) * scale
        keys = kv_ref[:, 0, :, at].reshape(tokens, HEAD_SIZE)
        values = kv_ref[:, 1, :, at].reshape(tokens, HEAD_SIZE)
        probs, own_prob = weigh(dot_t(queries.astype(bf16), keys) * scale, held, own_score)
        mixed = jnp.dot(probs, values, preferred_element_type=f32) + own_prob * own(h, 1)
        for g in range(group):
            attn[:, head_cols(h * group + g)] = mixed[g * seqs : (g + 1) * seqs]

    def residual_of(attention):
        rounded = attention.astype(bf16).astype(f32)
        return (hidden_ref[...].astype(f32) + rounded).astype(bf16).astype(f32)

    def norm_of(wide):
        mean = jnp.mean(wide * wide, -1, keepdims=True)
        return (wide * lax.rsqrt(mean + norm_eps) * gain_ref[...]).astype(bf16)

    def gate_of(normed):
        logits = dot_t(normed, router_ref[...])
        experts = logits.shape[1]
        expert_of = lax.broadcasted_iota(jnp.int32, (seqs, experts), 1)
        times = jnp.zeros((seqs, experts), f32)
        for k in range(ids_ref.shape[1]):
            times = times + jnp.where(ids_ref[:, k : k + 1] == expert_of, 1.0, 0.0)
        picked = jnp.where(times > 0, logits, masked_score)
        gate = times * jnp.exp(picked - jnp.max(picked, -1, keepdims=True))
        gate = gate / jnp.sum(gate, -1, keepdims=True)
        return jnp.concatenate([gate] * (128 // experts), 1)

    normed = norm_of(residual_of(attn[...]))
    x_a[mine, :, :D] = normed
    pl.semaphore_wait(barrier, devices - 1)

    def q_copy(to):
        return remote(q_send, q_recv.at[unit], q_sem.at[0], q_sem.at[1], device_of(to, 1 - core))

    for to in all_units():
        q_copy(to).start()
    loads[1].wait()
    page_copy = remote(pages_ref, other_pages, page_sem.at[0], page_sem.at[1], other_core)
    page_copy.start()


    def pass_on(pool, spot, count, at, to):
        buffer, rows, cols, n = pool
        ref = buffer.at[pl.ds(spot, count), rows, cols]
        return remote(ref, ref, xa_ssem.at[n], xa_rsem.at[n, at], to)

    far, near = lax.rem(line + 2, lines), line + 1 - 2 * lax.rem(line, 2)
    far_device, near_device = device(far, row, 1 - core), device(near, row, 1 - core)
    row_device = device(line, 1 - row, 1 - core)
    at_far, at_near, at_relay, at_core = 0, 1, 2, (7, 8)
    sources = (far, near, lax.rem(near + 2, lines), line)
    z_cores, y_cores = (1 - core, 1 - core, core), (core, core, 1 - core, 1 - core)

    def at_y(n):
        return 3 + n

    def cross(pool, spot, n):
        pass_on(pool, spot, 1, at_y(n), row_device).start()
        pass_on(pool, spot, 1, at_core[0], other_core).start()

    def z_arrive(pool, n):
        spot = place(sources[n], row, z_cores[n])
        pass_on(pool, spot, 1, n, other_row).wait_recv()
        if n == at_far:
            pass_on(pool, spot, 1, at_relay, near_device).start()
        cross(pool, spot, n)

    def y_arrive(pool, n):
        spot = place(sources[n], 1 - row, y_cores[n])
        pass_on(pool, spot, 1, at_y(n), other_row).wait_recv()
        pass_on(pool, spot, 1, at_core[1], other_core).start()

    def first_hops(pool):
        pass_on(pool, mine, 1, at_far, far_device).start()
        pass_on(pool, mine, 1, at_near, near_device).start()
        cross(pool, mine, 3)

    pieces = xa_ssem.shape[0]
    piece = D // pieces
    sizes = [piece] * (pieces - 1) + [piece + 128]
    pools = [(x_a, old_rows, pl.ds(n * piece, sizes[n]), n) for n in range(pieces)]
    for pool in pools[:-1]:
        first_hops(pool)
    gate = gate_of(normed)
    high = gate.astype(bf16)
    x_a[mine, :, D:] = jnp.where(
        lax.broadcasted_iota(jnp.int32, (seqs, 128), 1) < 128 // 2,
        high.astype(f32),
        gate - high.astype(f32),
    ).astype(bf16)
    first_hops(pools[-1])

    prompts = owners.shape[0]
    shape = (1, prompts * PAGE_TOKENS)
    prompt_of = lax.broadcasted_iota(jnp.int32, shape, 1) // PAGE_TOKENS
    owner_of, length_of = jnp.zeros(shape, jnp.int32), jnp.zeros(shape, jnp.int32)
    for p in range(prompts):
        owner_of = jnp.where(prompt_of == p, owners[p], owner_of)
        length_of = jnp.where(prompt_of == p, prompt_lengths[p], length_of)
    rank_of = jnp.zeros(shape, jnp.int32)
    for p in range(prompts):
        rank_of = rank_of + jnp.where((owner_of == owners[p]) & (prompt_of > p), 1, 0)
    slots = chips * seqs
    at_row = lax.broadcasted_iota(jnp.int32, (slots, 1), 0)
    row_unit = at_row // seqs
    row_owner = device_of(row_unit, 1 - core)
    match = (owner_of == row_owner) & (rank_of == lax.rem(at_row, MAXP))

    def allowed_at(position):
        ok = match & (length_of > position)
        return jnp.concatenate([jnp.where(ok, 1.0, 0.0)] * per_kv, 0)

    allowed = (allowed_at(me), allowed_at(other_core))
    page_copy.wait_recv()

    q_all = remote(q_recv, q_recv, q_sem.at[0], q_sem.at[1], other_core)
    q_all.wait_recv()
    wide_kv = per_kv * HEAD_SIZE

    def o_copy(to, h):
        cols = pl.ds(h * wide_kv, wide_kv)
        return remote(
            o_send.at[to, :, cols],
            o_recv.at[unit, :, cols],
            o_sem.at[0],
            o_sem.at[1],
            device_of(to, 1 - core),
        )

    def lse_copy(to):
        at = device_of(to, 1 - core)
        return remote(lse_send.at[to], lse_recv.at[unit], lse_sem.at[0], lse_sem.at[1], at)

    lane_of = lax.broadcasted_iota(jnp.int32, (slots, 128), 1)
    lse_all = jnp.zeros((slots, 128), f32)
    for h in range(KEY_VALUE_HEADS):
        at = head_cols(h)
        lanes = [h * per_kv + j for j in range(per_kv)]
        queries = jnp.concatenate(
            [q_recv[:, :, head_cols(hh)].reshape(slots, HEAD_SIZE) for hh in lanes], 0
        )
        scores = []
        for ref, ok in zip((pages_ref, other_pages), allowed):
            keys = ref[:, 0, :, at].reshape(prompts * PAGE_TOKENS, HEAD_SIZE)
            scores.append(jnp.where(ok > 0, dot_t(queries, keys) * scale, masked_score))
        peak = jnp.maximum(
            jnp.max(scores[0], -1, keepdims=True), jnp.max(scores[1], -1, keepdims=True)
        )
        total = jnp.zeros((slots * per_kv, 1), f32)
        mixed = jnp.zeros((slots * per_kv, HEAD_SIZE), f32)
        for ref, score in zip((pages_ref, other_pages), scores):
            weight = jnp.exp(score - peak)
            total = total + jnp.sum(weight, -1, keepdims=True)
            values = ref[:, 1, :, at].reshape(prompts * PAGE_TOKENS, HEAD_SIZE)
            mixed = mixed + jnp.dot(weight.astype(bf16), values, preferred_element_type=f32)
        mixed = mixed / total
        lse = jnp.where(peak > masked_score, peak + jnp.log(total), masked_score)
        for j, hh in enumerate(lanes):
            rows = slice(j * slots, (j + 1) * slots)
            o_send[:, :, head_cols(hh)] = mixed[rows].astype(bf16).reshape(chips, seqs, HEAD_SIZE)
            lse_all = jnp.where(lane_of == hh, lse[rows], lse_all)
        for to in all_units():
            o_copy(to, h).start()
    lse_send[...] = lse_all.reshape(chips, seqs, 128)

    for to in all_units():
        lse_copy(to).start()

    for pool in pools:
        z_arrive(pool, at_far)
    for pool in pools:
        z_arrive(pool, at_near)
    for pool in pools:
        y_arrive(pool, 3)
    for pool in pools:
        z_arrive(pool, at_relay)

    own_both = dkv_ref[...].astype(f32)
    own_key = spread_rows(own_both[:, 0])
    own_value = spread_rows(own_both[:, 1])
    lane = lax.broadcasted_iota(jnp.int32, (seqs, 128), 1)
    own_score = jnp.zeros((seqs, 128), f32)
    for hh in range(lane_heads):
        score = jnp.sum(
            q_packed[:, head_cols(hh)] * own_key[:, head_cols(hh // per_kv)], -1, keepdims=True
        )
        own_score = jnp.where(lane == hh, score * scale, own_score)
    new_count = jnp.int32(0)
    for p in range(prompts):
        new_count = new_count + (owners[p] == me).astype(jnp.int32)
    is_new = lax.broadcasted_iota(jnp.int32, (seqs, HEAD_SIZE), 0) < new_count

    o_all = (
        remote(o_recv, o_recv, o_sem.at[0], o_sem.at[1], other_core),
        remote(lse_recv, lse_recv, lse_sem.at[0], lse_sem.at[1], other_core),
    )
    for copy in o_all:
        copy.wait_recv()
    peak = own_score
    for u in range(chips):
        peak = jnp.maximum(peak, lse_recv[u])
    shares = [jnp.exp(lse_recv[u] - peak) for u in range(chips)]
    own_share = jnp.exp(own_score - peak)
    total = own_share
    for share in shares:
        total = total + share
    inverse = 1.0 / total
    shares = [share * inverse for share in shares]
    own_share = own_share * inverse
    for hh in range(lane_heads):
        at = head_cols(hh)
        mixed = own_share[:, hh : hh + 1] * own_value[:, head_cols(hh // per_kv)]
        for u in range(chips):
            mixed = mixed + shares[u][:, hh : hh + 1] * o_recv[u, :, at].astype(f32)
        for f in range(fold):
            cols = head_cols(fold * hh + f)
            attn[:, cols] = jnp.where(is_new, turn(mixed, -MAXP * f), attn[:, cols])
    wide = residual_of(attn[...])
    attn[...] = wide
    normed = norm_of(wide)
    x_b[mine] = normed

    b_pools = [(x_b, new_rows, 0), (gates_b, pl.ds(0, seqs), 1)]

    def b_copy(pool, to):
        buffer, rows, n = pool
        ref = buffer.at[mine, rows]
        return remote(ref, ref, xb_ssem.at[n], xb_rsem.at[n, 0], device_of(to, 1 - core))

    def b_core_copy(pool, spot, count):
        buffer, rows, n = pool
        ref = buffer.at[pl.ds(spot, count), rows]
        return remote(ref, ref, xb_ssem.at[n], xb_rsem.at[n, 1], other_core)

    def b_first(pool):
        for to in other_units():
            b_copy(pool, to).start()
        b_core_copy(pool, mine, 1).start()

    def b_pass(pool):
        buffer, rows, n = pool
        ref = buffer.at[pl.ds(0, chips - 1), rows]
        remote(ref, ref, xb_ssem.at[n], xb_rsem.at[n, 0], other_core).wait_recv()
        for source in other_units():
            b_core_copy(pool, (1 - core) * chips + source, 1).start()

    b_first(b_pools[0])
    gates_b[mine] = gate_of(normed)
    b_first(b_pools[1])

    for copy in weights:
        copy.wait()

    def activate(both, gate, parts):
        lanes_of = lax.broadcasted_iota(jnp.int32, gate.shape, 1)
        gate_proj, up_proj = both[:, :hidden], both[:, hidden:]
        kept_lanes = lanes_of == me // 2
        if parts == 2:
            kept_lanes = kept_lanes | (lanes_of == 128 // 2 + me // 2)
        scaled = jnp.sum(jnp.where(kept_lanes, gate, 0.0), -1, keepdims=True)
        return (gate_proj / (1.0 + jnp.exp(-gate_proj)) * up_proj * scaled).astype(bf16)

    total = devices * seqs

    def rows_of(ref):
        return ref[...].reshape(total, ref.shape[2])

    chunks = c_rsem.shape[1]
    ends = (0, D // 4, 5 * D // 8, D)

    def cut(i):
        return slice(ends[i], ends[i + 1])

    def core_copy(n, i):
        return remote(
            part_a.at[1 - core, kinds[n], :, old_rows, cut(i)],
            core_a.at[kinds[n], :, old_rows, cut(i)],
            c_ssem,
            c_rsem.at[n, i],
            other_core,
        )

    for n in range(2):
        for pool in pools:
            y_arrive(pool, n)

    def core_arrive(n):
        for pool in pools:
            pass_on(pool, 0, lines, at_core[n], other_core).wait_recv()

    def row_activated(at_row):
        x = jnp.concatenate(
            [
                x_a[pl.ds((at * 2 + at_row) * lines, lines)].reshape(lines * seqs, D + 128)
                for at in range(2)
            ],
            0,
        )
        both = jnp.dot(x[:, :D], w_in[...], preferred_element_type=f32)
        return activate(both, x[:, D:].astype(f32), 2)

    kinds = (row, 1 - row)

    def z_sum_copy(n, i, k):
        to = lax.rem(line + k, lines)
        return remote(
            z_send.at[k, kinds[n], old_rows, cut(i)],
            z_recv.at[k, kinds[n], old_rows, cut(i)],
            z_ssem,
            z_rsem.at[n, i],
            device(to, row, core),
        )

    def y_sum_copy(i):
        return remote(
            y_send.at[old_rows, cut(i)],
            y_recv.at[old_rows, cut(i)],
            y_ssem,
            y_rsem.at[i],
            other_row,
        )

    def held_by(at_row, at_line, i):
        return part_a[core, at_row, at_line, :, cut(i)].astype(f32) + core_a[
            at_row, at_line, :, cut(i)
        ].astype(f32)

    def z_step(n, i):
        core_copy(n, i).wait_recv()
        for k in (2, 1, 3):
            z_send[k, kinds[n], :, cut(i)] = held_by(
                kinds[n], lax.rem(line + k, lines), i
            ).astype(bf16)
            z_sum_copy(n, i, k).start()

    def y_step(i):
        for n in range(2):
            ref = z_recv.at[pl.ds(1, lines - 1), kinds[n], old_rows, cut(i)]
            remote(ref, ref, z_ssem, z_rsem.at[n, i], other_core).wait_recv()

        def summed(at_row):
            value = held_by(at_row, line, i)
            for k in range(1, lines):
                value = value + z_recv[k, at_row, :, cut(i)].astype(f32)
            return value

        y_send[:, cut(i)] = summed(1 - row).astype(bf16)
        y_sum_copy(i).start()
        kept[:, cut(i)] = attn[:, cut(i)] + summed(row)

    def down(n, i, activated):
        rows = jnp.dot(activated, w_down[:, cut(i)], preferred_element_type=f32)
        part_a[:, kinds[n], :, :, cut(i)] = rows.astype(bf16).reshape(
            2, lines, seqs, ends[i + 1] - ends[i]
        )
        core_copy(n, i).start()

    def expert_rows(n, between):
        core_arrive(n)
        activated = row_activated(kinds[n])
        between[0]()
        for i in range(chunks):
            down(n, i, activated)
            if i == 1:
                between[1]()
            if i >= behind:
                z_step(n, i - behind)
        for i in range(chunks - behind, chunks):
            z_step(n, i)

    def finish_gather():
        for pool in pools:
            y_arrive(pool, 2)

    def pass_b():
        for pool in b_pools:
            b_pass(pool)

    def nothing():
        pass

    behind = 1
    expert_rows(0, (finish_gather, nothing))
    expert_rows(1, (nothing, pass_b))

    for pool in b_pools:
        b_core_copy(pool, 0, chips).wait_recv()
    both = jnp.dot(rows_of(x_b), w_in[...], preferred_element_type=f32)
    activated = activate(both, rows_of(gates_b), 1)
    b_chunks = cb_rsem.shape[0]
    b_width = D // b_chunks

    def b_core(i):
        at = slice(i * b_width, (i + 1) * b_width)
        return remote(
            part_b.at[core, :, new_rows, at],
            core_b.at[:, new_rows, at],
            cb_ssem,
            cb_rsem.at[i],
            other_core,
        )

    for i in range(b_chunks):
        at = slice(i * b_width, (i + 1) * b_width)
        rows = jnp.dot(activated, w_down[:, at], preferred_element_type=f32)
        part_b[:, :, :, at] = rows.astype(bf16).reshape(2, chips, seqs, b_width)
        b_core(i).start()

    def b_return(to):
        return remote(
            sum_b.at[to, new_rows],
            recv_b.at[unit, new_rows],
            rb_sem.at[0],
            rb_sem.at[1],
            device_of(to, 1 - core),
        )

    for i in range(b_chunks):
        b_core(i).wait_recv()
    for to in all_units():
        sum_b[to] = (part_b[1 - core, to].astype(f32) + core_b[to].astype(f32)).astype(bf16)
        b_return(to).start()
    for i in range(chunks):
        y_step(i)
    b_all = remote(
        recv_b.at[:, new_rows], recv_b.at[:, new_rows], rb_sem.at[0], rb_sem.at[1], other_core
    )
    b_all.wait_recv()
    last = attn[...]
    for u in range(chips):
        last = last + recv_b[u].astype(f32)
    for i in range(chunks):
        y_sum_copy(i).wait_recv()
    answer = kept[...] + y_recv[...].astype(f32)
    is_b = lax.broadcasted_iota(jnp.int32, (seqs, D), 0) < MAXP
    out_ref[...] = jnp.where(is_b, last, answer).astype(bf16)

    for copy in (page_copy, q_all, b_all) + o_all:
        copy.wait_send()
    for pool in pools:
        pass_on(pool, 0, 4 * lines - 1, 0, other_core).wait_send()
    for n, (buffer, rows) in enumerate(((x_b, new_rows), (gates_b, pl.ds(0, seqs)))):
        ref = buffer.at[pl.ds(0, 2 * chips - 1), rows]
        remote(ref, ref, xb_ssem.at[n], xb_rsem.at[n, 0], other_core).wait_send()
    for ref, ssem, rsem in (
        (part_a.at[0, :, :, old_rows], c_ssem, c_rsem.at[0, 0]),
        (z_send.at[pl.ds(1, lines - 1), :, old_rows], z_ssem, z_rsem.at[0, 0]),
        (y_send.at[old_rows], y_ssem, y_rsem.at[0]),
        (part_b.at[0, :, new_rows], cb_ssem, cb_rsem.at[0]),
    ):
        remote(ref, ref, ssem, rsem, other_core).wait_send()


def dense(
    hidden_in,
    queries,
    decode_key_value,
    local_kv,
    page_table,
    seq_blocks,
    prompt_kv,
    prompt_owner,
    prompt_pages,
    norm_gain,
    router,
    w_gate,
    w_up,
    w_down,
    route_ids,
):
    devices = lax.axis_size("expert")
    seqs = hidden_in.shape[0]
    hidden = w_gate.shape[2]
    lines = devices // 4
    chips = devices // 2
    bf16, f32 = jnp.bfloat16, jnp.float32
    chunks = 3
    pieces = 1
    b_chunks = 2
    packed = D * MAXP // seqs
    loaded = (
        prompt_kv[0],
        queries,
        decode_key_value,
        page_table,
        local_kv,
        hidden_in,
        norm_gain[None, :],
        router.T,
        route_ids,
    )
    scalars = (prompt_owner, prompt_pages, seq_blocks)
    hbm = pl.BlockSpec(memory_space=pltpu.HBM)
    dma = pltpu.SemaphoreType.DMA
    return pl.pallas_call(
        functools.partial(layer_kernel, devices),
        out_shape=pltpu.VMEM((seqs, D), bf16),
        in_specs=[hbm] * (len(loaded) + 6),
        out_specs=pl.BlockSpec(memory_space=pltpu.VMEM),
        scratch_shapes=[pltpu.SMEM(a.shape, a.dtype) for a in scalars]
        + [pltpu.VMEM(a.shape, a.dtype) for a in loaded]
        + [
            pltpu.VMEM((D, 2 * hidden), bf16),
            pltpu.VMEM((hidden, D), bf16),
            pltpu.VMEM(loaded[0].shape, bf16),
            pltpu.VMEM((seqs, packed), bf16),
            pltpu.VMEM((chips, seqs, packed), bf16),
            pltpu.VMEM((chips, seqs, packed), bf16),
            pltpu.VMEM((chips, seqs, packed), bf16),
            pltpu.VMEM((chips, seqs, 128), f32),
            pltpu.VMEM((chips, seqs, 128), f32),
            pltpu.VMEM((seqs, D), f32),
            pltpu.VMEM((devices, seqs, D + 128), bf16),
            pltpu.VMEM((devices, seqs, D), bf16),
            pltpu.VMEM((devices, seqs, 128), f32),
            pltpu.VMEM((2, 2, lines, seqs, D), bf16),
            pltpu.VMEM((2, lines, seqs, D), bf16),
            pltpu.VMEM((lines, 2, seqs, D), bf16),
            pltpu.VMEM((lines, 2, seqs, D), bf16),
            pltpu.VMEM((seqs, D), bf16),
            pltpu.VMEM((seqs, D), bf16),
            pltpu.VMEM((seqs, D), f32),
            pltpu.VMEM((2, chips, seqs, D), bf16),
            pltpu.VMEM((chips, seqs, D), bf16),
            pltpu.VMEM((chips, seqs, D), bf16),
            pltpu.VMEM((chips, seqs, D), bf16),
            dma((len(loaded) + len(scalars),)),
            dma((3,)),
            dma((2,)),
            dma((2,)),
            dma((2,)),
            dma((2,)),
            dma((pieces,)),
            dma((pieces, 2 * lines + 1)),
            dma((2,)),
            dma((2, 2)),
            dma(()),
            dma((2, chunks)),
            dma(()),
            dma((2, chunks)),
            dma(()),
            dma((chunks,)),
            dma(()),
            dma((b_chunks,)),
            dma((2,)),
        ],
        compiler_params=pltpu.CompilerParams(
            collective_id=0, has_side_effects=True, vmem_limit_bytes=58 * 2**20
        ),
    )(*scalars, *loaded, w_gate, w_up, w_down)


def local(*arrays):
    devices = lax.axis_size("expert")
    experts = arrays[10].shape[1]
    if experts == TOPK and devices == 2 * experts and devices % 4 == 0:
        return dense(*arrays)
    return routed(*arrays)


def solution(mesh):
    return jax.shard_map(
        local,
        mesh=mesh,
        in_specs=(
            P(("groups", "expert"), None),
            P(("groups", "expert"), None),
            P(("groups", "expert"), None, None),
            P(("groups", "expert"), None, None, None),
            P(("groups", "expert"), None),
            P(("groups", "expert")),
            P(("groups", "expert"), None, None, None, None),
            P("groups"),
            P("groups"),
            P(),
            P(),
            P("expert", None, None),
            P("expert", None, None),
            P("expert", None, None),
            P(("groups", "expert"), None),
        ),
        out_specs=P(("groups", "expert"), None),
        check_vma=False,
    )
```
